32 devices in a mesh: lat: 4 (over y, x), lon: 8 (over z, core).
Axes of the slice: x: 2, y: 2, z: 4, core: 2. Of those that a mesh axis runs over, the one named last changes fastest.
Arguments:
- fields: bfloat16 [192, 256, 2, 256], P('lat', 'lon'), may hold values from -6 to 6
- ocean_mask: int32 [24, 32], P('lat'), may hold values from 0 to 1, as said below
- gain_one: float32 [256], replicated, may hold values from 0.1 to 1.9
- w_qkv: bfloat16 [256, 768], replicated, may hold values from -0.375 to 0.375
- rel_bias: float32 [8, 675], replicated, may hold values from -80 to 150
- w_proj: bfloat16 [256, 256], replicated, may hold values from -0.375 to 0.375
- gain_two: float32 [256], replicated, may hold values from 0.1 to 1.9
- w_up: bfloat16 [256, 1024], replicated, may hold values from -0.375 to 0.375
- w_down: bfloat16 [1024, 256], replicated, may hold values from -0.1875 to 0.1875
Outputs:
- ocean_out: bfloat16 [192, 256, 2, 256], P('lat', 'lon')
The draws below stay inside these ranges and needn't reach their ends.
Inputs may be any that keep to these rules, and one draw needn't show every extreme that they name: `ocean_mask`: the windows of the last row of windows (a = 23) are land. Each band of 6 rows of windows held by one index of lat holds exactly 10 ocean windows per longitude device. Taking the devices of a band in order of longitude index, each holding 4 columns of windows, the ocean windows of the first d devices number at least d * 10 and at most d * 10 + 10; the upper bound is reached for some d in every band, at places drawn anew. One device holds 0 to 20 ocean windows.
All inputs are finite; a program needn't handle non-finite values.
Results may differ from the reference program's by a relative error of at most 0.0057.
Values may be sent and summed in bfloat16 or wider, within the bound.
A program may use at most 64 MiB of HBM per device.

```python
import math
import jax
import jax.numpy as jnp
from jax import lax

C = 256
HEADS = 8
FF = 1024
WIN_LAT = 8
WIN_LON = 8
DEPTH = 2
LAT_WIN = 6
LON_WIN = 4
SLOTS = 10
BIAS_LEN = 675
NLAT_WIN = 24
NLON_WIN = 32
NLAT = 192
NLON = 256
OCEAN = 320
N_LAT = 4
N_LON = 8


def band_mask(key, band):
    first_key, second_key, third_key = jax.random.split(key, 3)
    device_ids = jnp.arange(N_LON, dtype=jnp.int32)
    excess = jax.random.randint(first_key, (N_LON,), 0, SLOTS + 1, dtype=jnp.int32)
    spot = jax.random.randint(second_key, (), 0, N_LON - 1, dtype=jnp.int32)
    excess = jnp.where(device_ids == spot, SLOTS, excess)
    excess = jnp.where(device_ids == spot - 1, 0, excess)
    excess = jnp.where(device_ids == N_LON - 1, 0, excess)
    earlier = jnp.concatenate([jnp.zeros((1,), jnp.int32), excess[:-1]])
    counts = SLOTS + excess - earlier
    total_windows = LAT_WIN * LON_WIN
    window_rows = jnp.arange(total_windows, dtype=jnp.int32) // LON_WIN
    blocked = jnp.logical_and(band == N_LAT - 1, window_rows == LAT_WIN - 1).astype(jnp.int32)

    def one_device(device, count):
        shuffled = jax.random.permutation(jax.random.fold_in(third_key, device), total_windows).astype(jnp.int32)
        score_ids = shuffled + total_windows * blocked
        ranking = jnp.argsort(jnp.argsort(score_ids))
        return (ranking < count).astype(jnp.int32).reshape(LAT_WIN, LON_WIN)
    tiles = jax.vmap(one_device)(device_ids, counts)
    return tiles.transpose(1, 0, 2).reshape(LAT_WIN, N_LON * LON_WIN)


def draw_ocean_mask(key, part):
    band_ids = jnp.arange(N_LAT, dtype=jnp.int32)
    keyed = jax.vmap(lambda band_id: jax.random.fold_in(key, band_id))(band_ids)
    bands = jax.vmap(band_mask)(keyed, band_ids)
    return bands.reshape(NLAT_WIN, NLON_WIN)


def draw_rel_bias(key, part):
    first_key, second_key, third_key = jax.random.split(jax.random.fold_in(key, 17), 3)
    table = jax.random.uniform(first_key, (HEADS, BIAS_LEN), jnp.float32, -2.0, 2.0)
    return table


def shard_levels(key, shape, shards, low, largest):
    gain = 1.0
    for dim, parts in shards:
        draws = jax.random.uniform(jax.random.fold_in(jax.random.fold_in(key, 6), dim), (parts,), jnp.float32, low / len(shards), largest / len(shards))
        gain = gain * jnp.repeat(jnp.exp(draws), shape[dim] // parts).reshape((-1,) + (1,) * (len(shape) - 1 - dim))
    return gain


def noise(key, shape, deviation, most, cuts=(), kind=jnp.bfloat16):
    array = deviation * jax.random.normal(key, shape, jnp.float32)
    if cuts:
        array = array * shard_levels(key, shape, cuts, -0.22, 0.18)
    return jnp.clip(array, -most, most).astype(kind)


def setup_inputs(seed: int = 0) -> dict:
    seeds = jax.random.split(jax.random.key(seed), 10)
    return {
        "fields": noise(seeds[0], (NLAT, NLON, DEPTH, C), 1.0, 6.0, ((0, 4), (1, 8))),
        "ocean_mask": draw_ocean_mask(jax.random.fold_in(seeds[9], 71), 0),
        "gain_one": jnp.clip(1.0 + 0.18 * jax.random.normal(seeds[2], (C,), jnp.float32), 0.1, 1.9),
        "w_qkv": noise(seeds[3], (C, 3 * C), C ** -0.5, 0.375),
        "rel_bias": draw_rel_bias(jax.random.fold_in(seeds[9], 71), 0),
        "w_proj": noise(seeds[5], (C, C), C ** -0.5, 0.375),
        "gain_two": jnp.clip(1.0 + 0.18 * jax.random.normal(seeds[6], (C,), jnp.float32), 0.1, 1.9),
        "w_up": noise(seeds[7], (C, FF), C ** -0.5, 0.375),
        "w_down": noise(seeds[8], (FF, C), FF ** -0.5, 0.1875),
    }


NORM_FLOOR = 0.25

def product(form, left, right):
    return jnp.einsum(form, left.astype(jnp.float32), right.astype(jnp.float32), precision=lax.Precision.HIGHEST)

def layer_norm(values, gain_vec):
    average = lax.optimization_barrier(jnp.mean(values, axis=-1, keepdims=True))
    centred = values - average
    spread = lax.optimization_barrier(jnp.mean(centred * centred, axis=-1, keepdims=True))
    return centred / jnp.sqrt(spread + NORM_FLOOR) * gain_vec

def bias_table(rel_bias, win_lat, win_lon, levels):
    tokens = win_lat * win_lon * levels
    token_ids = jnp.arange(tokens, dtype=jnp.int32)
    token_row = token_ids // (win_lon * levels)
    token_col = token_ids // levels % win_lon
    token_lev = token_ids % levels
    row_gap = token_row[:, None] - token_row[None, :] + win_lat - 1
    col_gap = token_col[:, None] - token_col[None, :] + win_lon - 1
    lev_gap = token_lev[:, None] - token_lev[None, :] + levels - 1
    lookup = ((row_gap * (2 * win_lon - 1) + col_gap) * (2 * levels - 1) + lev_gap).astype(jnp.int32)
    return jnp.take(rel_bias, lookup, axis=1)

def window_block(block, weights):
    gain_one, w_qkv, bias_full, w_proj, gain_two, w_up, w_down = weights
    window_count, tokens, features = block.shape
    head_count = bias_full.shape[0]
    head_dim = features // head_count
    score_scale = 1.0 / math.sqrt(head_dim)
    normed = layer_norm(block.astype(jnp.float32), gain_one).astype(jnp.bfloat16)
    triple = product('ntc,cf->ntf', normed, w_qkv).astype(jnp.bfloat16)
    triple = triple.reshape(window_count, tokens, 3, head_count, head_dim)
    query_part = triple[:, :, 0]
    key_part = triple[:, :, 1]
    value_part = triple[:, :, 2]
    scores = product('nthd,nshd->nhts', query_part, key_part) * score_scale + bias_full[None]
    row_top = lax.optimization_barrier(jnp.max(scores, axis=-1, keepdims=True))
    exponent = jnp.exp(scores - row_top)
    attn_prob = (exponent / lax.optimization_barrier(jnp.sum(exponent, axis=-1, keepdims=True))).astype(jnp.bfloat16)
    mixed = product('nhts,nshd->nthd', attn_prob, value_part).astype(jnp.bfloat16)
    mixed = mixed.reshape(window_count, tokens, features)
    middle = (block.astype(jnp.float32) + product('ntc,cf->ntf', mixed, w_proj)).astype(jnp.bfloat16)
    normed_two = layer_norm(middle.astype(jnp.float32), gain_two).astype(jnp.bfloat16)
    hidden = jax.nn.gelu(product('ntc,cf->ntf', normed_two, w_up), approximate=False).astype(jnp.bfloat16)
    return (middle.astype(jnp.float32) + product('ntf,fc->ntc', hidden, w_down)).astype(jnp.bfloat16)

def run_windows(windows, weights):
    total_rows = windows.shape[0]
    block_size = 8 if total_rows % 8 == 0 else total_rows
    grouped = windows.reshape((total_rows // block_size, block_size) + windows.shape[1:])

    def one_group(group_win):
        return window_block(group_win, weights)
    finished = lax.map(one_group, grouped)
    return finished.reshape(windows.shape)

def reference(fields, ocean_mask, gain_one, w_qkv, rel_bias, w_proj, gain_two, w_up, w_down):
    lat_cells, lon_cells, levels, features = fields.shape
    lat_half = WIN_LAT // 2
    lon_half = WIN_LON // 2
    shifted = jnp.concatenate([fields[lat_half:], jnp.zeros_like(fields[:lat_half])], axis=0)
    shifted = jnp.roll(shifted, -lon_half, axis=1)
    lat_windows = lat_cells // WIN_LAT
    lon_windows = lon_cells // WIN_LON
    total_windows = lat_windows * lon_windows
    windows = shifted.reshape(lat_windows, WIN_LAT, lon_windows, WIN_LON, levels, features)
    windows = windows.transpose(0, 2, 1, 3, 4, 5).reshape(total_windows, WIN_LAT * WIN_LON * levels, features)
    flat_mask = ocean_mask.reshape(total_windows).astype(jnp.int32)
    window_ids = jnp.arange(total_windows, dtype=jnp.int32)
    ocean_order = jnp.argsort((1 - flat_mask) * total_windows + window_ids)[:OCEAN].astype(jnp.int32)
    picked = jnp.take(windows, ocean_order, axis=0)
    bias_full = bias_table(rel_bias, WIN_LAT, WIN_LON, levels)
    weights = (gain_one, w_qkv, bias_full, w_proj, gain_two, w_up, w_down)
    finished = run_windows(picked, weights)
    result = jnp.zeros_like(windows).at[ocean_order].set(finished)
    result = result.reshape(lat_windows, lon_windows, WIN_LAT, WIN_LON, levels, features)
    return result.transpose(0, 2, 1, 3, 4, 5).reshape(lat_cells, lon_cells, levels, features)
```

```python
import functools
import math

import jax
import jax.numpy as jnp
from jax import lax
from jax.experimental import pallas as pl
from jax.experimental.pallas import tpu as pltpu
from jax.sharding import PartitionSpec as P

WIN_LAT = 8
WIN_LON = 8
NORM_FLOOR = 0.25
MESH = pl.DeviceIdType.MESH
LOG2E = math.log2(math.e)
ROOT_HALF = math.sqrt(0.5)
PAIR = 2
EARLY_PAIRS = 2
LEAVING_PAIRS = 4


def dot(left, right):
    return jnp.dot(left, right, preferred_element_type=jnp.float32)


def normalise(values, gain):
    share = 1.0 / values.shape[0]
    average = jnp.sum(values, axis=0, keepdims=True) * share
    centred = values - average
    spread = jnp.sum(centred * centred, axis=0, keepdims=True) * share
    return (centred * lax.rsqrt(spread + NORM_FLOOR) * gain).astype(jnp.bfloat16)


def wide(gain, columns):
    return jnp.concatenate([gain] * (columns // gain.shape[1]), axis=1)


def attention_steps(store, blocks, weights):
    qkv_t, proj_t, gain, bias = weights["qkv"], weights["proj"], weights["gain_one"], weights["bias"]
    tokens, features = blocks[0].shape
    half = bias.shape[0]
    dim = features // (2 * half)
    scale = LOG2E / math.sqrt(dim)
    values = jnp.concatenate([block.T for block in blocks], axis=1).astype(jnp.float32)
    normed = normalise(values, wide(gain[...], values.shape[1]))
    yield
    key_t = dot(qkv_t[features : 2 * features], normed).astype(jnp.bfloat16)
    query_t = (dot(qkv_t[:features], normed) * scale).astype(jnp.bfloat16)
    value_t = dot(qkv_t[2 * features :], normed).astype(jnp.bfloat16)
    yield
    lane_head = lax.broadcasted_iota(jnp.int32, (tokens, features), 1) // dim % half
    nothing = jnp.zeros((features // 2, tokens), jnp.bfloat16)
    ones = jnp.ones((16, tokens), jnp.bfloat16)
    mixed = []
    for n in range(len(blocks)):
        lanes = slice(n * tokens, (n + 1) * tokens)
        key = key_t[:, lanes].T
        masked = [jnp.where(lane_head == h, key, jnp.zeros_like(key)) for h in range(half)]
        upper = jnp.concatenate([query_t[: features // 2, lanes], nothing], axis=1)
        lower = jnp.concatenate([nothing, query_t[features // 2 :, lanes]], axis=1)
        every = dot(jnp.concatenate(masked, axis=0), jnp.concatenate([upper, lower], axis=0))
        first, second = [], []
        for h in range(half):
            scores = every[h * tokens : (h + 1) * tokens] + bias[h]
            power = jnp.exp2(scores - jnp.max(scores, axis=0, keepdims=True)).astype(jnp.bfloat16)
            one, two = h * dim, (h + half) * dim
            rows = [value_t[one : one + dim, lanes], value_t[two : two + dim, lanes], ones]
            piece = dot(jnp.concatenate(rows, axis=0), power)
            share = 1.0 / piece[2 * dim : 2 * dim + 1]
            first.append((piece[:dim, :tokens] * share[:, :tokens]).astype(jnp.bfloat16))
            second.append((piece[dim : 2 * dim, tokens:] * share[:, tokens:]).astype(jnp.bfloat16))
            yield
        mixed.append(jnp.concatenate(first + second, axis=0))
    mixed_t = jnp.concatenate(mixed, axis=1)
    store.append((values + dot(proj_t[...], mixed_t)).astype(jnp.bfloat16))
    yield


def mlp_steps(store, middle, weights, tokens):
    up_t, down_t, gain = weights["up"], weights["down"], weights["gain_two"]
    features, hidden = middle.shape[0], up_t.shape[0]
    residual = middle.astype(jnp.float32)
    normed = normalise(residual, wide(gain[...], middle.shape[1]))
    yield
    total = None
    for part in range(hidden // features):
        rows = slice(part * features, (part + 1) * features)
        grown = dot(up_t[rows], normed).astype(jnp.bfloat16)
        yield
        grown = grown * (jnp.bfloat16(1.0) + lax.erf(grown))
        piece = dot(down_t[:, rows], grown)
        total = piece if total is None else total + piece
        yield
    result = (residual + total * ROOT_HALF).astype(jnp.bfloat16)
    for n in range(middle.shape[1] // tokens):
        store.append(result[:, n * tokens : (n + 1) * tokens].T)
    yield


def drain(*steps):
    for step in steps:
        for _ in step:
            pass


def attend(blocks, weights):
    store = []
    drain(attention_steps(store, blocks, weights))
    return store[0]


def expand(middle, weights, tokens):
    store = []
    drain(mlp_steps(store, middle, weights, tokens))
    return store


def both(blocks, middle, weights, tokens):
    new, finished = [], []
    drain(mlp_steps(finished, middle, weights, tokens), attention_steps(new, blocks, weights))
    return new[0], finished


def bias_strips(rel_bias, padded, strips, levels):
    heads, length = rel_bias.shape
    col_step = 2 * levels - 1
    row_step = (2 * WIN_LON - 1) * col_step
    offsets = [c * col_step + lev for c in range(WIN_LON) for lev in range(levels)]
    top = offsets[-1]
    width = padded.shape[1] - 128
    padded[...] = jnp.zeros_like(padded)
    padded[:, :length] = rel_bias[...] * LOG2E
    table = padded[...]
    left = jnp.concatenate([table[:, top - q : top - q + width] for q in offsets], axis=0)
    group = WIN_LON * levels
    lane = lax.broadcasted_iota(jnp.int32, (width, strips.shape[2]), 1)
    inner = lane % group
    target = lane // group * row_step + inner // levels * col_step + inner % levels
    pick = lax.broadcasted_iota(jnp.int32, target.shape, 0) == target
    found = jnp.dot(
        left,
        pick.astype(jnp.float32),
        precision=lax.Precision.HIGHEST,
        preferred_element_type=jnp.float32,
    )
    for place in range(group):
        strips[:, place, :] = found[place * heads : (place + 1) * heads]


def bias_table(strips, bias):
    heads, group, _ = strips.shape
    tokens = WIN_LAT * group
    for row in range(WIN_LAT):
        first = (WIN_LAT - 1 - row) * group
        piece = strips[:, :, first : first + tokens]
        places = slice(row * group, (row + 1) * group)
        bias[:, places, :tokens] = piece[: heads // 2]
        bias[:, places, tokens:] = piece[heads // 2 :]


class Sizes:
    def __init__(self, fields_shape):
        self.rows = fields_shape[0] // WIN_LAT
        self.cols = fields_shape[1] // WIN_LON
        self.count = self.rows * self.cols
        self.late = -(-((self.rows - 1) * self.cols // 2) // PAIR) * PAIR
        self.early = EARLY_PAIRS * PAIR
        self.leaving = min(LEAVING_PAIRS * PAIR, self.late)
        self.edge = self.rows + self.cols - 1

    def interior(self, window):
        return window // self.cols < self.rows - 1 and window % self.cols < self.cols - 1


def share_out(sizes, mask, device):
    def tally(d):
        inside, outside = jnp.int32(0), jnp.int32(0)
        for window in range(sizes.count):
            ocean = mask[window // sizes.cols, d * sizes.cols + window % sizes.cols]
            if sizes.interior(window):
                inside = inside + ocean
            else:
                outside = outside + ocean
        return inside, outside

    last = lax.axis_size("lon") - 1

    def pass_on(d, carried):
        inside, outside = tally(d)
        early = jnp.minimum(inside, sizes.early)
        excess = carried + inside + outside - early - sizes.late
        leaving = jnp.minimum(jnp.minimum(excess, inside - early), sizes.leaving)
        return jnp.where(d == last, 0, jnp.maximum(leaving, 0))

    coming = lax.fori_loop(0, device, pass_on, jnp.int32(0))
    leaving = pass_on(device, coming)
    inside, outside = tally(device)
    return coming, leaving, jnp.minimum(inside, sizes.early), inside, outside


def main_kernel(
    sizes,
    fields, mask, rel_bias, gain_one, w_qkv, w_proj, gain_two, w_up, w_down,
    finished, returned, ext, qkv_t, proj_t, up_t, down_t, gain_one_t, gain_two_t, bias,
    local, arrived, leave, middle, places, inner, outer, rel_local, padded, strips,
    gain_one_raw, gain_two_raw, qkv_raw, proj_raw, up_raw, down_raw,
    load_sems, halo_send, halo_recv, out_send, out_recv, back_send, back_recv,
):
    lat_cells, lon_cells, levels, features = fields.shape
    lat_half, lon_half = WIN_LAT // 2, WIN_LON // 2
    tokens = WIN_LAT * WIN_LON * levels
    lat, lon = lax.axis_index("lat"), lax.axis_index("lon")
    lat_size, lon_size = lax.axis_size("lat"), lax.axis_size("lon")
    last = lon_size - 1
    west, east = (lon + lon_size - 1) % lon_size, (lon + 1) % lon_size
    barrier = pltpu.get_barrier_semaphore()

    def greet(row, col):
        pl.semaphore_signal(barrier, inc=1, device_id=(row, col), device_id_type=MESH)

    greet(lat, east)
    greet(lat, west)

    @pl.when(lat < lat_size - 1)
    def _():
        greet(lat + 1, lon)
        greet(lat + 1, east)

    def load(which, source, target):
        copy = pltpu.make_async_copy(source, target, load_sems.at[which])
        copy.start()
        return copy

    here = load(0, fields, local)
    plan = load(1, mask, places)
    table = load(2, rel_bias, rel_local)
    inside = load(3, fields, ext.at[pl.ds(0, lat_cells), pl.ds(0, lon_cells)])
    raw = [gain_one_raw, gain_two_raw, qkv_raw, proj_raw, up_raw, down_raw]
    sources = [gain_one, gain_two, w_qkv, w_proj, w_up, w_down]
    weight_loads = [load(4 + n, source, target) for n, (source, target) in enumerate(zip(sources, raw))]

    def transfer(source, target, send, recv, row, col):
        return pltpu.make_async_remote_copy(
            src_ref=source, dst_ref=target, send_sem=send, recv_sem=recv,
            device_id=(row, col), device_id_type=MESH,
        )

    up = jnp.maximum(lat - 1, 0)
    below, beside = pl.ds(lat_cells, lat_half), pl.ds(lon_cells, lon_half)
    rows, cols = pl.ds(lat_half, lat_cells - lat_half), pl.ds(lon_half, lon_cells - lon_half)
    top, left = pl.ds(0, lat_half), pl.ds(0, lon_half)
    to_north = transfer(
        local.at[top, cols], ext.at[below, cols], halo_send.at[0], halo_recv.at[0], up, lon
    )
    to_west = transfer(
        local.at[rows, left], ext.at[rows, beside], halo_send.at[1], halo_recv.at[1], lat, west
    )
    to_corner = transfer(
        local.at[top, left], ext.at[below, beside], halo_send.at[2], halo_recv.at[2], up, west
    )

    plan.wait()
    coming, going, early, _, edges = share_out(sizes, places, lon)
    first_col = lon * sizes.cols
    for chain, inside_only in ((inner, True), (outer, False)):
        following = jnp.int32(sizes.count)
        chain[0, sizes.count] = following
        chain[0, sizes.count + 1] = following
        for window in reversed(range(sizes.count)):
            if sizes.interior(window) == inside_only:
                ocean = places[window // sizes.cols, first_col + window % sizes.cols]
                following = jnp.where(ocean == 1, window, following)
            chain[0, window] = following
        spot = following
        for n in range(sizes.count):
            chain[1, n] = jnp.where(spot == sizes.count, 0, spot)
            spot = chain[0, spot + 1]

    here.wait()

    @pl.when(lat > 0)
    def _():
        pl.semaphore_wait(barrier, 4)
        to_north.start()
        to_corner.start()

    @pl.when(lat == 0)
    def _():
        pl.semaphore_wait(barrier, 2)

    to_west.start()

    def fetch(source, window):
        row, col = window // sizes.cols, window % sizes.cols
        row_cells = pl.ds(row * WIN_LAT + lat_half, WIN_LAT)
        return source[row_cells, pl.ds(col * WIN_LON + lon_half, WIN_LON)]

    def outward(slot):
        return transfer(
            leave.at[slot], arrived.at[slot], out_send.at[slot], out_recv.at[slot],
            lat, jnp.minimum(lon + 1, last),
        )

    def homeward(pair):
        slots = pl.ds(pair * PAIR, PAIR)
        return transfer(
            finished.at[pl.ds(sizes.early + pair * PAIR, PAIR)], returned.at[slots],
            back_send.at[pair], back_recv.at[pair], lat, jnp.maximum(lon - 1, 0),
        )

    def pack(slot, carry):
        leave[slot] = fetch(local, inner[1, sizes.early + slot])

        @pl.when(lon < last)
        def _():
            outward(slot).start()

        return carry

    lax.fori_loop(0, sizes.leaving, pack, 0)

    table.wait()
    bias_strips(rel_local, padded, strips, levels)
    bias_table(strips, bias)
    for copy in weight_loads:
        copy.wait()
    gain_one_t[...] = jnp.broadcast_to(gain_one_raw[...], (128, features)).T
    gain_two_t[...] = jnp.broadcast_to(gain_two_raw[...] * ROOT_HALF, (128, features)).T
    for source, target in ((qkv_raw, qkv_t), (proj_raw, proj_t), (up_raw, up_t), (down_raw, down_t)):
        target[...] = source[...].T
    weights = dict(
        qkv=qkv_t, proj=proj_t, up=up_t, down=down_t,
        gain_one=gain_one_t, gain_two=gain_two_t, bias=bias,
    )
    early_pairs, late_pairs, leaving_pairs = (
        sizes.early // PAIR, sizes.late // PAIR, sizes.leaving // PAIR
    )

    def early_blocks(step):
        windows = [fetch(local, inner[1, step * PAIR + n]) for n in range(PAIR)]
        return [window.reshape(tokens, features) for window in windows]

    def late_blocks(pair):
        blocks = []
        for n in range(PAIR):
            slot = pair * PAIR + n
            rank = slot - coming
            edge = jnp.clip(rank, 0, sizes.count - 1)
            other = jnp.clip(early + going + rank - edges, 0, sizes.count - 1)
            mine = fetch(ext, jnp.where(rank < edges, outer[1, edge], inner[1, other]))
            sent = arrived[jnp.minimum(slot, sizes.leaving - 1)]
            block = jnp.where(rank >= 0, mine, sent)
            blocks.append(block.reshape(tokens, features))
        return blocks

    def keep(step, results):
        for n, result in enumerate(results):
            finished[step * PAIR + n] = result.reshape(finished.shape[1:])

    middle[0] = attend(early_blocks(0), weights)

    def early_step(step, carry):
        old = middle[(step + 1) % 2]
        new, results = both(early_blocks(step), old, weights, tokens)
        keep(step - 1, results)
        middle[step % 2] = new
        return carry

    lax.fori_loop(1, early_pairs, early_step, 0)
    inside.wait()
    to_west.wait_recv()

    @pl.when(lat < lat_size - 1)
    def _():
        to_north.wait_recv()
        to_corner.wait_recv()

    def send_home(pair):
        @pl.when((pair >= 0) & (pair < leaving_pairs) & (lon > 0))
        def _():
            homeward(pair).start()

    def late_step(pair, carry):
        @pl.when((pair < leaving_pairs) & (lon > 0))
        def _():
            for n in range(PAIR):
                outward(pair * PAIR + n).wait_recv()

        step = early_pairs + pair
        old = middle[(step + 1) % 2]
        new, results = both(late_blocks(pair), old, weights, tokens)
        keep(step - 1, results)
        middle[step % 2] = new
        send_home(pair - 1)
        return carry

    lax.fori_loop(0, late_pairs, late_step, 0)
    steps = early_pairs + late_pairs
    keep(steps - 1, expand(middle[(steps - 1) % 2], weights, tokens))
    if late_pairs <= leaving_pairs:
        send_home(jnp.int32(late_pairs - 1))

    to_west.wait_send()

    @pl.when(lat > 0)
    def _():
        to_north.wait_send()
        to_corner.wait_send()

    @pl.when(lon > 0)
    def _():
        for pair in range(leaving_pairs):
            homeward(pair).wait_send()

    @pl.when(lon < last)
    def _():
        for slot in range(sizes.leaving):
            outward(slot).wait_send()
        for pair in range(leaving_pairs):
            homeward(pair).wait_recv()


def place_kernel(
    sizes,
    mask, where, finished, returned, ext, qkv_t, proj_t, up_t, down_t, gain_one_t, gain_two_t, bias,
    result, zero, extra, sems,
):
    lat_half, lon_half = WIN_LAT // 2, WIN_LON // 2
    coming, going, early, _, edges = share_out(sizes, mask, where[0])
    first_col = where[0] * sizes.cols
    room = sizes.late - coming
    zero[...] = jnp.zeros_like(zero)

    def spot(window):
        row, col = window // sizes.cols, window % sizes.cols
        return result.at[pl.ds(row * WIN_LAT, WIN_LAT), pl.ds(col * WIN_LON, WIN_LON)]

    def send(source, window):
        pltpu.make_async_copy(source, spot(window), sems.at[window]).start()

    def visit(leftover, window, carry):
        inside_rank, edge_rank = carry
        row, col = window // sizes.cols, window % sizes.cols
        ocean = mask[row, first_col + col]
        edge = ((row == sizes.rows - 1) | (col == sizes.cols - 1)).astype(jnp.int32)
        rank = jnp.where(edge == 1, edge_rank, edges + inside_rank - early - going)
        is_early = (edge == 0) & (inside_rank < early)
        is_gone = (edge == 0) & (inside_rank >= early) & (inside_rank < early + going)
        rest = (ocean == 1) & jnp.logical_not(is_early | is_gone)
        if leftover:

            @pl.when(rest & (rank >= room))
            def _():
                row_cells = pl.ds(row * WIN_LAT + lat_half, WIN_LAT)
                block = ext[row_cells, pl.ds(col * WIN_LON + lon_half, WIN_LON)]
                weights = dict(
                    qkv=qkv_t, proj=proj_t, up=up_t, down=down_t,
                    gain_one=gain_one_t, gain_two=gain_two_t, bias=bias,
                )
                tokens = block.shape[0] * block.shape[1] * block.shape[2]
                middle = attend([block.reshape(tokens, block.shape[3])], weights)
                extra[...] = expand(middle, weights, tokens)[0].reshape(extra.shape)
                copy = pltpu.make_async_copy(extra, spot(window), sems.at[window])
                copy.start()
                copy.wait()

        else:

            @pl.when(ocean == 0)
            def _():
                send(zero, window)

            @pl.when((ocean == 1) & is_early)
            def _():
                send(finished.at[inside_rank], window)

            @pl.when((ocean == 1) & is_gone)
            def _():
                send(returned.at[inside_rank - early], window)

            @pl.when(rest & (rank < room))
            def _():
                send(finished.at[sizes.early + coming + rank], window)

        mine = ocean * (1 - edge)
        left = jnp.where(rest & (rank >= room), 1, 0)
        return inside_rank + mine, edge_rank + ocean * edge, left

    def start(window, carry):
        inside_rank, edge_rank, total, lost = carry
        inside_rank, edge_rank, left = visit(False, window, (inside_rank, edge_rank))
        return inside_rank, edge_rank, total + left, lost | (left << window)

    none = jnp.int32(0)
    _, _, total, lost = lax.fori_loop(0, sizes.count, start, (none, none, none, none))

    @pl.when(total > 0)
    def _():
        def again(window, carry):
            inside_rank, edge_rank, _ = visit(True, window, carry)
            return inside_rank, edge_rank

        lax.fori_loop(0, sizes.count, again, (none, none))

    def finish(window, carry):
        @pl.when((lost >> window) & 1 == 0)
        def _():
            pltpu.make_async_copy(zero, spot(window), sems.at[window]).wait()

        return carry

    lax.fori_loop(0, sizes.count, finish, 0)


def vmem():
    return pl.BlockSpec(memory_space=pltpu.VMEM)


def smem():
    return pl.BlockSpec(memory_space=pltpu.SMEM)


def any_space():
    return pl.BlockSpec(memory_space=pl.ANY)


def cost(flops, moved):
    return pl.CostEstimate(flops=flops, bytes_accessed=moved, transcendentals=0)


def body(fields, ocean_mask, gain_one, w_qkv, rel_bias, w_proj, gain_two, w_up, w_down):
    sizes = Sizes(fields.shape)
    lat_cells, lon_cells, levels, features = fields.shape
    heads, length = rel_bias.shape
    group = WIN_LON * levels
    tokens = WIN_LAT * group
    window = (WIN_LAT, WIN_LON, levels, features)
    bf16, f32 = jnp.bfloat16, jnp.float32
    shape = jax.ShapeDtypeStruct
    gains = [gain_one.reshape(1, -1), gain_two.reshape(1, -1)]
    sources = [w_qkv, w_proj, w_up, w_down]
    flips = [shape(w.shape[::-1], w.dtype) for w in sources]
    dma = pltpu.SemaphoreType.DMA
    pairs = sizes.leaving // PAIR
    results = pl.pallas_call(
        functools.partial(main_kernel, sizes),
        out_shape=[
            shape((sizes.early + sizes.late,) + window, bf16),
            shape((sizes.leaving,) + window, bf16),
            shape((lat_cells + WIN_LAT // 2, lon_cells + WIN_LON // 2, levels, features), bf16),
        ]
        + flips
        + [shape((features, 128), f32)] * 2
        + [shape((heads // 2, tokens, 2 * tokens), f32)],
        in_specs=[any_space()] * 9,
        out_specs=[vmem()] * 10,
        scratch_shapes=[
            pltpu.VMEM(fields.shape, bf16),
            pltpu.VMEM((sizes.leaving,) + window, bf16),
            pltpu.VMEM((sizes.leaving,) + window, bf16),
            pltpu.VMEM((2, features, PAIR * tokens), bf16),
            pltpu.SMEM(ocean_mask.shape, jnp.int32),
            pltpu.SMEM((2, sizes.count + 2), jnp.int32),
            pltpu.SMEM((2, sizes.count + 2), jnp.int32),
            pltpu.VMEM(rel_bias.shape, f32),
            pltpu.VMEM((heads, (length + 255) // 128 * 128), f32),
            pltpu.VMEM((heads, group, 2 * tokens), f32),
        ]
        + [pltpu.VMEM(gain.shape, f32) for gain in gains]
        + [pltpu.VMEM(w.shape, bf16) for w in sources]
        + [dma((10,)), dma((3,)), dma((3,)), dma((sizes.leaving,)), dma((sizes.leaving,))]
        + [dma((pairs,)), dma((pairs,))],
        cost_estimate=cost(0, fields.size),
        compiler_params=pltpu.CompilerParams(
            collective_id=0, has_side_effects=True, vmem_limit_bytes=40 * 2**20
        ),
    )(fields, ocean_mask, rel_bias, gains[0], w_qkv, w_proj, gains[1], w_up, w_down)
    where = jnp.reshape(lax.axis_index("lon"), (1,)).astype(jnp.int32)
    return pl.pallas_call(
        functools.partial(place_kernel, sizes),
        out_shape=shape(fields.shape, fields.dtype),
        in_specs=[smem()] * 2 + [vmem()] * 10,
        out_specs=any_space(),
        scratch_shapes=[
            pltpu.VMEM(window, bf16),
            pltpu.VMEM(window, bf16),
            dma((sizes.count,)),
        ],
        cost_estimate=cost(0, 4 * fields.size),
        compiler_params=pltpu.CompilerParams(vmem_limit_bytes=12 * 2**20),
    )(ocean_mask, where, *results)


def solution(mesh):
    in_specs = (P("lat", "lon", None, None), P("lat", None), P(), P(), P(), P(), P(), P(), P())
    out_specs = P("lat", "lon", None, None)
    return jax.shard_map(body, mesh=mesh, in_specs=in_specs, out_specs=out_specs, check_vma=False)
```

```python
import functools
import math

import jax
import jax.numpy as jnp
from jax import lax
from jax.experimental import pallas as pl
from jax.experimental.pallas import tpu as pltpu
from jax.sharding import PartitionSpec as P

WIN_LAT = 8
WIN_LON = 8
NORM_FLOOR = 0.25
MESH = pl.DeviceIdType.MESH
LOG2E = math.log2(math.e)
ROOT_HALF = math.sqrt(0.5)
PAIR = 2
EARLY_PAIRS = 2
LEAVING_PAIRS = 4


def dot(left, right):
    return jnp.dot(left, right, preferred_element_type=jnp.float32)


def normalise(values, gain):
    share = 1.0 / values.shape[0]
    average = jnp.sum(values, axis=0, keepdims=True) * share
    centred = values - average
    spread = jnp.sum(centred * centred, axis=0, keepdims=True) * share
    return (centred * lax.rsqrt(spread + NORM_FLOOR) * gain).astype(jnp.bfloat16)


def wide(gain, columns):
    return jnp.concatenate([gain] * (columns // gain.shape[1]), axis=1)


def attention_steps(store, blocks, weights):
    qkv_t, proj_t, gain, bias = weights["qkv"], weights["proj"], weights["gain_one"], weights["bias"]
    tokens, features = blocks[0].shape
    half = bias.shape[0]
    dim = features // (2 * half)
    scale = LOG2E / math.sqrt(dim)
    values = jnp.concatenate([block.T for block in blocks], axis=1).astype(jnp.float32)
    normed = normalise(values, wide(gain[...], values.shape[1]))
    yield
    key_t = dot(qkv_t[features : 2 * features], normed).astype(jnp.bfloat16)
    query_t = (dot(qkv_t[:features], normed) * scale).astype(jnp.bfloat16)
    value_t = dot(qkv_t[2 * features :], normed).astype(jnp.bfloat16)
    yield
    lane_head = lax.broadcasted_iota(jnp.int32, (tokens, features), 1) // dim % half
    nothing = jnp.zeros((features // 2, tokens), jnp.bfloat16)
    ones = jnp.ones((16, tokens), jnp.bfloat16)
    mixed = []
    for n in range(len(blocks)):
        lanes = slice(n * tokens, (n + 1) * tokens)
        key = key_t[:, lanes].T
        masked = [jnp.where(lane_head == h, key, jnp.zeros_like(key)) for h in range(half)]
        upper = jnp.concatenate([query_t[: features // 2, lanes], nothing], axis=1)
        lower = jnp.concatenate([nothing, query_t[features // 2 :, lanes]], axis=1)
        every = dot(jnp.concatenate(masked, axis=0), jnp.concatenate([upper, lower], axis=0))
        first, second = [], []
        for h in range(half):
            scores = every[h * tokens : (h + 1) * tokens] + bias[h]
            power = jnp.exp2(scores - jnp.max(scores, axis=0, keepdims=True)).astype(jnp.bfloat16)
            one, two = h * dim, (h + half) * dim
            rows = [value_t[one : one + dim, lanes], value_t[two : two + dim, lanes], ones]
            piece = dot(jnp.concatenate(rows, axis=0), power)
            share = 1.0 / piece[2 * dim : 2 * dim + 1]
            first.append((piece[:dim, :tokens] * share[:, :tokens]).astype(jnp.bfloat16))
            second.append((piece[dim : 2 * dim, tokens:] * share[:, tokens:]).astype(jnp.bfloat16))
            yield
        mixed.append(jnp.concatenate(first + second, axis=0))
    mixed_t = jnp.concatenate(mixed, axis=1)
    store.append((values + dot(proj_t[...], mixed_t)).astype(jnp.bfloat16))
    yield


def mlp_steps(store, middle, weights, tokens):
    up_t, down_t, gain = weights["up"], weights["down"], weights["gain_two"]
    features, hidden = middle.shape[0], up_t.shape[0]
    residual = middle.astype(jnp.float32)
    normed = normalise(residual, wide(gain[...], middle.shape[1]))
    yield
    total = None
    for part in range(hidden // features):
        rows = slice(part * features, (part + 1) * features)
        grown = dot(up_t[rows], normed).astype(jnp.bfloat16)
        yield
        grown = grown * (jnp.bfloat16(1.0) + lax.erf(grown))
        piece = dot(down_t[:, rows], grown)
        total = piece if total is None else total + piece
        yield
    result = (residual + total * ROOT_HALF).astype(jnp.bfloat16)
    for n in range(middle.shape[1] // tokens):
        store.append(result[:, n * tokens : (n + 1) * tokens].T)
    yield


def drain(*steps):
    for step in steps:
        for _ in step:
            pass


def attend(blocks, weights):
    store = []
    drain(attention_steps(store, blocks, weights))
    return store[0]


def expand(middle, weights, tokens):
    store = []
    drain(mlp_steps(store, middle, weights, tokens))
    return store


def both(blocks, middle, weights, tokens):
    new, finished = [], []
    drain(mlp_steps(finished, middle, weights, tokens), attention_steps(new, blocks, weights))
    return new[0], finished


def bias_strips(rel_bias, padded, strips, levels):
    heads, length = rel_bias.shape
    col_step = 2 * levels - 1
    row_step = (2 * WIN_LON - 1) * col_step
    offsets = [c * col_step + lev for c in range(WIN_LON) for lev in range(levels)]
    top = offsets[-1]
    width = padded.shape[1] - 128
    padded[...] = jnp.zeros_like(padded)
    padded[:, :length] = rel_bias[...] * LOG2E
    table = padded[...]
    left = jnp.concatenate([table[:, top - q : top - q + width] for q in offsets], axis=0)
    group = WIN_LON * levels
    lane = lax.broadcasted_iota(jnp.int32, (width, strips.shape[2]), 1)
    inner = lane % group
    target = lane // group * row_step + inner // levels * col_step + inner % levels
    pick = lax.broadcasted_iota(jnp.int32, target.shape, 0) == target
    found = jnp.dot(
        left,
        pick.astype(jnp.float32),
        precision=lax.Precision.HIGHEST,
        preferred_element_type=jnp.float32,
    )
    for place in range(group):
        strips[:, place, :] = found[place * heads : (place + 1) * heads]


def bias_table(strips, bias):
    heads, group, _ = strips.shape
    tokens = WIN_LAT * group
    for row in range(WIN_LAT):
        first = (WIN_LAT - 1 - row) * group
        piece = strips[:, :, first : first + tokens]
        places = slice(row * group, (row + 1) * group)
        bias[:, places, :tokens] = piece[: heads // 2]
        bias[:, places, tokens:] = piece[heads // 2 :]


class Sizes:
    def __init__(self, fields_shape):
        self.rows = fields_shape[0] // WIN_LAT
        self.cols = fields_shape[1] // WIN_LON
        self.count = self.rows * self.cols
        self.late = -(-((self.rows - 1) * self.cols // 2) // PAIR) * PAIR
        self.early = EARLY_PAIRS * PAIR
        self.leaving = min(LEAVING_PAIRS * PAIR, self.late)
        self.edge = self.rows + self.cols - 1

    def interior(self, window):
        return window // self.cols < self.rows - 1 and window % self.cols < self.cols - 1


def share_out(sizes, mask, device):
    def tally(d):
        inside, outside = jnp.int32(0), jnp.int32(0)
        for window in range(sizes.count):
            ocean = mask[window // sizes.cols, d * sizes.cols + window % sizes.cols]
            if sizes.interior(window):
                inside = inside + ocean
            else:
                outside = outside + ocean
        return inside, outside

    last = lax.axis_size("lon") - 1

    def pass_on(d, carried):
        inside, outside = tally(d)
        early = jnp.minimum(inside, sizes.early)
        excess = carried + inside + outside - early - sizes.late
        leaving = jnp.minimum(jnp.minimum(excess, inside - early), sizes.leaving)
        return jnp.where(d == last, 0, jnp.maximum(leaving, 0))

    coming = lax.fori_loop(0, device, pass_on, jnp.int32(0))
    leaving = pass_on(device, coming)
    inside, outside = tally(device)
    return coming, leaving, jnp.minimum(inside, sizes.early), inside, outside


HEAD = 4


def plan_kernel(sizes, mask, where, plan):
    device = where[0]
    coming, going, early, _, edges = share_out(sizes, mask, device)
    for n, value in enumerate((coming, going, early, edges)):
        plan[n] = value
    for n in range(HEAD, HEAD + 2 * sizes.count + 2):
        plan[n] = 0
    for base, inside_only in ((HEAD, True), (HEAD + sizes.count + 1, False)):
        spot = jnp.int32(base)
        for window in range(sizes.count):
            if sizes.interior(window) == inside_only:
                ocean = mask[window // sizes.cols, device * sizes.cols + window % sizes.cols]
                plan[spot] = window * ocean
                spot = spot + ocean


def main_kernel(
    sizes,
    plan, fields, rel_bias, gain_one, w_qkv, w_proj, gain_two, w_up, w_down,
    finished, returned, ext, qkv_t, proj_t, up_t, down_t, gain_one_t, gain_two_t, bias,
    arrived, leave, middle, padded, strips,
    halo_send, halo_recv, out_send, out_recv, back_send, back_recv,
):
    lat_cells, lon_cells, levels, features = fields.shape
    lat_half, lon_half = WIN_LAT // 2, WIN_LON // 2
    tokens = WIN_LAT * WIN_LON * levels
    lat, lon = lax.axis_index("lat"), lax.axis_index("lon")
    lat_size, lon_size = lax.axis_size("lat"), lax.axis_size("lon")
    last = lon_size - 1
    west, east = (lon + lon_size - 1) % lon_size, (lon + 1) % lon_size
    barrier = pltpu.get_barrier_semaphore()

    def greet(row, col):
        pl.semaphore_signal(barrier, inc=1, device_id=(row, col), device_id_type=MESH)

    greet(lat, east)
    greet(lat, west)

    @pl.when(lat < lat_size - 1)
    def _():
        greet(lat + 1, lon)
        greet(lat + 1, east)

    coming, going, early, edges = (plan[n] for n in range(HEAD))

    def inner(rank):
        return plan[HEAD + rank]

    def outer(rank):
        return plan[HEAD + sizes.count + 1 + rank]

    def transfer(source, target, send, recv, row, col):
        return pltpu.make_async_remote_copy(
            src_ref=source, dst_ref=target, send_sem=send, recv_sem=recv,
            device_id=(row, col), device_id_type=MESH,
        )

    up = jnp.maximum(lat - 1, 0)
    below, beside = pl.ds(lat_cells, lat_half), pl.ds(lon_cells, lon_half)
    rows, cols = pl.ds(lat_half, lat_cells - lat_half), pl.ds(lon_half, lon_cells - lon_half)
    top, left = pl.ds(0, lat_half), pl.ds(0, lon_half)
    to_north = transfer(
        fields.at[top, cols], ext.at[below, cols], halo_send.at[0], halo_recv.at[0], up, lon
    )
    to_west = transfer(
        fields.at[rows, left], ext.at[rows, beside], halo_send.at[1], halo_recv.at[1], lat, west
    )
    to_corner = transfer(
        fields.at[top, left], ext.at[below, beside], halo_send.at[2], halo_recv.at[2], up, west
    )

    @pl.when(lat > 0)
    def _():
        pl.semaphore_wait(barrier, 4)
        to_north.start()
        to_corner.start()

    @pl.when(lat == 0)
    def _():
        pl.semaphore_wait(barrier, 2)

    to_west.start()

    def fetch(source, window):
        row, col = window // sizes.cols, window % sizes.cols
        row_cells = pl.ds(row * WIN_LAT + lat_half, WIN_LAT)
        return source[row_cells, pl.ds(col * WIN_LON + lon_half, WIN_LON)]

    def outward(slot):
        return transfer(
            leave.at[slot], arrived.at[slot], out_send.at[slot], out_recv.at[slot],
            lat, jnp.minimum(lon + 1, last),
        )

    def homeward(pair):
        slots = pl.ds(pair * PAIR, PAIR)
        return transfer(
            finished.at[pl.ds(sizes.early + pair * PAIR, PAIR)], returned.at[slots],
            back_send.at[pair], back_recv.at[pair], lat, jnp.maximum(lon - 1, 0),
        )

    def pack(slot, carry):
        leave[slot] = fetch(fields, inner(sizes.early + slot))

        @pl.when(lon < last)
        def _():
            outward(slot).start()

        return carry

    lax.fori_loop(0, sizes.leaving, pack, 0)
    for row in range(lat_half, lat_cells, WIN_LAT):
        cells = pl.ds(row, min(WIN_LAT, lat_cells - row))
        ext[cells, pl.ds(lon_half, lon_cells - lon_half)] = fields[
            cells, pl.ds(lon_half, lon_cells - lon_half)
        ]

    bias_strips(rel_bias, padded, strips, levels)
    bias_table(strips, bias)
    gain_one_t[...] = jnp.broadcast_to(gain_one[...], (128, features)).T
    gain_two_t[...] = jnp.broadcast_to(gain_two[...] * ROOT_HALF, (128, features)).T
    for source, target in ((w_qkv, qkv_t), (w_proj, proj_t), (w_up, up_t), (w_down, down_t)):
        target[...] = source[...].T
    weights = dict(
        qkv=qkv_t, proj=proj_t, up=up_t, down=down_t,
        gain_one=gain_one_t, gain_two=gain_two_t, bias=bias,
    )
    early_pairs, late_pairs, leaving_pairs = (
        sizes.early // PAIR, sizes.late // PAIR, sizes.leaving // PAIR
    )

    def early_blocks(step):
        windows = [fetch(fields, inner(step * PAIR + n)) for n in range(PAIR)]
        return [window.reshape(tokens, features) for window in windows]

    def late_blocks(pair):
        blocks = []
        for n in range(PAIR):
            slot = pair * PAIR + n
            rank = slot - coming
            edge = jnp.clip(rank, 0, sizes.count - 1)
            other = jnp.clip(early + going + rank - edges, 0, sizes.count - 1)
            mine = fetch(ext, jnp.where(rank < edges, outer(edge), inner(other)))
            sent = arrived[jnp.minimum(slot, sizes.leaving - 1)]
            block = jnp.where(rank >= 0, mine, sent)
            blocks.append(block.reshape(tokens, features))
        return blocks

    def keep(step, results):
        for n, result in enumerate(results):
            finished[step * PAIR + n] = result.reshape(finished.shape[1:])

    middle[0] = attend(early_blocks(0), weights)

    def early_step(step, carry):
        old = middle[(step + 1) % 2]
        new, results = both(early_blocks(step), old, weights, tokens)
        keep(step - 1, results)
        middle[step % 2] = new
        return carry

    lax.fori_loop(1, early_pairs, early_step, 0)
    to_west.wait_recv()

    @pl.when(lat < lat_size - 1)
    def _():
        to_north.wait_recv()
        to_corner.wait_recv()

    def send_home(pair):
        @pl.when((pair >= 0) & (pair < leaving_pairs) & (lon > 0))
        def _():
            homeward(pair).start()

    def late_step(pair, carry):
        @pl.when((pair < leaving_pairs) & (lon > 0))
        def _():
            for n in range(PAIR):
                outward(pair * PAIR + n).wait_recv()

        step = early_pairs + pair
        old = middle[(step + 1) % 2]
        new, results = both(late_blocks(pair), old, weights, tokens)
        keep(step - 1, results)
        middle[step % 2] = new
        send_home(pair - 1)
        return carry

    lax.fori_loop(0, late_pairs, late_step, 0)
    steps = early_pairs + late_pairs
    keep(steps - 1, expand(middle[(steps - 1) % 2], weights, tokens))
    if late_pairs <= leaving_pairs:
        send_home(jnp.int32(late_pairs - 1))

    to_west.wait_send()

    @pl.when(lat > 0)
    def _():
        to_north.wait_send()
        to_corner.wait_send()

    @pl.when(lon > 0)
    def _():
        for pair in range(leaving_pairs):
            homeward(pair).wait_send()

    @pl.when(lon < last)
    def _():
        for slot in range(sizes.leaving):
            outward(slot).wait_send()
        for pair in range(leaving_pairs):
            homeward(pair).wait_recv()


def place_kernel(
    sizes,
    mask, where, plan, finished, returned, ext, qkv_t, proj_t, up_t, down_t, gain_one_t, gain_two_t, bias,
    result, zero, extra, sems,
):
    lat_half, lon_half = WIN_LAT // 2, WIN_LON // 2
    coming, going, early, edges = (plan[n] for n in range(HEAD))
    first_col = where[0] * sizes.cols
    room = sizes.late - coming
    zero[...] = jnp.zeros_like(zero)

    def spot(window):
        row, col = window // sizes.cols, window % sizes.cols
        return result.at[pl.ds(row * WIN_LAT, WIN_LAT), pl.ds(col * WIN_LON, WIN_LON)]

    def send(source, window):
        pltpu.make_async_copy(source, spot(window), sems.at[window]).start()

    def visit(leftover, window, carry):
        inside_rank, edge_rank = carry
        row, col = window // sizes.cols, window % sizes.cols
        ocean = mask[row, first_col + col]
        edge = ((row == sizes.rows - 1) | (col == sizes.cols - 1)).astype(jnp.int32)
        rank = jnp.where(edge == 1, edge_rank, edges + inside_rank - early - going)
        is_early = (edge == 0) & (inside_rank < early)
        is_gone = (edge == 0) & (inside_rank >= early) & (inside_rank < early + going)
        rest = (ocean == 1) & jnp.logical_not(is_early | is_gone)
        if leftover:

            @pl.when(rest & (rank >= room))
            def _():
                row_cells = pl.ds(row * WIN_LAT + lat_half, WIN_LAT)
                block = ext[row_cells, pl.ds(col * WIN_LON + lon_half, WIN_LON)]
                weights = dict(
                    qkv=qkv_t, proj=proj_t, up=up_t, down=down_t,
                    gain_one=gain_one_t, gain_two=gain_two_t, bias=bias,
                )
                tokens = block.shape[0] * block.shape[1] * block.shape[2]
                middle = attend([block.reshape(tokens, block.shape[3])], weights)
                extra[...] = expand(middle, weights, tokens)[0].reshape(extra.shape)
                copy = pltpu.make_async_copy(extra, spot(window), sems.at[window])
                copy.start()
                copy.wait()

        else:

            @pl.when(ocean == 0)
            def _():
                send(zero, window)

            @pl.when((ocean == 1) & is_early)
            def _():
                send(finished.at[inside_rank], window)

            @pl.when((ocean == 1) & is_gone)
            def _():
                send(returned.at[inside_rank - early], window)

            @pl.when(rest & (rank < room))
            def _():
                send(finished.at[sizes.early + coming + rank], window)

        mine = ocean * (1 - edge)
        left = jnp.where(rest & (rank >= room), 1, 0)
        return inside_rank + mine, edge_rank + ocean * edge, left

    def start(window, carry):
        inside_rank, edge_rank, total, lost = carry
        inside_rank, edge_rank, left = visit(False, window, (inside_rank, edge_rank))
        return inside_rank, edge_rank, total + left, lost | (left << window)

    none = jnp.int32(0)
    _, _, total, lost = lax.fori_loop(0, sizes.count, start, (none, none, none, none))

    @pl.when(total > 0)
    def _():
        def again(window, carry):
            inside_rank, edge_rank, _ = visit(True, window, carry)
            return inside_rank, edge_rank

        lax.fori_loop(0, sizes.count, again, (none, none))

    def finish(window, carry):
        @pl.when((lost >> window) & 1 == 0)
        def _():
            pltpu.make_async_copy(zero, spot(window), sems.at[window]).wait()

        return carry

    lax.fori_loop(0, sizes.count, finish, 0)


def vmem():
    return pl.BlockSpec(memory_space=pltpu.VMEM)


def smem():
    return pl.BlockSpec(memory_space=pltpu.SMEM)


def any_space():
    return pl.BlockSpec(memory_space=pl.ANY)


def cost(flops, moved):
    return pl.CostEstimate(flops=flops, bytes_accessed=moved, transcendentals=0)


def body(fields, ocean_mask, gain_one, w_qkv, rel_bias, w_proj, gain_two, w_up, w_down):
    sizes = Sizes(fields.shape)
    lat_cells, lon_cells, levels, features = fields.shape
    heads, length = rel_bias.shape
    group = WIN_LON * levels
    tokens = WIN_LAT * group
    window = (WIN_LAT, WIN_LON, levels, features)
    bf16, f32 = jnp.bfloat16, jnp.float32
    shape = jax.ShapeDtypeStruct
    gains = [gain_one.reshape(1, -1), gain_two.reshape(1, -1)]
    sources = [w_qkv, w_proj, w_up, w_down]
    flips = [shape(w.shape[::-1], w.dtype) for w in sources]
    dma = pltpu.SemaphoreType.DMA
    pairs = sizes.leaving // PAIR
    where = jnp.reshape(lax.axis_index("lon"), (1,)).astype(jnp.int32)
    plan = pl.pallas_call(
        functools.partial(plan_kernel, sizes),
        out_shape=shape((HEAD + 2 * sizes.count + 2,), jnp.int32),
        in_specs=[smem()] * 2,
        out_specs=smem(),
        cost_estimate=cost(2**36, 2**26),
        compiler_params=pltpu.CompilerParams(vmem_limit_bytes=2**20),
    )(ocean_mask, where)
    results = pl.pallas_call(
        functools.partial(main_kernel, sizes),
        out_shape=[
            shape((sizes.early + sizes.late,) + window, bf16),
            shape((sizes.leaving,) + window, bf16),
            shape((lat_cells + WIN_LAT // 2, lon_cells + WIN_LON // 2, levels, features), bf16),
        ]
        + flips
        + [shape((features, 128), f32)] * 2
        + [shape((heads // 2, tokens, 2 * tokens), f32)],
        in_specs=[smem()] + [vmem()] * 8,
        out_specs=[vmem()] * 10,
        scratch_shapes=[
            pltpu.VMEM((sizes.leaving,) + window, bf16),
            pltpu.VMEM((sizes.leaving,) + window, bf16),
            pltpu.VMEM((2, features, PAIR * tokens), bf16),
            pltpu.VMEM((heads, (length + 255) // 128 * 128), f32),
            pltpu.VMEM((heads, group, 2 * tokens), f32),
        ]
        + [dma((3,)), dma((3,)), dma((sizes.leaving,)), dma((sizes.leaving,))]
        + [dma((pairs,)), dma((pairs,))],
        cost_estimate=cost(0, fields.size),
        compiler_params=pltpu.CompilerParams(
            collective_id=0, has_side_effects=True, vmem_limit_bytes=24 * 2**20
        ),
    )(plan, fields, rel_bias, gains[0], w_qkv, w_proj, gains[1], w_up, w_down)
    return pl.pallas_call(
        functools.partial(place_kernel, sizes),
        out_shape=shape(fields.shape, fields.dtype),
        in_specs=[smem()] * 3 + [vmem()] * 10,
        out_specs=any_space(),
        scratch_shapes=[
            pltpu.VMEM(window, bf16),
            pltpu.VMEM(window, bf16),
            dma((sizes.count,)),
        ],
        cost_estimate=cost(0, 4 * fields.size),
        compiler_params=pltpu.CompilerParams(vmem_limit_bytes=12 * 2**20),
    )(ocean_mask, where, plan, *results)


def solution(mesh):
    in_specs = (P("lat", "lon", None, None), P("lat", None), P(), P(), P(), P(), P(), P(), P())
    out_specs = P("lat", "lon", None, None)
    return jax.shard_map(body, mesh=mesh, in_specs=in_specs, out_specs=out_specs, check_vma=False)
```

```python
import functools
import math

import jax
import jax.numpy as jnp
from jax import lax
from jax.experimental import pallas as pl
from jax.experimental.pallas import tpu as pltpu
from jax.sharding import PartitionSpec as P

WIN_LAT = 8
WIN_LON = 8
NORM_FLOOR = 0.25
MESH = pl.DeviceIdType.MESH
LOG2E = math.log2(math.e)
ROOT_HALF = math.sqrt(0.5)
PAIR = 2
EARLY_PAIRS = 2
LEAVING_PAIRS = 3


def dot(left, right):
    return jnp.dot(left, right, preferred_element_type=jnp.float32)


def normalise(values, gain):
    share = 1.0 / values.shape[0]
    average = jnp.sum(values, axis=0, keepdims=True) * share
    centred = values - average
    spread = jnp.sum(centred * centred, axis=0, keepdims=True) * share
    return (centred * lax.rsqrt(spread + NORM_FLOOR) * gain).astype(jnp.bfloat16)


def wide(gain, columns):
    return jnp.concatenate([gain] * (columns // gain.shape[1]), axis=1)


def flip_steps(store, blocks, weights):
    flipped = jnp.concatenate([block.T for block in blocks], axis=1)
    gain = wide(weights["gain_one"][...], flipped.shape[1])
    store.extend([flipped, normalise(flipped.astype(jnp.float32), gain)])
    yield


def attention_steps(store, flipped, normed, weights):
    qkv_t, proj_t, bias = weights["qkv"], weights["proj"], weights["bias"]
    features, columns = normed.shape
    half, tokens, _ = bias.shape
    dim = features // (2 * half)
    scale = LOG2E / math.sqrt(dim)
    key_t = dot(qkv_t[features : 2 * features], normed).astype(jnp.bfloat16)
    yield
    query_t = (dot(qkv_t[:features], normed) * scale).astype(jnp.bfloat16)
    yield
    value_t = dot(qkv_t[2 * features :], normed).astype(jnp.bfloat16)
    yield
    lane_head = lax.broadcasted_iota(jnp.int32, (tokens, features), 1) // dim % half
    nothing = jnp.zeros((features // 2, tokens), jnp.bfloat16)
    ones = jnp.ones((16, tokens), jnp.bfloat16)
    spans = [slice(n, n + tokens) for n in range(0, columns, tokens)]
    every = []
    for lanes in spans:
        key = key_t[:, lanes].T
        masked = [jnp.where(lane_head == h, key, jnp.zeros_like(key)) for h in range(half)]
        upper = jnp.concatenate([query_t[: features // 2, lanes], nothing], axis=1)
        lower = jnp.concatenate([nothing, query_t[features // 2 :, lanes]], axis=1)
        every.append(dot(jnp.concatenate(masked, axis=0), jnp.concatenate([upper, lower], axis=0)))
        yield
    mixed = []
    for lanes, products in zip(spans, every):
        first, second = [], []
        for h in range(half):
            scores = products[h * tokens : (h + 1) * tokens] + bias[h]
            power = jnp.exp2(scores - jnp.max(scores, axis=0, keepdims=True)).astype(jnp.bfloat16)
            one, two = h * dim, (h + half) * dim
            rows = [value_t[one : one + dim, lanes], value_t[two : two + dim, lanes], ones]
            piece = dot(jnp.concatenate(rows, axis=0), power)
            share = 1.0 / piece[2 * dim : 2 * dim + 1]
            first.append((piece[:dim, :tokens] * share[:, :tokens]).astype(jnp.bfloat16))
            second.append((piece[dim : 2 * dim, tokens:] * share[:, tokens:]).astype(jnp.bfloat16))
            yield
        mixed.append(jnp.concatenate(first + second, axis=0))
    projected = dot(proj_t[...], jnp.concatenate(mixed, axis=1))
    store.append((flipped.astype(jnp.float32) + projected).astype(jnp.bfloat16))
    yield


def mlp_steps(store, middle, weights, tokens):
    up_t, down_t, gain = weights["up"], weights["down"], weights["gain_two"]
    features, hidden = middle.shape[0], up_t.shape[0]
    residual = middle.astype(jnp.float32)
    normed = normalise(residual, wide(gain[...], middle.shape[1]))
    yield
    total = None
    for part in range(hidden // features):
        rows = slice(part * features, (part + 1) * features)
        grown = dot(up_t[rows], normed)
        yield
        grown = (grown * (1.0 + lax.erf(grown))).astype(jnp.bfloat16)
        piece = dot(down_t[:, rows], grown)
        total = piece if total is None else total + piece
        yield
    result = (residual + total * ROOT_HALF).astype(jnp.bfloat16)
    for n in range(middle.shape[1] // tokens):
        store.append(result[:, n * tokens : (n + 1) * tokens].T)
    yield


def weave(*steps):
    steps = list(steps)
    while steps:
        for chain in list(steps):
            try:
                next(chain)
            except StopIteration:
                steps.remove(chain)


def bias_strips(rel_bias, padded, strips, levels):
    heads, length = rel_bias.shape
    col_step = 2 * levels - 1
    row_step = (2 * WIN_LON - 1) * col_step
    offsets = [c * col_step + lev for c in range(WIN_LON) for lev in range(levels)]
    top = offsets[-1]
    width = padded.shape[1] - 128
    padded[...] = jnp.zeros_like(padded)
    padded[:, :length] = rel_bias[...] * LOG2E
    table = padded[...]
    left = jnp.concatenate([table[:, top - q : top - q + width] for q in offsets], axis=0)
    group = WIN_LON * levels
    lane = lax.broadcasted_iota(jnp.int32, (width, strips.shape[2]), 1)
    inner = lane % group
    target = lane // group * row_step + inner // levels * col_step + inner % levels
    pick = lax.broadcasted_iota(jnp.int32, target.shape, 0) == target
    found = jnp.dot(
        left,
        pick.astype(jnp.float32),
        precision=lax.Precision.HIGHEST,
        preferred_element_type=jnp.float32,
    )
    for place in range(group):
        strips[:, place, :] = found[place * heads : (place + 1) * heads]


def bias_table(strips, bias):
    heads, group, _ = strips.shape
    tokens = WIN_LAT * group
    for row in range(WIN_LAT):
        first = (WIN_LAT - 1 - row) * group
        piece = strips[:, :, first : first + tokens]
        places = slice(row * group, (row + 1) * group)
        bias[:, places, :tokens] = piece[: heads // 2]
        bias[:, places, tokens:] = piece[heads // 2 :]


class Sizes:
    def __init__(self, fields_shape):
        self.rows = fields_shape[0] // WIN_LAT
        self.cols = fields_shape[1] // WIN_LON
        self.count = self.rows * self.cols
        self.late = -(-((self.rows - 1) * self.cols // 2) // PAIR) * PAIR
        self.early = EARLY_PAIRS * PAIR
        self.leaving = min(LEAVING_PAIRS * PAIR, self.late)
        self.edge = self.rows + self.cols - 1

    def interior(self, window):
        return window // self.cols < self.rows - 1 and window % self.cols < self.cols - 1


def share_out(sizes, mask, device):
    def tally(d):
        inside, outside = jnp.int32(0), jnp.int32(0)
        for window in range(sizes.count):
            ocean = mask[window // sizes.cols, d * sizes.cols + window % sizes.cols]
            if sizes.interior(window):
                inside = inside + ocean
            else:
                outside = outside + ocean
        return inside, outside

    last = lax.axis_size("lon") - 1

    def pass_on(d, carried):
        inside, outside = tally(d)
        early = jnp.minimum(inside, sizes.early)
        excess = carried + inside + outside - early - sizes.late
        leaving = jnp.minimum(jnp.minimum(excess, inside - early), sizes.leaving)
        return jnp.where(d == last, 0, jnp.maximum(leaving, 0))

    coming = lax.fori_loop(0, device, pass_on, jnp.int32(0))
    leaving = pass_on(device, coming)
    inside, outside = tally(device)
    return coming, leaving, jnp.minimum(inside, sizes.early), inside, outside


def first_kernel(token):
    token[...] = jnp.zeros_like(token)


def main_kernel(
    sizes,
    mask, token, fields, rel_bias, gain_one, w_qkv, w_proj, gain_two, w_up, w_down,
    results, codes, ext, qkv_t, proj_t, up_t, down_t, gain_one_t, gain_two_t, bias,
    arrived, leave, flipped, normed, middle, inner, outer, padded, strips,
    halo_send, halo_recv, out_send, out_recv, back_send, back_recv,
):
    lat_cells, lon_cells, levels, features = fields.shape
    lat_half, lon_half = WIN_LAT // 2, WIN_LON // 2
    tokens = WIN_LAT * WIN_LON * levels
    lat, lon = lax.axis_index("lat"), lax.axis_index("lon")
    lat_size, lon_size = lax.axis_size("lat"), lax.axis_size("lon")
    last = lon_size - 1
    west, east = (lon + lon_size - 1) % lon_size, (lon + 1) % lon_size
    barrier = pltpu.get_barrier_semaphore()

    def greet(row, col):
        pl.semaphore_signal(barrier, inc=1, device_id=(row, col), device_id_type=MESH)

    greet(lat, east)
    greet(lat, west)

    @pl.when(lat < lat_size - 1)
    def _():
        greet(lat + 1, lon)
        greet(lat + 1, east)

    def transfer(source, target, send, recv, row, col):
        return pltpu.make_async_remote_copy(
            src_ref=source, dst_ref=target, send_sem=send, recv_sem=recv,
            device_id=(row, col), device_id_type=MESH,
        )

    up = jnp.maximum(lat - 1, 0)
    below, beside = pl.ds(lat_cells, lat_half), pl.ds(lon_cells, lon_half)
    rows, cols = pl.ds(lat_half, lat_cells - lat_half), pl.ds(lon_half, lon_cells - lon_half)
    top, left = pl.ds(0, lat_half), pl.ds(0, lon_half)
    to_north = transfer(
        fields.at[top, cols], ext.at[below, cols], halo_send.at[0], halo_recv.at[0], up, lon
    )
    to_west = transfer(
        fields.at[rows, left], ext.at[rows, beside], halo_send.at[1], halo_recv.at[1], lat, west
    )
    to_corner = transfer(
        fields.at[top, left], ext.at[below, beside], halo_send.at[2], halo_recv.at[2], up, west
    )

    @pl.when(lat > 0)
    def _():
        pl.semaphore_wait(barrier, 4)
        to_north.start()
        to_corner.start()

    @pl.when(lat == 0)
    def _():
        pl.semaphore_wait(barrier, 2)

    to_west.start()
    coming, going, early, _, edges = share_out(sizes, mask, lon)
    first_col = lon * sizes.cols
    for chain, inside_only in ((inner, True), (outer, False)):
        following = jnp.int32(sizes.count)
        chain[0, sizes.count] = following
        chain[0, sizes.count + 1] = following
        for window in reversed(range(sizes.count)):
            if sizes.interior(window) == inside_only:
                ocean = mask[window // sizes.cols, first_col + window % sizes.cols]
                following = jnp.where(ocean == 1, window, following)
            chain[0, window] = following
        spot = following
        for n in range(sizes.count):
            chain[1, n] = jnp.where(spot == sizes.count, 0, spot)
            spot = chain[0, spot + 1]

    def fetch(source, window):
        row, col = window // sizes.cols, window % sizes.cols
        row_cells = pl.ds(row * WIN_LAT + lat_half, WIN_LAT)
        return source[row_cells, pl.ds(col * WIN_LON + lon_half, WIN_LON)]

    def outward(slot):
        return transfer(
            leave.at[slot], arrived.at[slot], out_send.at[slot], out_recv.at[slot],
            lat, jnp.minimum(lon + 1, last),
        )

    def homeward(pair):
        slots = pl.ds(sizes.early + sizes.late + pair * PAIR, PAIR)
        return transfer(
            results.at[pl.ds(sizes.early + pair * PAIR, PAIR)], results.at[slots],
            back_send.at[pair], back_recv.at[pair], lat, jnp.maximum(lon - 1, 0),
        )

    def pack(slot, carry):
        leave[slot] = fetch(fields, inner[1, sizes.early + slot])

        @pl.when(lon < last)
        def _():
            outward(slot).start()

        return carry

    lax.fori_loop(0, sizes.leaving, pack, 0)
    bias_strips(rel_bias, padded, strips, levels)
    bias_table(strips, bias)
    gain_one_t[...] = jnp.broadcast_to(gain_one[...], (128, features)).T
    gain_two_t[...] = jnp.broadcast_to(gain_two[...] * ROOT_HALF, (128, features)).T
    for source, target in ((w_qkv, qkv_t), (w_proj, proj_t), (w_up, up_t), (w_down, down_t)):
        target[...] = source[...].T
    weights = dict(
        qkv=qkv_t, proj=proj_t, up=up_t, down=down_t,
        gain_one=gain_one_t, gain_two=gain_two_t, bias=bias,
    )
    early_pairs, late_pairs, leaving_pairs = (
        sizes.early // PAIR, sizes.late // PAIR, sizes.leaving // PAIR
    )

    def early_blocks(step):
        windows = [fetch(fields, inner[1, step * PAIR + n]) for n in range(PAIR)]
        return [window.reshape(tokens, features) for window in windows]

    def late_blocks(pair):
        blocks = []
        for n in range(PAIR):
            slot = pair * PAIR + n
            rank = slot - coming
            edge = jnp.clip(rank, 0, sizes.count - 1)
            other = jnp.clip(early + going + rank - edges, 0, sizes.count - 1)
            mine = fetch(ext, jnp.where(rank < edges, outer[1, edge], inner[1, other]))
            sent = arrived[jnp.minimum(slot, sizes.leaving - 1)]
            block = jnp.where(rank >= 0, mine, sent)
            blocks.append(block.reshape(tokens, features))
        return blocks

    def put(step, flip):
        flipped[step % 2], normed[step % 2] = flip

    def keep(step, windows):
        for n, window in enumerate(windows):
            results[step * PAIR + n] = window.reshape(results.shape[1:])

    def advance(step, before=True, blocks=None):
        new, windows, flip = [], [], []
        chains = [attention_steps(new, flipped[step % 2], normed[step % 2], weights)]
        if before:
            chains.insert(0, mlp_steps(windows, middle[(step + 1) % 2], weights, tokens))
        weave(*chains)
        if blocks is not None:
            weave(flip_steps(flip, blocks, weights))
            put(step + 1, flip)
        if before:
            keep(step - 1, windows)
        middle[step % 2] = new[0]

    def prepare(step, blocks):
        flip = []
        weave(flip_steps(flip, blocks, weights))
        put(step, flip)

    prepare(0, early_blocks(0))
    advance(0, before=False, blocks=early_blocks(1) if early_pairs > 1 else None)

    def early_step(step, carry):
        advance(step, blocks=early_blocks(step + 1))
        return carry

    lax.fori_loop(1, early_pairs - 1, early_step, 0)
    if early_pairs > 1:
        advance(early_pairs - 1)
    inside_rows, inside_cols = pl.ds(lat_half, lat_cells - lat_half), pl.ds(lon_half, lon_cells - lon_half)
    ext[inside_rows, inside_cols] = fields[inside_rows, inside_cols]
    to_west.wait_recv()

    @pl.when(lat < lat_size - 1)
    def _():
        to_north.wait_recv()
        to_corner.wait_recv()

    def receive(pair):
        @pl.when((pair < leaving_pairs) & (lon > 0))
        def _():
            for n in range(PAIR):
                outward(pair * PAIR + n).wait_recv()

    def send_home(pair):
        @pl.when((pair >= 0) & (pair < leaving_pairs) & (lon > 0))
        def _():
            homeward(pair).start()

    receive(jnp.int32(0))
    prepare(early_pairs, late_blocks(0))

    def late_step(pair, carry):
        receive(pair + 1)
        advance(early_pairs + pair, blocks=late_blocks(jnp.minimum(pair + 1, late_pairs - 1)))
        send_home(pair - 1)
        return carry

    lax.fori_loop(0, late_pairs, late_step, 0)
    steps = early_pairs + late_pairs
    windows = []
    weave(mlp_steps(windows, middle[(steps - 1) % 2], weights, tokens))
    keep(steps - 1, windows)
    if late_pairs <= leaving_pairs:
        send_home(jnp.int32(late_pairs - 1))

    room = sizes.late - coming
    back = sizes.early + sizes.late
    results[back + sizes.leaving] = jnp.zeros(results.shape[1:], results.dtype)
    inside_rank, edge_rank = jnp.int32(0), jnp.int32(0)
    for window in range(sizes.count):
        ocean = mask[window // sizes.cols, first_col + window % sizes.cols]
        if sizes.interior(window):
            rank = edges + inside_rank - early - going
        else:
            rank = edge_rank
        code = jnp.where(rank < room, sizes.early + coming + rank, -1)
        if sizes.interior(window):
            code = jnp.where(inside_rank < early + going, back + inside_rank - early, code)
            code = jnp.where(inside_rank < early, inside_rank, code)
            inside_rank = inside_rank + ocean
        else:
            edge_rank = edge_rank + ocean
        codes[window] = jnp.where(ocean == 1, code, back + sizes.leaving)

    to_west.wait_send()

    @pl.when(lat > 0)
    def _():
        to_north.wait_send()
        to_corner.wait_send()

    @pl.when(lon > 0)
    def _():
        for pair in range(leaving_pairs):
            homeward(pair).wait_send()

    @pl.when(lon < last)
    def _():
        for slot in range(sizes.leaving):
            outward(slot).wait_send()
        for pair in range(leaving_pairs):
            homeward(pair).wait_recv()


def place_kernel(
    sizes,
    codes, results, ext, qkv_t, proj_t, up_t, down_t, gain_one_t, gain_two_t, bias,
    output, extra, sems,
):
    lat_half, lon_half = WIN_LAT // 2, WIN_LON // 2
    nothing = results.shape[0] - 1

    def spot(window):
        row, col = window // sizes.cols, window % sizes.cols
        return output.at[pl.ds(row * WIN_LAT, WIN_LAT), pl.ds(col * WIN_LON, WIN_LON)]

    lost = jnp.int32(0)
    for window in range(sizes.count):
        code = codes[window]
        lost = jnp.minimum(lost, code)
        source = results.at[jnp.where(code < 0, nothing, code)]
        pltpu.make_async_copy(source, spot(window), sems.at[window]).start()
    for window in range(sizes.count):
        pltpu.make_async_copy(results.at[nothing], spot(window), sems.at[window]).wait()

    @pl.when(lost < 0)
    def _():
        def again(window, carry):
            @pl.when(codes[window] < 0)
            def _():
                row, col = window // sizes.cols, window % sizes.cols
                row_cells = pl.ds(row * WIN_LAT + lat_half, WIN_LAT)
                block = ext[row_cells, pl.ds(col * WIN_LON + lon_half, WIN_LON)]
                weights = dict(
                    qkv=qkv_t, proj=proj_t, up=up_t, down=down_t,
                    gain_one=gain_one_t, gain_two=gain_two_t, bias=bias,
                )
                tokens = block.shape[0] * block.shape[1] * block.shape[2]
                flip, middle, windows = [], [], []
                weave(flip_steps(flip, [block.reshape(tokens, block.shape[3])], weights))
                weave(attention_steps(middle, flip[0], flip[1], weights))
                weave(mlp_steps(windows, middle[0], weights, tokens))
                extra[...] = windows[0].reshape(extra.shape)
                copy = pltpu.make_async_copy(extra, spot(window), sems.at[window])
                copy.start()
                copy.wait()

            return carry

        lax.fori_loop(0, sizes.count, again, 0)


def vmem():
    return pl.BlockSpec(memory_space=pltpu.VMEM)


def smem():
    return pl.BlockSpec(memory_space=pltpu.SMEM)


def any_space():
    return pl.BlockSpec(memory_space=pl.ANY)


def cost(flops, moved):
    return pl.CostEstimate(flops=flops, bytes_accessed=moved, transcendentals=0)


def body(fields, ocean_mask, gain_one, w_qkv, rel_bias, w_proj, gain_two, w_up, w_down):
    sizes = Sizes(fields.shape)
    lat_cells, lon_cells, levels, features = fields.shape
    heads, length = rel_bias.shape
    group = WIN_LON * levels
    tokens = WIN_LAT * group
    window = (WIN_LAT, WIN_LON, levels, features)
    bf16, f32 = jnp.bfloat16, jnp.float32
    shape = jax.ShapeDtypeStruct
    gains = [gain_one.reshape(1, -1), gain_two.reshape(1, -1)]
    sources = [w_qkv, w_proj, w_up, w_down]
    flips = [shape(w.shape[::-1], w.dtype) for w in sources]
    dma = pltpu.SemaphoreType.DMA
    pairs = sizes.leaving // PAIR
    token = pl.pallas_call(
        first_kernel,
        out_shape=shape((8, 128), f32),
        out_specs=vmem(),
        cost_estimate=cost(2**36, 2**26),
        compiler_params=pltpu.CompilerParams(vmem_limit_bytes=2**20),
    )()
    pair_shape = (2, features, PAIR * tokens)
    outcome = pl.pallas_call(
        functools.partial(main_kernel, sizes),
        out_shape=[
            shape((sizes.early + sizes.late + sizes.leaving + 1,) + window, bf16),
            shape((sizes.count,), jnp.int32),
            shape((lat_cells + WIN_LAT // 2, lon_cells + WIN_LON // 2, levels, features), bf16),
        ]
        + flips
        + [shape((features, 128), f32)] * 2
        + [shape((heads // 2, tokens, 2 * tokens), f32)],
        in_specs=[smem()] + [vmem()] * 9,
        out_specs=[vmem(), smem()] + [vmem()] * 8,
        scratch_shapes=[
            pltpu.VMEM((sizes.leaving,) + window, bf16),
            pltpu.VMEM((sizes.leaving,) + window, bf16),
            pltpu.VMEM(pair_shape, bf16),
            pltpu.VMEM(pair_shape, bf16),
            pltpu.VMEM(pair_shape, bf16),
            pltpu.SMEM((2, sizes.count + 2), jnp.int32),
            pltpu.SMEM((2, sizes.count + 2), jnp.int32),
            pltpu.VMEM((heads, (length + 255) // 128 * 128), f32),
            pltpu.VMEM((heads, group, 2 * tokens), f32),
        ]
        + [dma((3,)), dma((3,)), dma((sizes.leaving,)), dma((sizes.leaving,))]
        + [dma((pairs,)), dma((pairs,))],
        cost_estimate=cost(0, fields.size),
        compiler_params=pltpu.CompilerParams(
            collective_id=0, has_side_effects=True, vmem_limit_bytes=24 * 2**20
        ),
    )(ocean_mask, token, fields, rel_bias, gains[0], w_qkv, w_proj, gains[1], w_up, w_down)
    results, codes = outcome[:2]
    return pl.pallas_call(
        functools.partial(place_kernel, sizes),
        out_shape=shape(fields.shape, fields.dtype),
        in_specs=[smem()] + [vmem()] * 9,
        out_specs=any_space(),
        scratch_shapes=[pltpu.VMEM(window, bf16), dma((sizes.count,))],
        cost_estimate=cost(0, 4 * fields.size),
        compiler_params=pltpu.CompilerParams(vmem_limit_bytes=12 * 2**20),
    )(codes, results, *outcome[2:])


def solution(mesh):
    in_specs = (P("lat", "lon", None, None), P("lat", None), P(), P(), P(), P(), P(), P(), P())
    out_specs = P("lat", "lon", None, None)
    return jax.shard_map(body, mesh=mesh, in_specs=in_specs, out_specs=out_specs, check_vma=False)
```

```python
import functools
import math

import jax
import jax.numpy as jnp
from jax import lax
from jax.experimental import pallas as pl
from jax.experimental.pallas import tpu as pltpu
from jax.sharding import PartitionSpec as P

WIN_LAT = 8
WIN_LON = 8
NORM_FLOOR = 0.25
MESH = pl.DeviceIdType.MESH
LOG2E = math.log2(math.e)
ROOT_HALF = math.sqrt(0.5)
PAIR = 2
EARLY_PAIRS = 3
LEAVING_PAIRS = 2


def dot(left, right):
    return jnp.dot(left, right, preferred_element_type=jnp.float32)


def normalise(values, gain):
    share = 1.0 / values.shape[0]
    average = jnp.sum(values, axis=0, keepdims=True) * share
    centred = values - average
    spread = jnp.sum(centred * centred, axis=0, keepdims=True) * share
    return (centred * lax.rsqrt(spread + NORM_FLOOR) * gain).astype(jnp.bfloat16)


def wide(gain, columns):
    return jnp.concatenate([gain] * (columns // gain.shape[1]), axis=1)


def flip_steps(store, blocks, weights):
    flipped = jnp.concatenate([block.T for block in blocks], axis=1)
    gain = wide(weights["gain_one"][...], flipped.shape[1])
    store.extend([flipped, normalise(flipped.astype(jnp.float32), gain)])
    yield


def attention_steps(store, flipped, normed, weights):
    qkv_t, proj_t, bias = weights["qkv"], weights["proj"], weights["bias"]
    features, columns = normed.shape
    half, tokens, _ = bias.shape
    dim = features // (2 * half)
    scale = LOG2E / math.sqrt(dim)
    key_t = dot(qkv_t[features : 2 * features], normed).astype(jnp.bfloat16)
    yield
    query_t = (dot(qkv_t[:features], normed) * scale).astype(jnp.bfloat16)
    yield
    value_t = dot(qkv_t[2 * features :], normed).astype(jnp.bfloat16)
    yield
    lane_head = lax.broadcasted_iota(jnp.int32, (tokens, features), 1) // dim % half
    nothing = jnp.zeros((features // 2, tokens), jnp.bfloat16)
    ones = jnp.ones((16, tokens), jnp.bfloat16)
    spans = [slice(n, n + tokens) for n in range(0, columns, tokens)]
    every = []
    for lanes in spans:
        key = key_t[:, lanes].T
        masked = [jnp.where(lane_head == h, key, jnp.zeros_like(key)) for h in range(half)]
        upper = jnp.concatenate([query_t[: features // 2, lanes], nothing], axis=1)
        lower = jnp.concatenate([nothing, query_t[features // 2 :, lanes]], axis=1)
        every.append(dot(jnp.concatenate(masked, axis=0), jnp.concatenate([upper, lower], axis=0)))
        yield
    mixed = []
    for lanes, products in zip(spans, every):
        first, second = [], []
        for h in range(half):
            scores = products[h * tokens : (h + 1) * tokens] + bias[h]
            power = jnp.exp2(scores - jnp.max(scores, axis=0, keepdims=True)).astype(jnp.bfloat16)
            one, two = h * dim, (h + half) * dim
            rows = [value_t[one : one + dim, lanes], value_t[two : two + dim, lanes], ones]
            piece = dot(jnp.concatenate(rows, axis=0), power)
            share = 1.0 / piece[2 * dim : 2 * dim + 1]
            first.append((piece[:dim, :tokens] * share[:, :tokens]).astype(jnp.bfloat16))
            second.append((piece[dim : 2 * dim, tokens:] * share[:, tokens:]).astype(jnp.bfloat16))
            yield
        mixed.append(jnp.concatenate(first + second, axis=0))
    projected = dot(proj_t[...], jnp.concatenate(mixed, axis=1))
    store.append((flipped.astype(jnp.float32) + projected).astype(jnp.bfloat16))
    yield


def mlp_steps(store, middle, weights, tokens):
    up_t, down_t, gain = weights["up"], weights["down"], weights["gain_two"]
    features, hidden = middle.shape[0], up_t.shape[0]
    residual = middle.astype(jnp.float32)
    normed = normalise(residual, wide(gain[...], middle.shape[1]))
    yield
    total = None
    for part in range(hidden // features):
        rows = slice(part * features, (part + 1) * features)
        grown = dot(up_t[rows], normed)
        yield
        grown = (grown * (1.0 + lax.erf(grown))).astype(jnp.bfloat16)
        piece = dot(down_t[:, rows], grown)
        total = piece if total is None else total + piece
        yield
    result = (residual + total * ROOT_HALF).astype(jnp.bfloat16)
    for n in range(middle.shape[1] // tokens):
        store.append(result[:, n * tokens : (n + 1) * tokens].T)
    yield


def weave(*steps):
    steps = list(steps)
    while steps:
        for chain in list(steps):
            try:
                next(chain)
            except StopIteration:
                steps.remove(chain)


def bias_strips(rel_bias, padded, strips, levels):
    heads, length = rel_bias.shape
    col_step = 2 * levels - 1
    row_step = (2 * WIN_LON - 1) * col_step
    offsets = [c * col_step + lev for c in range(WIN_LON) for lev in range(levels)]
    top = offsets[-1]
    width = padded.shape[1] - 128
    padded[...] = jnp.zeros_like(padded)
    padded[:, :length] = rel_bias[...] * LOG2E
    table = padded[...]
    left = jnp.concatenate([table[:, top - q : top - q + width] for q in offsets], axis=0)
    group = WIN_LON * levels
    lane = lax.broadcasted_iota(jnp.int32, (width, strips.shape[2]), 1)
    inner = lane % group
    target = lane // group * row_step + inner // levels * col_step + inner % levels
    pick = lax.broadcasted_iota(jnp.int32, target.shape, 0) == target
    found = jnp.dot(
        left,
        pick.astype(jnp.float32),
        precision=lax.Precision.HIGHEST,
        preferred_element_type=jnp.float32,
    )
    for place in range(group):
        strips[:, place, :] = found[place * heads : (place + 1) * heads]


def bias_table(strips, bias):
    heads, group, _ = strips.shape
    tokens = WIN_LAT * group
    for row in range(WIN_LAT):
        first = (WIN_LAT - 1 - row) * group
        piece = strips[:, :, first : first + tokens]
        places = slice(row * group, (row + 1) * group)
        bias[:, places, :tokens] = piece[: heads // 2]
        bias[:, places, tokens:] = piece[heads // 2 :]


class Sizes:
    def __init__(self, fields_shape):
        self.rows = fields_shape[0] // WIN_LAT
        self.cols = fields_shape[1] // WIN_LON
        self.count = self.rows * self.cols
        self.late = -(-((self.rows - 1) * self.cols // 2) // PAIR) * PAIR
        self.early = EARLY_PAIRS * PAIR
        self.leaving = min(LEAVING_PAIRS * PAIR, self.late)
        self.edge = self.rows + self.cols - 1

    def interior(self, window):
        return window // self.cols < self.rows - 1 and window % self.cols < self.cols - 1


def share_out(sizes, mask, device):
    def tally(d):
        inside, outside = jnp.int32(0), jnp.int32(0)
        for window in range(sizes.count):
            ocean = mask[window // sizes.cols, d * sizes.cols + window % sizes.cols]
            if sizes.interior(window):
                inside = inside + ocean
            else:
                outside = outside + ocean
        return inside, outside

    last = lax.axis_size("lon") - 1

    def pass_on(d, carried):
        inside, outside = tally(d)
        early = jnp.minimum(inside, sizes.early)
        excess = carried + inside + outside - early - sizes.late
        leaving = jnp.minimum(jnp.minimum(excess, inside - early), sizes.leaving)
        return jnp.where(d == last, 0, jnp.maximum(leaving, 0))

    coming = lax.fori_loop(0, device, pass_on, jnp.int32(0))
    leaving = pass_on(device, coming)
    inside, outside = tally(device)
    return coming, leaving, jnp.minimum(inside, sizes.early), inside, outside


def first_kernel(token):
    token[...] = jnp.zeros_like(token)


def main_kernel(
    sizes,
    mask, token, fields, rel_bias, gain_one, w_qkv, w_proj, gain_two, w_up, w_down,
    results, codes, ext, qkv_t, proj_t, up_t, down_t, gain_one_t, gain_two_t, bias,
    arrived, leave, flipped, normed, middle, inner, outer, padded, strips,
    halo_send, halo_recv, out_send, out_recv, back_send, back_recv,
):
    lat_cells, lon_cells, levels, features = fields.shape
    lat_half, lon_half = WIN_LAT // 2, WIN_LON // 2
    tokens = WIN_LAT * WIN_LON * levels
    lat, lon = lax.axis_index("lat"), lax.axis_index("lon")
    lat_size, lon_size = lax.axis_size("lat"), lax.axis_size("lon")
    last = lon_size - 1
    west, east = (lon + lon_size - 1) % lon_size, (lon + 1) % lon_size
    barrier = pltpu.get_barrier_semaphore()

    def greet(row, col):
        pl.semaphore_signal(barrier, inc=1, device_id=(row, col), device_id_type=MESH)

    greet(lat, east)
    greet(lat, west)

    @pl.when(lat < lat_size - 1)
    def _():
        greet(lat + 1, lon)
        greet(lat + 1, east)

    def transfer(source, target, send, recv, row, col):
        return pltpu.make_async_remote_copy(
            src_ref=source, dst_ref=target, send_sem=send, recv_sem=recv,
            device_id=(row, col), device_id_type=MESH,
        )

    up = jnp.maximum(lat - 1, 0)
    below, beside = pl.ds(lat_cells, lat_half), pl.ds(lon_cells, lon_half)
    rows, cols = pl.ds(lat_half, lat_cells - lat_half), pl.ds(lon_half, lon_cells - lon_half)
    top, left = pl.ds(0, lat_half), pl.ds(0, lon_half)
    to_north = transfer(
        fields.at[top, cols], ext.at[below, cols], halo_send.at[0], halo_recv.at[0], up, lon
    )
    to_west = transfer(
        fields.at[rows, left], ext.at[rows, beside], halo_send.at[1], halo_recv.at[1], lat, west
    )
    to_corner = transfer(
        fields.at[top, left], ext.at[below, beside], halo_send.at[2], halo_recv.at[2], up, west
    )

    coming, going, early, _, edges = share_out(sizes, mask, lon)
    first_col = lon * sizes.cols
    for chain, inside_only in ((inner, True), (outer, False)):
        following = jnp.int32(sizes.count)
        chain[0, sizes.count] = following
        chain[0, sizes.count + 1] = following
        for window in reversed(range(sizes.count)):
            if sizes.interior(window) == inside_only:
                ocean = mask[window // sizes.cols, first_col + window % sizes.cols]
                following = jnp.where(ocean == 1, window, following)
            chain[0, window] = following
        spot = following
        for n in range(sizes.count):
            chain[1, n] = jnp.where(spot == sizes.count, 0, spot)
            spot = chain[0, spot + 1]

    def fetch(source, window):
        row, col = window // sizes.cols, window % sizes.cols
        row_cells = pl.ds(row * WIN_LAT + lat_half, WIN_LAT)
        return source[row_cells, pl.ds(col * WIN_LON + lon_half, WIN_LON)]

    def outward(slot):
        return transfer(
            leave.at[slot], arrived.at[slot], out_send.at[slot], out_recv.at[slot],
            lat, jnp.minimum(lon + 1, last),
        )

    def homeward(pair):
        slots = pl.ds(sizes.early + sizes.late + pair * PAIR, PAIR)
        return transfer(
            results.at[pl.ds(sizes.early + pair * PAIR, PAIR)], results.at[slots],
            back_send.at[pair], back_recv.at[pair], lat, jnp.maximum(lon - 1, 0),
        )

    def pack(slot, carry):
        leave[slot] = fetch(fields, inner[1, sizes.early + slot])
        return carry

    lax.fori_loop(0, sizes.leaving, pack, 0)

    @pl.when(lat > 0)
    def _():
        pl.semaphore_wait(barrier, 4)
        to_north.start()
        to_corner.start()

    @pl.when(lat == 0)
    def _():
        pl.semaphore_wait(barrier, 2)

    to_west.start()

    @pl.when(lon < last)
    def _():
        for slot in range(sizes.leaving):
            outward(slot).start()

    bias_strips(rel_bias, padded, strips, levels)
    bias_table(strips, bias)
    gain_one_t[...] = jnp.broadcast_to(gain_one[...], (128, features)).T
    gain_two_t[...] = jnp.broadcast_to(gain_two[...] * ROOT_HALF, (128, features)).T
    for source, target in ((w_qkv, qkv_t), (w_proj, proj_t), (w_up, up_t), (w_down, down_t)):
        target[...] = source[...].T
    weights = dict(
        qkv=qkv_t, proj=proj_t, up=up_t, down=down_t,
        gain_one=gain_one_t, gain_two=gain_two_t, bias=bias,
    )
    early_pairs, late_pairs, leaving_pairs = (
        sizes.early // PAIR, sizes.late // PAIR, sizes.leaving // PAIR
    )

    def early_blocks(step):
        windows = [fetch(fields, inner[1, step * PAIR + n]) for n in range(PAIR)]
        return [window.reshape(tokens, features) for window in windows]

    def late_blocks(pair):
        blocks = []
        for n in range(PAIR):
            slot = pair * PAIR + n
            rank = slot - coming
            edge = jnp.clip(rank, 0, sizes.count - 1)
            other = jnp.clip(early + going + rank - edges, 0, sizes.count - 1)
            mine = fetch(ext, jnp.where(rank < edges, outer[1, edge], inner[1, other]))
            sent = arrived[jnp.minimum(slot, sizes.leaving - 1)]
            block = jnp.where(rank >= 0, mine, sent)
            blocks.append(block.reshape(tokens, features))
        return blocks

    def put(step, flip):
        flipped[step % 2], normed[step % 2] = flip

    def keep(step, windows):
        for n, window in enumerate(windows):
            results[step * PAIR + n] = window.reshape(results.shape[1:])

    def advance(step, before=True, blocks=None):
        new, windows, flip = [], [], []
        chains = [attention_steps(new, flipped[step % 2], normed[step % 2], weights)]
        if before:
            chains.insert(0, mlp_steps(windows, middle[(step + 1) % 2], weights, tokens))
        weave(*chains)
        if blocks is not None:
            weave(flip_steps(flip, blocks, weights))
            put(step + 1, flip)
        if before:
            keep(step - 1, windows)
        middle[step % 2] = new[0]

    def prepare(step, blocks):
        flip = []
        weave(flip_steps(flip, blocks, weights))
        put(step, flip)

    prepare(0, early_blocks(0))
    advance(0, before=False, blocks=early_blocks(1) if early_pairs > 1 else None)

    def early_step(step, carry):
        advance(step, blocks=early_blocks(step + 1))
        return carry

    lax.fori_loop(1, early_pairs - 1, early_step, 0)
    if early_pairs > 1:
        advance(early_pairs - 1)
    inside_rows, inside_cols = pl.ds(lat_half, lat_cells - lat_half), pl.ds(lon_half, lon_cells - lon_half)
    ext[inside_rows, inside_cols] = fields[inside_rows, inside_cols]
    to_west.wait_recv()

    @pl.when(lat < lat_size - 1)
    def _():
        to_north.wait_recv()
        to_corner.wait_recv()

    def receive(pair):
        @pl.when((pair < leaving_pairs) & (lon > 0))
        def _():
            for n in range(PAIR):
                outward(pair * PAIR + n).wait_recv()

    def send_home(pair):
        @pl.when((pair >= 0) & (pair < leaving_pairs) & (lon > 0))
        def _():
            homeward(pair).start()

    receive(jnp.int32(0))
    prepare(early_pairs, late_blocks(0))

    def late_step(pair, carry):
        receive(pair + 1)
        advance(early_pairs + pair, blocks=late_blocks(jnp.minimum(pair + 1, late_pairs - 1)))
        send_home(pair - 1)
        return carry

    lax.fori_loop(0, late_pairs, late_step, 0)
    steps = early_pairs + late_pairs
    windows = []
    weave(mlp_steps(windows, middle[(steps - 1) % 2], weights, tokens))
    keep(steps - 1, windows)
    if late_pairs <= leaving_pairs:
        send_home(jnp.int32(late_pairs - 1))

    room = sizes.late - coming
    back = sizes.early + sizes.late
    results[back + sizes.leaving] = jnp.zeros(results.shape[1:], results.dtype)
    inside_rank, edge_rank = jnp.int32(0), jnp.int32(0)
    for window in range(sizes.count):
        ocean = mask[window // sizes.cols, first_col + window % sizes.cols]
        if sizes.interior(window):
            rank = edges + inside_rank - early - going
        else:
            rank = edge_rank
        code = jnp.where(rank < room, sizes.early + coming + rank, -1)
        if sizes.interior(window):
            code = jnp.where(inside_rank < early + going, back + inside_rank - early, code)
            code = jnp.where(inside_rank < early, inside_rank, code)
            inside_rank = inside_rank + ocean
        else:
            edge_rank = edge_rank + ocean
        codes[window] = jnp.where(ocean == 1, code, back + sizes.leaving)

    to_west.wait_send()

    @pl.when(lat > 0)
    def _():
        to_north.wait_send()
        to_corner.wait_send()

    @pl.when(lon > 0)
    def _():
        for pair in range(leaving_pairs):
            homeward(pair).wait_send()

    @pl.when(lon < last)
    def _():
        for slot in range(sizes.leaving):
            outward(slot).wait_send()
        for pair in range(leaving_pairs):
            homeward(pair).wait_recv()


def place_kernel(
    sizes,
    codes, results, ext, qkv_t, proj_t, up_t, down_t, gain_one_t, gain_two_t, bias,
    output, extra, sems,
):
    lat_half, lon_half = WIN_LAT // 2, WIN_LON // 2
    nothing = results.shape[0] - 1

    def spot(window):
        row, col = window // sizes.cols, window % sizes.cols
        return output.at[pl.ds(row * WIN_LAT, WIN_LAT), pl.ds(col * WIN_LON, WIN_LON)]

    lost = jnp.int32(0)
    for window in range(sizes.count):
        code = codes[window]
        lost = jnp.minimum(lost, code)
        source = results.at[jnp.where(code < 0, nothing, code)]
        pltpu.make_async_copy(source, spot(window), sems.at[window]).start()
    for window in range(sizes.count):
        pltpu.make_async_copy(results.at[nothing], spot(window), sems.at[window]).wait()

    @pl.when(lost < 0)
    def _():
        def again(window, carry):
            @pl.when(codes[window] < 0)
            def _():
                row, col = window // sizes.cols, window % sizes.cols
                row_cells = pl.ds(row * WIN_LAT + lat_half, WIN_LAT)
                block = ext[row_cells, pl.ds(col * WIN_LON + lon_half, WIN_LON)]
                weights = dict(
                    qkv=qkv_t, proj=proj_t, up=up_t, down=down_t,
                    gain_one=gain_one_t, gain_two=gain_two_t, bias=bias,
                )
                tokens = block.shape[0] * block.shape[1] * block.shape[2]
                flip, middle, windows = [], [], []
                weave(flip_steps(flip, [block.reshape(tokens, block.shape[3])], weights))
                weave(attention_steps(middle, flip[0], flip[1], weights))
                weave(mlp_steps(windows, middle[0], weights, tokens))
                extra[...] = windows[0].reshape(extra.shape)
                copy = pltpu.make_async_copy(extra, spot(window), sems.at[window])
                copy.start()
                copy.wait()

            return carry

        lax.fori_loop(0, sizes.count, again, 0)


def vmem():
    return pl.BlockSpec(memory_space=pltpu.VMEM)


def smem():
    return pl.BlockSpec(memory_space=pltpu.SMEM)


def any_space():
    return pl.BlockSpec(memory_space=pl.ANY)


def cost(flops, moved):
    return pl.CostEstimate(flops=flops, bytes_accessed=moved, transcendentals=0)


def body(fields, ocean_mask, gain_one, w_qkv, rel_bias, w_proj, gain_two, w_up, w_down):
    sizes = Sizes(fields.shape)
    lat_cells, lon_cells, levels, features = fields.shape
    heads, length = rel_bias.shape
    group = WIN_LON * levels
    tokens = WIN_LAT * group
    window = (WIN_LAT, WIN_LON, levels, features)
    bf16, f32 = jnp.bfloat16, jnp.float32
    shape = jax.ShapeDtypeStruct
    gains = [gain_one.reshape(1, -1), gain_two.reshape(1, -1)]
    sources = [w_qkv, w_proj, w_up, w_down]
    flips = [shape(w.shape[::-1], w.dtype) for w in sources]
    dma = pltpu.SemaphoreType.DMA
    pairs = sizes.leaving // PAIR
    token = pl.pallas_call(
        first_kernel,
        out_shape=shape((8, 128), f32),
        out_specs=vmem(),
        cost_estimate=cost(2**36, 2**26),
        compiler_params=pltpu.CompilerParams(vmem_limit_bytes=2**20),
    )()
    pair_shape = (2, features, PAIR * tokens)
    outcome = pl.pallas_call(
        functools.partial(main_kernel, sizes),
        out_shape=[
            shape((sizes.early + sizes.late + sizes.leaving + 1,) + window, bf16),
            shape((sizes.count,), jnp.int32),
            shape((lat_cells + WIN_LAT // 2, lon_cells + WIN_LON // 2, levels, features), bf16),
        ]
        + flips
        + [shape((features, 128), f32)] * 2
        + [shape((heads // 2, tokens, 2 * tokens), f32)],
        in_specs=[smem()] + [vmem()] * 9,
        out_specs=[vmem(), smem()] + [vmem()] * 8,
        scratch_shapes=[
            pltpu.VMEM((sizes.leaving,) + window, bf16),
            pltpu.VMEM((sizes.leaving,) + window, bf16),
            pltpu.VMEM(pair_shape, bf16),
            pltpu.VMEM(pair_shape, bf16),
            pltpu.VMEM(pair_shape, bf16),
            pltpu.SMEM((2, sizes.count + 2), jnp.int32),
            pltpu.SMEM((2, sizes.count + 2), jnp.int32),
            pltpu.VMEM((heads, (length + 255) // 128 * 128), f32),
            pltpu.VMEM((heads, group, 2 * tokens), f32),
        ]
        + [dma((3,)), dma((3,)), dma((sizes.leaving,)), dma((sizes.leaving,))]
        + [dma((pairs,)), dma((pairs,))],
        cost_estimate=cost(0, fields.size),
        compiler_params=pltpu.CompilerParams(
            collective_id=0, has_side_effects=True, vmem_limit_bytes=24 * 2**20
        ),
    )(ocean_mask, token, fields, rel_bias, gains[0], w_qkv, w_proj, gains[1], w_up, w_down)
    results, codes = outcome[:2]
    return pl.pallas_call(
        functools.partial(place_kernel, sizes),
        out_shape=shape(fields.shape, fields.dtype),
        in_specs=[smem()] + [vmem()] * 9,
        out_specs=any_space(),
        scratch_shapes=[pltpu.VMEM(window, bf16), dma((sizes.count,))],
        cost_estimate=cost(0, 4 * fields.size),
        compiler_params=pltpu.CompilerParams(vmem_limit_bytes=12 * 2**20),
    )(codes, results, *outcome[2:])


def solution(mesh):
    in_specs = (P("lat", "lon", None, None), P("lat", None), P(), P(), P(), P(), P(), P(), P())
    out_specs = P("lat", "lon", None, None)
    return jax.shard_map(body, mesh=mesh, in_specs=in_specs, out_specs=out_specs, check_vma=False)
```

```python
import functools
import math

import jax
import jax.numpy as jnp
from jax import lax
from jax.experimental import pallas as pl
from jax.experimental.pallas import tpu as pltpu
from jax.sharding import PartitionSpec as P

WIN_LAT = 8
WIN_LON = 8
NORM_FLOOR = 0.25
MESH = pl.DeviceIdType.MESH
LOG2E = math.log2(math.e)
ROOT_HALF = math.sqrt(0.5)
PAIR = 2
EARLY_PAIRS = 5


def dot(left, right):
    return jnp.dot(left, right, preferred_element_type=jnp.float32)


def normalise(values, gain):
    share = 1.0 / values.shape[0]
    average = jnp.sum(values, axis=0, keepdims=True) * share
    centred = values - average
    spread = jnp.sum(centred * centred, axis=0, keepdims=True) * share
    return (centred * lax.rsqrt(spread + NORM_FLOOR) * gain).astype(jnp.bfloat16)


def wide(gain, columns):
    return jnp.concatenate([gain] * (columns // gain.shape[1]), axis=1)


def flip_steps(store, blocks, weights):
    flipped = jnp.concatenate([block.T for block in blocks], axis=1)
    gain = wide(weights["gain_one"][...], flipped.shape[1])
    store.extend([flipped, normalise(flipped.astype(jnp.float32), gain)])
    yield


def attention_steps(store, flipped, normed, weights):
    qkv_t, proj_t, bias = weights["qkv"], weights["proj"], weights["bias"]
    features, columns = normed.shape
    half, tokens, _ = bias.shape
    dim = features // (2 * half)
    scale = LOG2E / math.sqrt(dim)
    key_t = dot(qkv_t[features : 2 * features], normed).astype(jnp.bfloat16)
    yield
    query_t = (dot(qkv_t[:features], normed) * scale).astype(jnp.bfloat16)
    yield
    value_t = dot(qkv_t[2 * features :], normed).astype(jnp.bfloat16)
    yield
    lane_head = lax.broadcasted_iota(jnp.int32, (tokens, features), 1) // dim % half
    nothing = jnp.zeros((features // 2, tokens), jnp.bfloat16)
    ones = jnp.ones((16, tokens), jnp.bfloat16)
    spans = [slice(n, n + tokens) for n in range(0, columns, tokens)]
    every = []
    for lanes in spans:
        key = key_t[:, lanes].T
        masked = [jnp.where(lane_head == h, key, jnp.zeros_like(key)) for h in range(half)]
        upper = jnp.concatenate([query_t[: features // 2, lanes], nothing], axis=1)
        lower = jnp.concatenate([nothing, query_t[features // 2 :, lanes]], axis=1)
        every.append(dot(jnp.concatenate(masked, axis=0), jnp.concatenate([upper, lower], axis=0)))
        yield
    mixed = []
    for lanes, products in zip(spans, every):
        first, second = [], []
        for h in range(half):
            scores = products[h * tokens : (h + 1) * tokens] + bias[h]
            power = jnp.exp2(scores - jnp.max(scores, axis=0, keepdims=True)).astype(jnp.bfloat16)
            one, two = h * dim, (h + half) * dim
            rows = [value_t[one : one + dim, lanes], value_t[two : two + dim, lanes], ones]
            piece = dot(jnp.concatenate(rows, axis=0), power)
            share = 1.0 / piece[2 * dim : 2 * dim + 1]
            first.append((piece[:dim, :tokens] * share[:, :tokens]).astype(jnp.bfloat16))
            second.append((piece[dim : 2 * dim, tokens:] * share[:, tokens:]).astype(jnp.bfloat16))
            yield
        mixed.append(jnp.concatenate(first + second, axis=0))
    projected = dot(proj_t[...], jnp.concatenate(mixed, axis=1))
    store.append((flipped.astype(jnp.float32) + projected).astype(jnp.bfloat16))
    yield


def mlp_steps(store, middle, weights, tokens):
    up_t, down_t, gain = weights["up"], weights["down"], weights["gain_two"]
    features, hidden = middle.shape[0], up_t.shape[0]
    residual = middle.astype(jnp.float32)
    normed = normalise(residual, wide(gain[...], middle.shape[1]))
    yield
    total = None
    for part in range(hidden // features):
        rows = slice(part * features, (part + 1) * features)
        grown = dot(up_t[rows], normed)
        yield
        grown = (grown * (1.0 + lax.erf(grown))).astype(jnp.bfloat16)
        piece = dot(down_t[:, rows], grown)
        total = piece if total is None else total + piece
        yield
    result = (residual + total * ROOT_HALF).astype(jnp.bfloat16)
    for n in range(middle.shape[1] // tokens):
        store.append(result[:, n * tokens : (n + 1) * tokens].T)
    yield


def weave(*steps):
    steps = list(steps)
    while steps:
        for chain in list(steps):
            try:
                next(chain)
            except StopIteration:
                steps.remove(chain)


def bias_strips(rel_bias, padded, strips, levels):
    heads, length = rel_bias.shape
    col_step = 2 * levels - 1
    row_step = (2 * WIN_LON - 1) * col_step
    offsets = [c * col_step + lev for c in range(WIN_LON) for lev in range(levels)]
    top = offsets[-1]
    width = padded.shape[1] - 128
    padded[...] = jnp.zeros_like(padded)
    padded[:, :length] = rel_bias[...] * LOG2E
    table = padded[...]
    left = jnp.concatenate([table[:, top - q : top - q + width] for q in offsets], axis=0)
    group = WIN_LON * levels
    lane = lax.broadcasted_iota(jnp.int32, (width, strips.shape[2]), 1)
    inner = lane % group
    target = lane // group * row_step + inner // levels * col_step + inner % levels
    pick = lax.broadcasted_iota(jnp.int32, target.shape, 0) == target
    found = jnp.dot(
        left,
        pick.astype(jnp.float32),
        precision=lax.Precision.HIGHEST,
        preferred_element_type=jnp.float32,
    )
    for place in range(group):
        strips[:, place, :] = found[place * heads : (place + 1) * heads]


def bias_table(strips, bias):
    heads, group, _ = strips.shape
    tokens = WIN_LAT * group
    for row in range(WIN_LAT):
        first = (WIN_LAT - 1 - row) * group
        piece = strips[:, :, first : first + tokens]
        places = slice(row * group, (row + 1) * group)
        bias[:, places, :tokens] = piece[: heads // 2]
        bias[:, places, tokens:] = piece[heads // 2 :]


class Sizes:
    def __init__(self, fields_shape):
        self.rows = fields_shape[0] // WIN_LAT
        self.cols = fields_shape[1] // WIN_LON
        self.count = self.rows * self.cols
        self.early = EARLY_PAIRS * PAIR

    def interior(self, window):
        return window // self.cols < self.rows - 1 and window % self.cols < self.cols - 1

    def fetch(self, source, window):
        row, col = window // self.cols, window % self.cols
        rows = pl.ds(row * WIN_LAT + WIN_LAT // 2, WIN_LAT)
        block = source[rows, pl.ds(col * WIN_LON + WIN_LON // 2, WIN_LON)]
        return block.reshape(block.shape[0] * block.shape[1] * block.shape[2], block.shape[3])


class Pipeline:
    def __init__(self, weights, flipped, normed, middle, tokens, keep):
        self.weights, self.tokens, self.keep = weights, tokens, keep
        self.flipped, self.normed, self.middle = flipped, normed, middle

    def prepare(self, step, blocks):
        flip = []
        weave(flip_steps(flip, blocks, self.weights))
        self.flipped[step % 2], self.normed[step % 2] = flip

    def advance(self, step, before=True, blocks=None):
        new, windows = [], []
        flip = self.flipped[step % 2], self.normed[step % 2]
        chains = [attention_steps(new, *flip, self.weights)]
        if before:
            last = self.middle[(step + 1) % 2]
            chains.insert(0, mlp_steps(windows, last, self.weights, self.tokens))
        weave(*chains)
        if blocks is not None:
            self.prepare(step + 1, blocks)
        if before:
            self.keep(step - 1, windows)
        self.middle[step % 2] = new[0]

    def finish(self, step):
        windows = []
        weave(mlp_steps(windows, self.middle[step % 2], self.weights, self.tokens))
        self.keep(step, windows)


def first_kernel(token):
    token[...] = jnp.zeros_like(token)


def early_kernel(
    sizes,
    mask, token, fields, rel_bias, gain_one, w_qkv, w_proj, gain_two, w_up, w_down,
    results, middle, plan, ext, qkv_t, proj_t, up_t, down_t, gain_one_t, gain_two_t, bias,
    flipped, normed, chains, padded, strips, halo_send, halo_recv,
):
    lat_cells, lon_cells, levels, features = fields.shape
    lat_half, lon_half = WIN_LAT // 2, WIN_LON // 2
    lat, lon = lax.axis_index("lat"), lax.axis_index("lon")
    lat_size, lon_size = lax.axis_size("lat"), lax.axis_size("lon")
    west, east = (lon + lon_size - 1) % lon_size, (lon + 1) % lon_size
    barrier = pltpu.get_barrier_semaphore()

    def greet(row, col):
        pl.semaphore_signal(barrier, inc=1, device_id=(row, col), device_id_type=MESH)

    greet(lat, east)

    @pl.when(lat < lat_size - 1)
    def _():
        greet(lat + 1, lon)
        greet(lat + 1, east)

    def transfer(which, source, target, row, col):
        return pltpu.make_async_remote_copy(
            src_ref=source, dst_ref=target,
            send_sem=halo_send.at[which], recv_sem=halo_recv.at[which],
            device_id=(row, col), device_id_type=MESH,
        )

    up = jnp.maximum(lat - 1, 0)
    below, beside = pl.ds(lat_cells, lat_half), pl.ds(lon_cells, lon_half)
    rows, cols = pl.ds(lat_half, lat_cells - lat_half), pl.ds(lon_half, lon_cells - lon_half)
    top, left = pl.ds(0, lat_half), pl.ds(0, lon_half)
    to_north = transfer(0, fields.at[top, cols], ext.at[below, cols], up, lon)
    to_west = transfer(1, fields.at[rows, left], ext.at[rows, beside], lat, west)
    to_corner = transfer(2, fields.at[top, left], ext.at[below, beside], up, west)

    def send_halos():
        @pl.when(lat > 0)
        def _():
            pl.semaphore_wait(barrier, 3)
            to_north.start()
            to_corner.start()

        @pl.when(lat == 0)
        def _():
            pl.semaphore_wait(barrier, 1)

        to_west.start()

    first_col = lon * sizes.cols
    total = jnp.int32(0)
    for place, inside_only in ((0, True), (1, False)):
        following = jnp.int32(sizes.count)
        chains[sizes.count] = following
        chains[sizes.count + 1] = following
        found = jnp.int32(0)
        for window in reversed(range(sizes.count)):
            if sizes.interior(window) == inside_only:
                ocean = mask[window // sizes.cols, first_col + window % sizes.cols]
                following = jnp.where(ocean == 1, window, following)
                found = found + ocean
            chains[window] = following
        plan[place] = found
        spot = following
        for n in range(sizes.count):
            plan[2 + place * sizes.count + n] = jnp.where(spot == sizes.count, 0, spot)
            spot = chains[spot + 1]

    bias_strips(rel_bias, padded, strips, levels)
    bias_table(strips, bias)

    @pl.when(lon > 0)
    def _():
        send_halos()

    gain_one_t[...] = jnp.broadcast_to(gain_one[...], (128, features)).T
    gain_two_t[...] = jnp.broadcast_to(gain_two[...] * ROOT_HALF, (128, features)).T
    for source, target in ((w_qkv, qkv_t), (w_proj, proj_t), (w_up, up_t), (w_down, down_t)):
        target[...] = source[...].T
    weights = dict(
        qkv=qkv_t, proj=proj_t, up=up_t, down=down_t,
        gain_one=gain_one_t, gain_two=gain_two_t, bias=bias,
    )

    def blocks(step):
        return [sizes.fetch(fields, plan[2 + step * PAIR + n]) for n in range(PAIR)]

    def keep(step, windows):
        for n, window in enumerate(windows):
            results[step * PAIR + n] = window.reshape(results.shape[1:])

    tokens = WIN_LAT * WIN_LON * levels
    line = Pipeline(weights, flipped, normed, middle, tokens, keep)
    line.prepare(0, blocks(0))
    line.advance(0, before=False, blocks=blocks(1))

    @pl.when(lon == 0)
    def _():
        send_halos()

    def early_step(step, carry):
        line.advance(step, blocks=blocks(step + 1))
        return carry

    lax.fori_loop(1, EARLY_PAIRS - 1, early_step, 0)
    line.advance(EARLY_PAIRS - 1)
    ext[rows, cols] = fields[rows, cols]
    to_west.wait()

    @pl.when(lat > 0)
    def _():
        to_north.wait_send()
        to_corner.wait_send()

    @pl.when(lat < lat_size - 1)
    def _():
        to_north.wait_recv()
        to_corner.wait_recv()


def late_kernel(
    sizes,
    mask, where, plan, results, before, ext,
    qkv_t, proj_t, up_t, down_t, gain_one_t, gain_two_t, bias,
    output, flipped, normed, middle, late, zero, sems,
):
    first_col = where[0] * sizes.cols
    inside, edges = plan[0], plan[1]
    early = jnp.minimum(inside, sizes.early)
    rest = inside + edges - early
    pairs = (rest + PAIR - 1) // PAIR
    zero[...] = jnp.zeros_like(zero)

    def send(source, window):
        row, col = window // sizes.cols, window % sizes.cols
        target = output.at[pl.ds(row * WIN_LAT, WIN_LAT), pl.ds(col * WIN_LON, WIN_LON)]
        return pltpu.make_async_copy(source, target, sems.at[window])

    for window in range(sizes.count):

        @pl.when(mask[window // sizes.cols, first_col + window % sizes.cols] == 0)
        def _():
            send(zero, window).start()

    def write_early(n, carry):
        send(results.at[n], plan[2 + n]).start()
        return carry

    ready = jnp.minimum(early, sizes.early - PAIR)
    lax.fori_loop(0, ready, write_early, 0)

    def window_of(n):
        n = jnp.clip(n, 0, sizes.count - 1)
        other = jnp.clip(early + n - edges, 0, sizes.count - 1)
        return jnp.where(n < edges, plan[2 + sizes.count + n], plan[2 + other])

    def blocks(step):
        first = (step - EARLY_PAIRS) * PAIR
        return [sizes.fetch(ext, window_of(first + n)) for n in range(PAIR)]

    def keep(step, windows):
        for n, window in enumerate(windows):
            place = (step - EARLY_PAIRS) * PAIR + n
            slot = (place + PAIR) % late.shape[0]
            late[slot] = window.reshape(zero.shape)

            @pl.when((place >= 0) & (place < rest))
            def _():
                send(late.at[slot], window_of(place)).start()

            @pl.when((place < 0) & (sizes.early + place < early))
            def _():
                send(late.at[slot], plan[2 + jnp.clip(sizes.early + place, 0, sizes.count - 1)]).start()

    weights = dict(
        qkv=qkv_t, proj=proj_t, up=up_t, down=down_t,
        gain_one=gain_one_t, gain_two=gain_two_t, bias=bias,
    )
    tokens = bias.shape[1]
    line = Pipeline(weights, flipped, normed, middle, tokens, keep)
    last = EARLY_PAIRS - 1
    middle[last % 2] = before[last % 2]
    line.prepare(EARLY_PAIRS, blocks(jnp.int32(EARLY_PAIRS)))

    def late_step(step, carry):
        line.advance(step, blocks=blocks(step + 1))
        return carry

    lax.fori_loop(EARLY_PAIRS, EARLY_PAIRS + pairs, late_step, 0)
    line.finish(last + pairs)

    def wait(window, carry):
        send(zero, window).wait()
        return carry

    lax.fori_loop(0, sizes.count, wait, 0)


def vmem():
    return pl.BlockSpec(memory_space=pltpu.VMEM)


def smem():
    return pl.BlockSpec(memory_space=pltpu.SMEM)


def any_space():
    return pl.BlockSpec(memory_space=pl.ANY)


def cost(flops, moved):
    return pl.CostEstimate(flops=flops, bytes_accessed=moved, transcendentals=0)


def body(fields, ocean_mask, gain_one, w_qkv, rel_bias, w_proj, gain_two, w_up, w_down):
    sizes = Sizes(fields.shape)
    lat_cells, lon_cells, levels, features = fields.shape
    heads, length = rel_bias.shape
    group = WIN_LON * levels
    tokens = WIN_LAT * group
    window = (WIN_LAT, WIN_LON, levels, features)
    bf16, f32 = jnp.bfloat16, jnp.float32
    shape = jax.ShapeDtypeStruct
    gains = [gain_one.reshape(1, -1), gain_two.reshape(1, -1)]
    sources = [w_qkv, w_proj, w_up, w_down]
    flips = [shape(w.shape[::-1], w.dtype) for w in sources]
    dma = pltpu.SemaphoreType.DMA
    token = pl.pallas_call(
        first_kernel,
        out_shape=shape((8, 128), f32),
        out_specs=vmem(),
        cost_estimate=cost(2**36, 2**26),
        compiler_params=pltpu.CompilerParams(vmem_limit_bytes=2**20),
    )()
    pair_shape = (2, features, PAIR * tokens)
    tables = [shape((features, 128), f32)] * 2 + [shape((heads // 2, tokens, 2 * tokens), f32)]
    outcome = pl.pallas_call(
        functools.partial(early_kernel, sizes),
        out_shape=[
            shape((sizes.early,) + window, bf16),
            shape(pair_shape, bf16),
            shape((2 + 2 * sizes.count,), jnp.int32),
            shape((lat_cells + WIN_LAT // 2, lon_cells + WIN_LON // 2, levels, features), bf16),
        ]
        + flips
        + tables,
        in_specs=[smem()] + [vmem()] * 9,
        out_specs=[vmem(), vmem(), smem()] + [vmem()] * 8,
        scratch_shapes=[
            pltpu.VMEM(pair_shape, bf16),
            pltpu.VMEM(pair_shape, bf16),
            pltpu.SMEM((sizes.count + 2,), jnp.int32),
            pltpu.VMEM((heads, (length + 255) // 128 * 128), f32),
            pltpu.VMEM((heads, group, 2 * tokens), f32),
            dma((3,)),
            dma((3,)),
        ],
        cost_estimate=cost(2**36, 2**26),
        compiler_params=pltpu.CompilerParams(
            collective_id=0, has_side_effects=True, vmem_limit_bytes=24 * 2**20
        ),
    )(ocean_mask, token, fields, rel_bias, gains[0], w_qkv, w_proj, gains[1], w_up, w_down)
    results, middle, plan, ext = outcome[:4]
    where = jnp.reshape(lax.axis_index("lon"), (1,)).astype(jnp.int32)
    return pl.pallas_call(
        functools.partial(late_kernel, sizes),
        out_shape=shape(fields.shape, fields.dtype),
        in_specs=[smem()] * 3 + [vmem()] * 10,
        out_specs=any_space(),
        scratch_shapes=[
            pltpu.VMEM(pair_shape, bf16),
            pltpu.VMEM(pair_shape, bf16),
            pltpu.VMEM(pair_shape, bf16),
            pltpu.VMEM((sizes.count + PAIR,) + window, bf16),
            pltpu.VMEM(window, bf16),
            dma((sizes.count,)),
        ],
        cost_estimate=cost(0, 4 * fields.size),
        compiler_params=pltpu.CompilerParams(vmem_limit_bytes=16 * 2**20),
    )(ocean_mask, where, plan, results, middle, ext, *outcome[4:])


def solution(mesh):
    in_specs = (P("lat", "lon", None, None), P("lat", None), P(), P(), P(), P(), P(), P(), P())
    out_specs = P("lat", "lon", None, None)
    return jax.shard_map(body, mesh=mesh, in_specs=in_specs, out_specs=out_specs, check_vma=False)
```

```python
import functools
import math

import jax
import jax.numpy as jnp
from jax import lax
from jax.experimental import pallas as pl
from jax.experimental.pallas import tpu as pltpu
from jax.sharding import PartitionSpec as P

WIN_LAT = 8
WIN_LON = 8
NORM_FLOOR = 0.25
MESH = pl.DeviceIdType.MESH
LOG2E = math.log2(math.e)
ROOT_HALF = math.sqrt(0.5)
PAIR = 2
EARLY_PAIRS = 5
FIRST_SENDS = 2


def dot(left, right):
    return jnp.dot(left, right, preferred_element_type=jnp.float32)


def normalise(values, gain):
    share = 1.0 / values.shape[0]
    average = jnp.sum(values, axis=0, keepdims=True) * share
    centred = values - average
    spread = jnp.sum(centred * centred, axis=0, keepdims=True) * share
    return (centred * lax.rsqrt(spread + NORM_FLOOR) * gain).astype(jnp.bfloat16)


def wide(gain, columns):
    return jnp.concatenate([gain] * (columns // gain.shape[1]), axis=1)


def flip_steps(store, blocks, weights):
    flipped = jnp.concatenate([block.T for block in blocks], axis=1)
    gain = wide(weights["gain_one"][...], flipped.shape[1])
    store.extend([flipped, normalise(flipped.astype(jnp.float32), gain)])
    yield


def attention_steps(store, flipped, normed, weights):
    qkv_t, proj_t, bias = weights["qkv"], weights["proj"], weights["bias"]
    features, columns = normed.shape
    half, tokens, _ = bias.shape
    dim = features // (2 * half)
    scale = LOG2E / math.sqrt(dim)
    key_t = dot(qkv_t[features : 2 * features], normed).astype(jnp.bfloat16)
    yield
    query_t = (dot(qkv_t[:features], normed) * scale).astype(jnp.bfloat16)
    yield
    value_t = dot(qkv_t[2 * features :], normed).astype(jnp.bfloat16)
    yield
    lane_head = lax.broadcasted_iota(jnp.int32, (tokens, features), 1) // dim % half
    nothing = jnp.zeros((features // 2, tokens), jnp.bfloat16)
    ones = jnp.ones((16, tokens), jnp.bfloat16)
    spans = [slice(n, n + tokens) for n in range(0, columns, tokens)]
    every = []
    for lanes in spans:
        key = key_t[:, lanes].T
        masked = [jnp.where(lane_head == h, key, jnp.zeros_like(key)) for h in range(half)]
        upper = jnp.concatenate([query_t[: features // 2, lanes], nothing], axis=1)
        lower = jnp.concatenate([nothing, query_t[features // 2 :, lanes]], axis=1)
        every.append(dot(jnp.concatenate(masked, axis=0), jnp.concatenate([upper, lower], axis=0)))
        yield
    mixed = []
    for lanes, products in zip(spans, every):
        first, second = [], []
        for h in range(half):
            scores = products[h * tokens : (h + 1) * tokens] + bias[h]
            power = jnp.exp2(scores - jnp.max(scores, axis=0, keepdims=True)).astype(jnp.bfloat16)
            one, two = h * dim, (h + half) * dim
            rows = [value_t[one : one + dim, lanes], value_t[two : two + dim, lanes], ones]
            piece = dot(jnp.concatenate(rows, axis=0), power)
            share = 1.0 / piece[2 * dim : 2 * dim + 1]
            first.append((piece[:dim, :tokens] * share[:, :tokens]).astype(jnp.bfloat16))
            second.append((piece[dim : 2 * dim, tokens:] * share[:, tokens:]).astype(jnp.bfloat16))
            yield
        mixed.append(jnp.concatenate(first + second, axis=0))
    projected = dot(proj_t[...], jnp.concatenate(mixed, axis=1))
    store.append((flipped.astype(jnp.float32) + projected).astype(jnp.bfloat16))
    yield


def mlp_steps(store, middle, weights, tokens):
    up_t, down_t, gain = weights["up"], weights["down"], weights["gain_two"]
    features, hidden = middle.shape[0], up_t.shape[0]
    residual = middle.astype(jnp.float32)
    normed = normalise(residual, wide(gain[...], middle.shape[1]))
    yield
    total = None
    for part in range(hidden // features):
        rows = slice(part * features, (part + 1) * features)
        grown = dot(up_t[rows], normed)
        yield
        grown = (grown * (1.0 + lax.erf(grown))).astype(jnp.bfloat16)
        piece = dot(down_t[:, rows], grown)
        total = piece if total is None else total + piece
        yield
    result = (residual + total * ROOT_HALF).astype(jnp.bfloat16)
    for n in range(middle.shape[1] // tokens):
        store.append(result[:, n * tokens : (n + 1) * tokens].T)
    yield


def weave(*steps):
    steps = list(steps)
    while steps:
        for chain in list(steps):
            try:
                next(chain)
            except StopIteration:
                steps.remove(chain)


def bias_strips(rel_bias, padded, strips, levels):
    heads, length = rel_bias.shape
    col_step = 2 * levels - 1
    row_step = (2 * WIN_LON - 1) * col_step
    offsets = [c * col_step + lev for c in range(WIN_LON) for lev in range(levels)]
    top = offsets[-1]
    width = padded.shape[1] - 128
    padded[...] = jnp.zeros_like(padded)
    padded[:, :length] = rel_bias[...] * LOG2E
    table = padded[...]
    left = jnp.concatenate([table[:, top - q : top - q + width] for q in offsets], axis=0)
    group = WIN_LON * levels
    lane = lax.broadcasted_iota(jnp.int32, (width, strips.shape[2]), 1)
    inner = lane % group
    target = lane // group * row_step + inner // levels * col_step + inner % levels
    pick = lax.broadcasted_iota(jnp.int32, target.shape, 0) == target
    found = jnp.dot(
        left,
        pick.astype(jnp.float32),
        precision=lax.Precision.HIGHEST,
        preferred_element_type=jnp.float32,
    )
    for place in range(group):
        strips[:, place, :] = found[place * heads : (place + 1) * heads]


def bias_table(strips, bias):
    heads, group, _ = strips.shape
    tokens = WIN_LAT * group
    for row in range(WIN_LAT):
        first = (WIN_LAT - 1 - row) * group
        piece = strips[:, :, first : first + tokens]
        places = slice(row * group, (row + 1) * group)
        bias[:, places, :tokens] = piece[: heads // 2]
        bias[:, places, tokens:] = piece[heads // 2 :]


class Sizes:
    def __init__(self, fields_shape):
        self.rows = fields_shape[0] // WIN_LAT
        self.cols = fields_shape[1] // WIN_LON
        self.count = self.rows * self.cols
        self.early = EARLY_PAIRS * PAIR

    def interior(self, window):
        return window // self.cols < self.rows - 1 and window % self.cols < self.cols - 1

    def fetch(self, source, window):
        row, col = window // self.cols, window % self.cols
        rows = pl.ds(row * WIN_LAT + WIN_LAT // 2, WIN_LAT)
        block = source[rows, pl.ds(col * WIN_LON + WIN_LON // 2, WIN_LON)]
        return block.reshape(block.shape[0] * block.shape[1] * block.shape[2], block.shape[3])


class Pipeline:
    def __init__(self, weights, flipped, normed, middle, tokens, keep):
        self.weights, self.tokens, self.keep = weights, tokens, keep
        self.flipped, self.normed, self.middle = flipped, normed, middle

    def prepare(self, step, blocks):
        flip = []
        weave(flip_steps(flip, blocks, self.weights))
        self.flipped[step % 2], self.normed[step % 2] = flip

    def advance(self, step, before=True, blocks=None):
        new, windows = [], []
        flip = self.flipped[step % 2], self.normed[step % 2]
        chains = [attention_steps(new, *flip, self.weights)]
        if before:
            last = self.middle[(step + 1) % 2]
            chains.insert(0, mlp_steps(windows, last, self.weights, self.tokens))
        weave(*chains)
        if blocks is not None:
            self.prepare(step + 1, blocks)
        if before:
            self.keep(step - 1, windows)
        self.middle[step % 2] = new[0]

    def finish(self, step):
        windows = []
        weave(mlp_steps(windows, self.middle[step % 2], self.weights, self.tokens))
        self.keep(step, windows)


def first_kernel(token):
    token[...] = jnp.zeros_like(token)


def table_kernel(levels, token, rel_bias, bias, padded, strips):
    bias_strips(rel_bias, padded, strips, levels)
    bias_table(strips, bias)


def early_kernel(
    sizes,
    mask, bias, fields, gain_one, w_qkv, w_proj, gain_two, w_up, w_down,
    results, middle, plan, ext, qkv_t, proj_t, up_t, down_t, gain_one_t, gain_two_t,
    flipped, normed, chains, halo_send, halo_recv,
):
    lat_cells, lon_cells, levels, features = fields.shape
    lat_half, lon_half = WIN_LAT // 2, WIN_LON // 2
    lat, lon = lax.axis_index("lat"), lax.axis_index("lon")
    lat_size, lon_size = lax.axis_size("lat"), lax.axis_size("lon")
    west, east = (lon + lon_size - 1) % lon_size, (lon + 1) % lon_size
    barrier = pltpu.get_barrier_semaphore()

    def greet(row, col):
        pl.semaphore_signal(barrier, inc=1, device_id=(row, col), device_id_type=MESH)

    greet(lat, east)

    @pl.when(lat < lat_size - 1)
    def _():
        greet(lat + 1, lon)
        greet(lat + 1, east)

    def transfer(which, source, target, row, col):
        return pltpu.make_async_remote_copy(
            src_ref=source, dst_ref=target,
            send_sem=halo_send.at[which], recv_sem=halo_recv.at[which],
            device_id=(row, col), device_id_type=MESH,
        )

    up = jnp.maximum(lat - 1, 0)
    below, beside = pl.ds(lat_cells, lat_half), pl.ds(lon_cells, lon_half)
    rows, cols = pl.ds(lat_half, lat_cells - lat_half), pl.ds(lon_half, lon_cells - lon_half)
    top, left = pl.ds(0, lat_half), pl.ds(0, lon_half)
    to_north = transfer(0, fields.at[top, cols], ext.at[below, cols], up, lon)
    to_west = transfer(1, fields.at[rows, left], ext.at[rows, beside], lat, west)
    to_corner = transfer(2, fields.at[top, left], ext.at[below, beside], up, west)

    def send_halos():
        @pl.when(lat > 0)
        def _():
            pl.semaphore_wait(barrier, 3)
            to_north.start()
            to_corner.start()

        @pl.when(lat == 0)
        def _():
            pl.semaphore_wait(barrier, 1)

        to_west.start()

    first_col = lon * sizes.cols
    total = jnp.int32(0)
    for place, inside_only in ((0, True), (1, False)):
        following = jnp.int32(sizes.count)
        chains[sizes.count] = following
        chains[sizes.count + 1] = following
        found = jnp.int32(0)
        for window in reversed(range(sizes.count)):
            if sizes.interior(window) == inside_only:
                ocean = mask[window // sizes.cols, first_col + window % sizes.cols]
                following = jnp.where(ocean == 1, window, following)
                found = found + ocean
            chains[window] = following
        plan[place] = found
        spot = following
        for n in range(sizes.count):
            plan[2 + place * sizes.count + n] = jnp.where(spot == sizes.count, 0, spot)
            spot = chains[spot + 1]

    for window in range(sizes.count):
        plan[2 + 2 * sizes.count + window] = mask[
            window // sizes.cols, first_col + window % sizes.cols
        ]
    gain_one_t[...] = jnp.broadcast_to(gain_one[...], (128, features)).T
    gain_two_t[...] = jnp.broadcast_to(gain_two[...] * ROOT_HALF, (128, features)).T
    for source, target in ((w_qkv, qkv_t), (w_proj, proj_t), (w_up, up_t), (w_down, down_t)):
        target[...] = source[...].T
    weights = dict(
        qkv=qkv_t, proj=proj_t, up=up_t, down=down_t,
        gain_one=gain_one_t, gain_two=gain_two_t, bias=bias,
    )

    def blocks(step):
        return [sizes.fetch(fields, plan[2 + step * PAIR + n]) for n in range(PAIR)]

    def keep(step, windows):
        for n, window in enumerate(windows):
            results[step * PAIR + n] = window.reshape(results.shape[1:])

    tokens = WIN_LAT * WIN_LON * levels
    line = Pipeline(weights, flipped, normed, middle, tokens, keep)
    line.prepare(0, blocks(0))
    line.advance(0, before=False, blocks=blocks(1))

    @pl.when(lon > 0)
    def _():
        send_halos()

    def early_step(step, carry):
        line.advance(step, blocks=blocks(step + 1))

        @pl.when((lon == 0) & (step == min(FIRST_SENDS, EARLY_PAIRS - 2)))
        def _():
            send_halos()

        return carry

    lax.fori_loop(1, EARLY_PAIRS - 1, early_step, 0)
    line.advance(EARLY_PAIRS - 1)
    ext[rows, cols] = fields[rows, cols]
    to_west.wait()

    @pl.when(lat > 0)
    def _():
        to_north.wait_send()
        to_corner.wait_send()

    @pl.when(lat < lat_size - 1)
    def _():
        to_north.wait_recv()
        to_corner.wait_recv()


def late_kernel(
    sizes,
    plan, results, before, ext,
    qkv_t, proj_t, up_t, down_t, gain_one_t, gain_two_t, bias,
    output, flipped, normed, middle, late, zero, sems,
):
    inside, edges = plan[0], plan[1]
    early = jnp.minimum(inside, sizes.early)
    rest = inside + edges - early
    pairs = (rest + PAIR - 1) // PAIR
    zero[...] = jnp.zeros_like(zero)

    def send(source, window):
        row, col = window // sizes.cols, window % sizes.cols
        target = output.at[pl.ds(row * WIN_LAT, WIN_LAT), pl.ds(col * WIN_LON, WIN_LON)]
        return pltpu.make_async_copy(source, target, sems.at[window])

    for window in range(sizes.count):

        @pl.when(plan[2 + 2 * sizes.count + window] == 0)
        def _():
            send(zero, window).start()

    def write_early(n, carry):
        send(results.at[n], plan[2 + n]).start()
        return carry

    ready = jnp.minimum(early, sizes.early - PAIR)
    lax.fori_loop(0, ready, write_early, 0)

    def window_of(n):
        n = jnp.clip(n, 0, sizes.count - 1)
        other = jnp.clip(early + n - edges, 0, sizes.count - 1)
        return jnp.where(n < edges, plan[2 + sizes.count + n], plan[2 + other])

    def blocks(step):
        first = (step - EARLY_PAIRS) * PAIR
        return [sizes.fetch(ext, window_of(first + n)) for n in range(PAIR)]

    def keep(step, windows):
        for n, window in enumerate(windows):
            place = (step - EARLY_PAIRS) * PAIR + n
            slot = (place + PAIR) % late.shape[0]
            late[slot] = window.reshape(zero.shape)

            @pl.when((place >= 0) & (place < rest))
            def _():
                send(late.at[slot], window_of(place)).start()

            @pl.when((place < 0) & (sizes.early + place < early))
            def _():
                send(late.at[slot], plan[2 + jnp.clip(sizes.early + place, 0, sizes.count - 1)]).start()

    weights = dict(
        qkv=qkv_t, proj=proj_t, up=up_t, down=down_t,
        gain_one=gain_one_t, gain_two=gain_two_t, bias=bias,
    )
    tokens = bias.shape[1]
    line = Pipeline(weights, flipped, normed, middle, tokens, keep)
    last = EARLY_PAIRS - 1
    middle[last % 2] = before[last % 2]
    line.prepare(EARLY_PAIRS, blocks(jnp.int32(EARLY_PAIRS)))

    def late_step(step, carry):
        line.advance(step, blocks=blocks(step + 1))
        return carry

    lax.fori_loop(EARLY_PAIRS, EARLY_PAIRS + pairs, late_step, 0)
    line.finish(last + pairs)

    def wait(window, carry):
        send(zero, window).wait()
        return carry

    lax.fori_loop(0, sizes.count, wait, 0)


def vmem():
    return pl.BlockSpec(memory_space=pltpu.VMEM)


def smem():
    return pl.BlockSpec(memory_space=pltpu.SMEM)


def any_space():
    return pl.BlockSpec(memory_space=pl.ANY)


def cost(flops, moved):
    return pl.CostEstimate(flops=flops, bytes_accessed=moved, transcendentals=0)


def body(fields, ocean_mask, gain_one, w_qkv, rel_bias, w_proj, gain_two, w_up, w_down):
    sizes = Sizes(fields.shape)
    lat_cells, lon_cells, levels, features = fields.shape
    heads, length = rel_bias.shape
    group = WIN_LON * levels
    tokens = WIN_LAT * group
    window = (WIN_LAT, WIN_LON, levels, features)
    bf16, f32 = jnp.bfloat16, jnp.float32
    shape = jax.ShapeDtypeStruct
    gains = [gain_one.reshape(1, -1), gain_two.reshape(1, -1)]
    sources = [w_qkv, w_proj, w_up, w_down]
    flips = [shape(w.shape[::-1], w.dtype) for w in sources]
    dma = pltpu.SemaphoreType.DMA
    token = pl.pallas_call(
        first_kernel,
        out_shape=shape((8, 128), f32),
        out_specs=vmem(),
        cost_estimate=cost(2**36, 2**26),
        compiler_params=pltpu.CompilerParams(vmem_limit_bytes=2**20),
    )()
    bias = pl.pallas_call(
        functools.partial(table_kernel, levels),
        out_shape=shape((heads // 2, tokens, 2 * tokens), f32),
        in_specs=[vmem()] * 2,
        out_specs=vmem(),
        scratch_shapes=[
            pltpu.VMEM((heads, (length + 255) // 128 * 128), f32),
            pltpu.VMEM((heads, group, 2 * tokens), f32),
        ],
        cost_estimate=cost(0, 2**10),
        compiler_params=pltpu.CompilerParams(vmem_limit_bytes=6 * 2**20),
    )(token, rel_bias)
    pair_shape = (2, features, PAIR * tokens)
    tables = [shape((features, 128), f32)] * 2
    outcome = pl.pallas_call(
        functools.partial(early_kernel, sizes),
        out_shape=[
            shape((sizes.early,) + window, bf16),
            shape(pair_shape, bf16),
            shape((2 + 3 * sizes.count,), jnp.int32),
            shape((lat_cells + WIN_LAT // 2, lon_cells + WIN_LON // 2, levels, features), bf16),
        ]
        + flips
        + tables,
        in_specs=[smem()] + [vmem()] * 8,
        out_specs=[vmem(), vmem(), smem()] + [vmem()] * 7,
        scratch_shapes=[
            pltpu.VMEM(pair_shape, bf16),
            pltpu.VMEM(pair_shape, bf16),
            pltpu.SMEM((sizes.count + 2,), jnp.int32),
            dma((3,)),
            dma((3,)),
        ],
        cost_estimate=cost(2**36, 2**26),
        compiler_params=pltpu.CompilerParams(
            collective_id=0, has_side_effects=True, vmem_limit_bytes=24 * 2**20
        ),
    )(ocean_mask, bias, fields, gains[0], w_qkv, w_proj, gains[1], w_up, w_down)
    results, middle, plan, ext = outcome[:4]
    return pl.pallas_call(
        functools.partial(late_kernel, sizes),
        out_shape=shape(fields.shape, fields.dtype),
        in_specs=[smem()] + [vmem()] * 10,
        out_specs=any_space(),
        scratch_shapes=[
            pltpu.VMEM(pair_shape, bf16),
            pltpu.VMEM(pair_shape, bf16),
            pltpu.VMEM(pair_shape, bf16),
            pltpu.VMEM((sizes.count + PAIR,) + window, bf16),
            pltpu.VMEM(window, bf16),
            dma((sizes.count,)),
        ],
        cost_estimate=cost(0, 4 * fields.size),
        compiler_params=pltpu.CompilerParams(vmem_limit_bytes=16 * 2**20),
    )(plan, results, middle, ext, *outcome[4:], bias)


def solution(mesh):
    in_specs = (P("lat", "lon", None, None), P("lat", None), P(), P(), P(), P(), P(), P(), P())
    out_specs = P("lat", "lon", None, None)
    return jax.shard_map(body, mesh=mesh, in_specs=in_specs, out_specs=out_specs, check_vma=False)
```

```python
import functools
import math

import jax
import jax.numpy as jnp
from jax import lax
from jax.experimental import pallas as pl
from jax.experimental.pallas import tpu as pltpu
from jax.sharding import PartitionSpec as P

WIN_LAT = 8
WIN_LON = 8
NORM_FLOOR = 0.25
MESH = pl.DeviceIdType.MESH
LOG2E = math.log2(math.e)
ROOT_HALF = math.sqrt(0.5)
PAIR = 2
EARLY_PAIRS = 5
MORE_PAIRS = 1
FIRST_SENDS = 2


def dot(left, right):
    return jnp.dot(left, right, preferred_element_type=jnp.float32)


def normalise(values, gain):
    share = 1.0 / values.shape[0]
    average = jnp.sum(values, axis=0, keepdims=True) * share
    centred = values - average
    spread = jnp.sum(centred * centred, axis=0, keepdims=True) * share
    return (centred * lax.rsqrt(spread + NORM_FLOOR) * gain).astype(jnp.bfloat16)


def wide(gain, columns):
    return jnp.concatenate([gain] * (columns // gain.shape[1]), axis=1)


def flip_steps(store, blocks, weights):
    flipped = jnp.concatenate([block.T for block in blocks], axis=1)
    gain = wide(weights["gain_one"][...], flipped.shape[1])
    store.extend([flipped, normalise(flipped.astype(jnp.float32), gain)])
    yield


def attention_steps(store, flipped, normed, weights):
    qkv_t, proj_t, bias = weights["qkv"], weights["proj"], weights["bias"]
    features, columns = normed.shape
    half, tokens, _ = bias.shape
    dim = features // (2 * half)
    scale = LOG2E / math.sqrt(dim)
    key_t = dot(qkv_t[features : 2 * features], normed).astype(jnp.bfloat16)
    yield
    query_t = (dot(qkv_t[:features], normed) * scale).astype(jnp.bfloat16)
    yield
    value_t = dot(qkv_t[2 * features :], normed).astype(jnp.bfloat16)
    yield
    lane_head = lax.broadcasted_iota(jnp.int32, (tokens, features), 1) // dim % half
    nothing = jnp.zeros((features // 2, tokens), jnp.bfloat16)
    ones = jnp.ones((16, tokens), jnp.bfloat16)
    spans = [slice(n, n + tokens) for n in range(0, columns, tokens)]
    every = []
    for lanes in spans:
        key = key_t[:, lanes].T
        masked = [jnp.where(lane_head == h, key, jnp.zeros_like(key)) for h in range(half)]
        upper = jnp.concatenate([query_t[: features // 2, lanes], nothing], axis=1)
        lower = jnp.concatenate([nothing, query_t[features // 2 :, lanes]], axis=1)
        every.append(dot(jnp.concatenate(masked, axis=0), jnp.concatenate([upper, lower], axis=0)))
        yield
    mixed = []
    for lanes, products in zip(spans, every):
        first, second = [], []
        for h in range(half):
            scores = products[h * tokens : (h + 1) * tokens] + bias[h]
            power = jnp.exp2(scores - jnp.max(scores, axis=0, keepdims=True)).astype(jnp.bfloat16)
            one, two = h * dim, (h + half) * dim
            rows = [value_t[one : one + dim, lanes], value_t[two : two + dim, lanes], ones]
            piece = dot(jnp.concatenate(rows, axis=0), power)
            share = 1.0 / piece[2 * dim : 2 * dim + 1]
            first.append((piece[:dim, :tokens] * share[:, :tokens]).astype(jnp.bfloat16))
            second.append((piece[dim : 2 * dim, tokens:] * share[:, tokens:]).astype(jnp.bfloat16))
            yield
        mixed.append(jnp.concatenate(first + second, axis=0))
    projected = dot(proj_t[...], jnp.concatenate(mixed, axis=1))
    store.append((flipped.astype(jnp.float32) + projected).astype(jnp.bfloat16))
    yield


def mlp_steps(store, middle, weights, tokens):
    up_t, down_t, gain = weights["up"], weights["down"], weights["gain_two"]
    features, hidden = middle.shape[0], up_t.shape[0]
    residual = middle.astype(jnp.float32)
    normed = normalise(residual, wide(gain[...], middle.shape[1]))
    yield
    total = None
    for part in range(hidden // features):
        rows = slice(part * features, (part + 1) * features)
        grown = dot(up_t[rows], normed)
        yield
        grown = (grown * (1.0 + lax.erf(grown))).astype(jnp.bfloat16)
        piece = dot(down_t[:, rows], grown)
        total = piece if total is None else total + piece
        yield
    result = (residual + total * ROOT_HALF).astype(jnp.bfloat16)
    for n in range(middle.shape[1] // tokens):
        store.append(result[:, n * tokens : (n + 1) * tokens].T)
    yield


def weave(*steps):
    steps = list(steps)
    while steps:
        for chain in list(steps):
            try:
                next(chain)
            except StopIteration:
                steps.remove(chain)


def bias_strips(rel_bias, padded, strips, levels):
    heads, length = rel_bias.shape
    col_step = 2 * levels - 1
    row_step = (2 * WIN_LON - 1) * col_step
    offsets = [c * col_step + lev for c in range(WIN_LON) for lev in range(levels)]
    top = offsets[-1]
    width = padded.shape[1] - 128
    padded[...] = jnp.zeros_like(padded)
    padded[:, :length] = rel_bias[...] * LOG2E
    table = padded[...]
    left = jnp.concatenate([table[:, top - q : top - q + width] for q in offsets], axis=0)
    group = WIN_LON * levels
    lane = lax.broadcasted_iota(jnp.int32, (width, strips.shape[2]), 1)
    inner = lane % group
    target = lane // group * row_step + inner // levels * col_step + inner % levels
    pick = lax.broadcasted_iota(jnp.int32, target.shape, 0) == target
    found = jnp.dot(
        left,
        pick.astype(jnp.float32),
        precision=lax.Precision.HIGHEST,
        preferred_element_type=jnp.float32,
    )
    for place in range(group):
        strips[:, place, :] = found[place * heads : (place + 1) * heads]


def bias_table(strips, bias):
    heads, group, _ = strips.shape
    tokens = WIN_LAT * group
    for row in range(WIN_LAT):
        first = (WIN_LAT - 1 - row) * group
        piece = strips[:, :, first : first + tokens]
        places = slice(row * group, (row + 1) * group)
        bias[:, places, :tokens] = piece[: heads // 2]
        bias[:, places, tokens:] = piece[heads // 2 :]


class Sizes:
    def __init__(self, fields_shape):
        self.rows = fields_shape[0] // WIN_LAT
        self.cols = fields_shape[1] // WIN_LON
        self.count = self.rows * self.cols
        self.early = (EARLY_PAIRS + MORE_PAIRS) * PAIR

    def interior(self, window):
        return window // self.cols < self.rows - 1 and window % self.cols < self.cols - 1

    def fetch(self, source, window):
        row, col = window // self.cols, window % self.cols
        rows = pl.ds(row * WIN_LAT + WIN_LAT // 2, WIN_LAT)
        block = source[rows, pl.ds(col * WIN_LON + WIN_LON // 2, WIN_LON)]
        return block.reshape(block.shape[0] * block.shape[1] * block.shape[2], block.shape[3])


class Pipeline:
    def __init__(self, weights, flipped, normed, middle, tokens, keep):
        self.weights, self.tokens, self.keep = weights, tokens, keep
        self.flipped, self.normed, self.middle = flipped, normed, middle

    def prepare(self, step, blocks):
        flip = []
        weave(flip_steps(flip, blocks, self.weights))
        self.flipped[step % 2], self.normed[step % 2] = flip

    def advance(self, step, before=True, blocks=None):
        new, windows = [], []
        flip = self.flipped[step % 2], self.normed[step % 2]
        chains = [attention_steps(new, *flip, self.weights)]
        if before:
            last = self.middle[(step + 1) % 2]
            chains.insert(0, mlp_steps(windows, last, self.weights, self.tokens))
        weave(*chains)
        if blocks is not None:
            self.prepare(step + 1, blocks)
        if before:
            self.keep(step - 1, windows)
        self.middle[step % 2] = new[0]

    def finish(self, step):
        windows = []
        weave(mlp_steps(windows, self.middle[step % 2], self.weights, self.tokens))
        self.keep(step, windows)


def first_kernel(token):
    token[...] = jnp.zeros_like(token)


def table_kernel(levels, token, rel_bias, bias, padded, strips):
    bias_strips(rel_bias, padded, strips, levels)
    bias_table(strips, bias)


def early_kernel(
    sizes,
    mask, bias, fields, gain_one, w_qkv, w_proj, gain_two, w_up, w_down,
    results, middle, plan, ext, qkv_t, proj_t, up_t, down_t, gain_one_t, gain_two_t,
    flipped, normed, chains, halo_send, halo_recv,
):
    lat_cells, lon_cells, levels, features = fields.shape
    lat_half, lon_half = WIN_LAT // 2, WIN_LON // 2
    lat, lon = lax.axis_index("lat"), lax.axis_index("lon")
    lat_size, lon_size = lax.axis_size("lat"), lax.axis_size("lon")
    west, east = (lon + lon_size - 1) % lon_size, (lon + 1) % lon_size
    barrier = pltpu.get_barrier_semaphore()

    def greet(row, col):
        pl.semaphore_signal(barrier, inc=1, device_id=(row, col), device_id_type=MESH)

    greet(lat, east)

    @pl.when(lat < lat_size - 1)
    def _():
        greet(lat + 1, lon)
        greet(lat + 1, east)

    def transfer(which, source, target, row, col):
        return pltpu.make_async_remote_copy(
            src_ref=source, dst_ref=target,
            send_sem=halo_send.at[which], recv_sem=halo_recv.at[which],
            device_id=(row, col), device_id_type=MESH,
        )

    up = jnp.maximum(lat - 1, 0)
    below, beside = pl.ds(lat_cells, lat_half), pl.ds(lon_cells, lon_half)
    rows, cols = pl.ds(lat_half, lat_cells - lat_half), pl.ds(lon_half, lon_cells - lon_half)
    top, left = pl.ds(0, lat_half), pl.ds(0, lon_half)
    to_north = transfer(0, fields.at[top, cols], ext.at[below, cols], up, lon)
    to_west = transfer(1, fields.at[rows, left], ext.at[rows, beside], lat, west)
    to_corner = transfer(2, fields.at[top, left], ext.at[below, beside], up, west)

    def send_halos():
        @pl.when(lat > 0)
        def _():
            pl.semaphore_wait(barrier, 3)
            to_north.start()
            to_corner.start()

        @pl.when(lat == 0)
        def _():
            pl.semaphore_wait(barrier, 1)

        to_west.start()

    first_col = lon * sizes.cols
    total = jnp.int32(0)
    for place, inside_only in ((0, True), (1, False)):
        following = jnp.int32(sizes.count)
        chains[sizes.count] = following
        chains[sizes.count + 1] = following
        found = jnp.int32(0)
        for window in reversed(range(sizes.count)):
            if sizes.interior(window) == inside_only:
                ocean = mask[window // sizes.cols, first_col + window % sizes.cols]
                following = jnp.where(ocean == 1, window, following)
                found = found + ocean
            chains[window] = following
        plan[place] = found
        spot = following
        for n in range(sizes.count):
            plan[2 + place * sizes.count + n] = jnp.where(spot == sizes.count, 0, spot)
            spot = chains[spot + 1]

    for window in range(sizes.count):
        plan[2 + 2 * sizes.count + window] = mask[
            window // sizes.cols, first_col + window % sizes.cols
        ]
    early_pairs = jnp.where(lon == 0, EARLY_PAIRS + MORE_PAIRS, EARLY_PAIRS)
    plan[2 + 3 * sizes.count] = early_pairs
    gain_one_t[...] = jnp.broadcast_to(gain_one[...], (128, features)).T
    gain_two_t[...] = jnp.broadcast_to(gain_two[...] * ROOT_HALF, (128, features)).T
    for source, target in ((w_qkv, qkv_t), (w_proj, proj_t), (w_up, up_t), (w_down, down_t)):
        target[...] = source[...].T
    weights = dict(
        qkv=qkv_t, proj=proj_t, up=up_t, down=down_t,
        gain_one=gain_one_t, gain_two=gain_two_t, bias=bias,
    )

    def blocks(step):
        return [sizes.fetch(fields, plan[2 + step * PAIR + n]) for n in range(PAIR)]

    def keep(step, windows):
        for n, window in enumerate(windows):
            results[step * PAIR + n] = window.reshape(results.shape[1:])

    tokens = WIN_LAT * WIN_LON * levels
    line = Pipeline(weights, flipped, normed, middle, tokens, keep)
    line.prepare(0, blocks(0))
    line.advance(0, before=False, blocks=blocks(1))

    @pl.when(lon > 0)
    def _():
        send_halos()

    def early_step(step, carry):
        line.advance(step, blocks=blocks(step + 1))

        @pl.when((lon == 0) & (step == min(FIRST_SENDS, EARLY_PAIRS - 2)))
        def _():
            send_halos()

        return carry

    lax.fori_loop(1, early_pairs - 1, early_step, 0)
    line.advance(early_pairs - 1)
    ext[rows, cols] = fields[rows, cols]
    to_west.wait()

    @pl.when(lat > 0)
    def _():
        to_north.wait_send()
        to_corner.wait_send()

    @pl.when(lat < lat_size - 1)
    def _():
        to_north.wait_recv()
        to_corner.wait_recv()


def late_kernel(
    sizes,
    plan, results, before, ext,
    qkv_t, proj_t, up_t, down_t, gain_one_t, gain_two_t, bias,
    output, flipped, normed, middle, late, zero, sems,
):
    inside, edges, lead = plan[0], plan[1], plan[2 + 3 * sizes.count]
    early = jnp.minimum(inside, lead * PAIR)
    rest = inside + edges - early
    pairs = (rest + PAIR - 1) // PAIR
    zero[...] = jnp.zeros_like(zero)

    def send(source, window):
        row, col = window // sizes.cols, window % sizes.cols
        target = output.at[pl.ds(row * WIN_LAT, WIN_LAT), pl.ds(col * WIN_LON, WIN_LON)]
        return pltpu.make_async_copy(source, target, sems.at[window])

    for window in range(sizes.count):

        @pl.when(plan[2 + 2 * sizes.count + window] == 0)
        def _():
            send(zero, window).start()

    def write_early(n, carry):
        send(results.at[n], plan[2 + n]).start()
        return carry

    ready = jnp.minimum(early, (lead - 1) * PAIR)
    lax.fori_loop(0, ready, write_early, 0)

    def window_of(n):
        n = jnp.clip(n, 0, sizes.count - 1)
        other = jnp.clip(early + n - edges, 0, sizes.count - 1)
        return jnp.where(n < edges, plan[2 + sizes.count + n], plan[2 + other])

    def blocks(step):
        first = (step - lead) * PAIR
        return [sizes.fetch(ext, window_of(first + n)) for n in range(PAIR)]

    def keep(step, windows):
        for n, window in enumerate(windows):
            place = (step - lead) * PAIR + n
            slot = (place + PAIR) % late.shape[0]
            late[slot] = window.reshape(zero.shape)

            @pl.when((place >= 0) & (place < rest))
            def _():
                send(late.at[slot], window_of(place)).start()

            older = lead * PAIR + place

            @pl.when((place < 0) & (older < early))
            def _():
                send(late.at[slot], plan[2 + jnp.clip(older, 0, sizes.count - 1)]).start()

    weights = dict(
        qkv=qkv_t, proj=proj_t, up=up_t, down=down_t,
        gain_one=gain_one_t, gain_two=gain_two_t, bias=bias,
    )
    tokens = bias.shape[1]
    line = Pipeline(weights, flipped, normed, middle, tokens, keep)
    last = lead - 1
    middle[last % 2] = before[last % 2]
    line.prepare(lead, blocks(lead))

    def late_step(step, carry):
        line.advance(step, blocks=blocks(step + 1))
        return carry

    lax.fori_loop(lead, lead + pairs, late_step, 0)
    line.finish(last + pairs)

    def wait(window, carry):
        send(zero, window).wait()
        return carry

    lax.fori_loop(0, sizes.count, wait, 0)


def vmem():
    return pl.BlockSpec(memory_space=pltpu.VMEM)


def smem():
    return pl.BlockSpec(memory_space=pltpu.SMEM)


def any_space():
    return pl.BlockSpec(memory_space=pl.ANY)


def cost(flops, moved):
    return pl.CostEstimate(flops=flops, bytes_accessed=moved, transcendentals=0)


def body(fields, ocean_mask, gain_one, w_qkv, rel_bias, w_proj, gain_two, w_up, w_down):
    sizes = Sizes(fields.shape)
    lat_cells, lon_cells, levels, features = fields.shape
    heads, length = rel_bias.shape
    group = WIN_LON * levels
    tokens = WIN_LAT * group
    window = (WIN_LAT, WIN_LON, levels, features)
    bf16, f32 = jnp.bfloat16, jnp.float32
    shape = jax.ShapeDtypeStruct
    gains = [gain_one.reshape(1, -1), gain_two.reshape(1, -1)]
    sources = [w_qkv, w_proj, w_up, w_down]
    flips = [shape(w.shape[::-1], w.dtype) for w in sources]
    dma = pltpu.SemaphoreType.DMA
    token = pl.pallas_call(
        first_kernel,
        out_shape=shape((8, 128), f32),
        out_specs=vmem(),
        cost_estimate=cost(2**36, 2**26),
        compiler_params=pltpu.CompilerParams(vmem_limit_bytes=2**20),
    )()
    bias = pl.pallas_call(
        functools.partial(table_kernel, levels),
        out_shape=shape((heads // 2, tokens, 2 * tokens), f32),
        in_specs=[vmem()] * 2,
        out_specs=vmem(),
        scratch_shapes=[
            pltpu.VMEM((heads, (length + 255) // 128 * 128), f32),
            pltpu.VMEM((heads, group, 2 * tokens), f32),
        ],
        cost_estimate=cost(0, 2**10),
        compiler_params=pltpu.CompilerParams(vmem_limit_bytes=6 * 2**20),
    )(token, rel_bias)
    pair_shape = (2, features, PAIR * tokens)
    tables = [shape((features, 128), f32)] * 2
    outcome = pl.pallas_call(
        functools.partial(early_kernel, sizes),
        out_shape=[
            shape((sizes.early,) + window, bf16),
            shape(pair_shape, bf16),
            shape((3 + 3 * sizes.count,), jnp.int32),
            shape((lat_cells + WIN_LAT // 2, lon_cells + WIN_LON // 2, levels, features), bf16),
        ]
        + flips
        + tables,
        in_specs=[smem()] + [vmem()] * 8,
        out_specs=[vmem(), vmem(), smem()] + [vmem()] * 7,
        scratch_shapes=[
            pltpu.VMEM(pair_shape, bf16),
            pltpu.VMEM(pair_shape, bf16),
            pltpu.SMEM((sizes.count + 2,), jnp.int32),
            dma((3,)),
            dma((3,)),
        ],
        cost_estimate=cost(2**36, 2**26),
        compiler_params=pltpu.CompilerParams(
            collective_id=0, has_side_effects=True, vmem_limit_bytes=24 * 2**20
        ),
    )(ocean_mask, bias, fields, gains[0], w_qkv, w_proj, gains[1], w_up, w_down)
    results, middle, plan, ext = outcome[:4]
    return pl.pallas_call(
        functools.partial(late_kernel, sizes),
        out_shape=shape(fields.shape, fields.dtype),
        in_specs=[smem()] + [vmem()] * 10,
        out_specs=any_space(),
        scratch_shapes=[
            pltpu.VMEM(pair_shape, bf16),
            pltpu.VMEM(pair_shape, bf16),
            pltpu.VMEM(pair_shape, bf16),
            pltpu.VMEM((sizes.count + PAIR,) + window, bf16),
            pltpu.VMEM(window, bf16),
            dma((sizes.count,)),
        ],
        cost_estimate=cost(0, 4 * fields.size),
        compiler_params=pltpu.CompilerParams(vmem_limit_bytes=16 * 2**20),
    )(plan, results, middle, ext, *outcome[4:], bias)


def solution(mesh):
    in_specs = (P("lat", "lon", None, None), P("lat", None), P(), P(), P(), P(), P(), P(), P())
    out_specs = P("lat", "lon", None, None)
    return jax.shard_map(body, mesh=mesh, in_specs=in_specs, out_specs=out_specs, check_vma=False)
```

```python
import functools
import math

import jax
import jax.numpy as jnp
from jax import lax
from jax.experimental import pallas as pl
from jax.experimental.pallas import tpu as pltpu
from jax.sharding import PartitionSpec as P

WIN_LAT = 8
WIN_LON = 8
NORM_FLOOR = 0.25
MESH = pl.DeviceIdType.MESH
LOG2E = math.log2(math.e)
ROOT_HALF = math.sqrt(0.5)
PAIR = 2
EARLY_PAIRS = 5
MORE_PAIRS = 1
FIRST_SENDS = 2


def dot(left, right):
    return jnp.dot(left, right, preferred_element_type=jnp.float32)


def normalise(values, gain):
    share = 1.0 / values.shape[0]
    average = jnp.sum(values, axis=0, keepdims=True) * share
    centred = values - average
    spread = jnp.sum(centred * centred, axis=0, keepdims=True) * share
    return (centred * lax.rsqrt(spread + NORM_FLOOR) * gain).astype(jnp.bfloat16)


def wide(gain, columns):
    return jnp.concatenate([gain] * (columns // gain.shape[1]), axis=1)


def flip_steps(store, blocks, weights):
    flipped = jnp.concatenate([block.T for block in blocks], axis=1)
    gain = wide(weights["gain_one"][...], flipped.shape[1])
    store.extend([flipped, normalise(flipped.astype(jnp.float32), gain)])
    yield


def attention_steps(store, flipped, normed, weights):
    qkv_t, proj_t, bias = weights["qkv"], weights["proj"], weights["bias"]
    features, columns = normed.shape
    half, tokens, _ = bias.shape
    dim = features // (2 * half)
    scale = LOG2E / math.sqrt(dim)
    key_t = dot(qkv_t[features : 2 * features], normed).astype(jnp.bfloat16)
    yield
    query_t = (dot(qkv_t[:features], normed) * scale).astype(jnp.bfloat16)
    yield
    value_t = dot(qkv_t[2 * features :], normed).astype(jnp.bfloat16)
    yield
    lane_head = lax.broadcasted_iota(jnp.int32, (tokens, features), 1) // dim % half
    nothing = jnp.zeros((features // 2, tokens), jnp.bfloat16)
    ones = jnp.ones((16, tokens), jnp.bfloat16)
    spans = [slice(n, n + tokens) for n in range(0, columns, tokens)]
    every = []
    for lanes in spans:
        key = key_t[:, lanes].T
        masked = [jnp.where(lane_head == h, key, jnp.zeros_like(key)) for h in range(half)]
        upper = jnp.concatenate([query_t[: features // 2, lanes], nothing], axis=1)
        lower = jnp.concatenate([nothing, query_t[features // 2 :, lanes]], axis=1)
        every.append(dot(jnp.concatenate(masked, axis=0), jnp.concatenate([upper, lower], axis=0)))
        yield
    mixed = []
    for lanes, products in zip(spans, every):
        first, second = [], []
        for h in range(half):
            scores = products[h * tokens : (h + 1) * tokens] + bias[h]
            power = jnp.exp2(scores - jnp.max(scores, axis=0, keepdims=True)).astype(jnp.bfloat16)
            one, two = h * dim, (h + half) * dim
            rows = [value_t[one : one + dim, lanes], value_t[two : two + dim, lanes], ones]
            piece = dot(jnp.concatenate(rows, axis=0), power)
            share = 1.0 / piece[2 * dim : 2 * dim + 1]
            first.append((piece[:dim, :tokens] * share[:, :tokens]).astype(jnp.bfloat16))
            second.append((piece[dim : 2 * dim, tokens:] * share[:, tokens:]).astype(jnp.bfloat16))
            yield
        mixed.append(jnp.concatenate(first + second, axis=0))
    projected = dot(proj_t[...], jnp.concatenate(mixed, axis=1))
    store.append((flipped.astype(jnp.float32) + projected).astype(jnp.bfloat16))
    yield


def mlp_steps(store, middle, weights, tokens):
    up_t, down_t, gain = weights["up"], weights["down"], weights["gain_two"]
    features, hidden = middle.shape[0], up_t.shape[0]
    residual = middle.astype(jnp.float32)
    normed = normalise(residual, wide(gain[...], middle.shape[1]))
    yield
    total = None
    for part in range(hidden // features):
        rows = slice(part * features, (part + 1) * features)
        grown = dot(up_t[rows], normed)
        yield
        grown = (grown * (1.0 + lax.erf(grown))).astype(jnp.bfloat16)
        piece = dot(down_t[:, rows], grown)
        total = piece if total is None else total + piece
        yield
    result = (residual + total * ROOT_HALF).astype(jnp.bfloat16)
    for n in range(middle.shape[1] // tokens):
        store.append(result[:, n * tokens : (n + 1) * tokens].T)
    yield


def weave(*steps):
    steps = list(steps)
    while steps:
        for chain in list(steps):
            try:
                next(chain)
            except StopIteration:
                steps.remove(chain)


def bias_strips(rel_bias, padded, strips, levels):
    heads, length = rel_bias.shape
    col_step = 2 * levels - 1
    row_step = (2 * WIN_LON - 1) * col_step
    offsets = [c * col_step + lev for c in range(WIN_LON) for lev in range(levels)]
    top = offsets[-1]
    width = padded.shape[1] - 128
    padded[...] = jnp.zeros_like(padded)
    padded[:, :length] = rel_bias[...] * LOG2E
    table = padded[...]
    left = jnp.concatenate([table[:, top - q : top - q + width] for q in offsets], axis=0)
    group = WIN_LON * levels
    lane = lax.broadcasted_iota(jnp.int32, (width, strips.shape[2]), 1)
    inner = lane % group
    target = lane // group * row_step + inner // levels * col_step + inner % levels
    pick = lax.broadcasted_iota(jnp.int32, target.shape, 0) == target
    found = jnp.dot(
        left,
        pick.astype(jnp.float32),
        precision=lax.Precision.HIGHEST,
        preferred_element_type=jnp.float32,
    )
    for place in range(group):
        strips[:, place, :] = found[place * heads : (place + 1) * heads]


def bias_table(strips, bias):
    heads, group, _ = strips.shape
    tokens = WIN_LAT * group
    for row in range(WIN_LAT):
        first = (WIN_LAT - 1 - row) * group
        piece = strips[:, :, first : first + tokens]
        places = slice(row * group, (row + 1) * group)
        bias[:, places, :tokens] = piece[: heads // 2]
        bias[:, places, tokens:] = piece[heads // 2 :]


class Sizes:
    def __init__(self, fields_shape):
        self.rows = fields_shape[0] // WIN_LAT
        self.cols = fields_shape[1] // WIN_LON
        self.count = self.rows * self.cols
        self.early = (EARLY_PAIRS + MORE_PAIRS) * PAIR

    def interior(self, window):
        return window // self.cols < self.rows - 1 and window % self.cols < self.cols - 1

    def fetch(self, source, window):
        row, col = window // self.cols, window % self.cols
        rows = pl.ds(row * WIN_LAT + WIN_LAT // 2, WIN_LAT)
        block = source[rows, pl.ds(col * WIN_LON + WIN_LON // 2, WIN_LON)]
        return block.reshape(block.shape[0] * block.shape[1] * block.shape[2], block.shape[3])


class Pipeline:
    def __init__(self, weights, flipped, normed, middle, tokens, keep):
        self.weights, self.tokens, self.keep = weights, tokens, keep
        self.flipped, self.normed, self.middle = flipped, normed, middle

    def prepare(self, step, blocks):
        flip = []
        weave(flip_steps(flip, blocks, self.weights))
        self.flipped[step % 2], self.normed[step % 2] = flip

    def advance(self, step, before=True, blocks=None):
        new, windows = [], []
        flip = self.flipped[step % 2], self.normed[step % 2]
        chains = [attention_steps(new, *flip, self.weights)]
        if before:
            last = self.middle[(step + 1) % 2]
            chains.insert(0, mlp_steps(windows, last, self.weights, self.tokens))
        weave(*chains)
        if blocks is not None:
            self.prepare(step + 1, blocks)
        if before:
            self.keep(step - 1, windows)
        self.middle[step % 2] = new[0]

    def finish(self, step):
        windows = []
        weave(mlp_steps(windows, self.middle[step % 2], self.weights, self.tokens))
        self.keep(step, windows)


def first_kernel(token):
    token[...] = jnp.zeros_like(token)


def table_kernel(levels, token, rel_bias, bias, padded, strips):
    bias_strips(rel_bias, padded, strips, levels)
    bias_table(strips, bias)


def early_kernel(
    sizes,
    mask, bias, fields, gain_one, w_qkv, w_proj, gain_two, w_up, w_down,
    results, middle, plan, ext, qkv_t, proj_t, up_t, down_t, gain_one_t, gain_two_t,
    flipped, normed, chains, halo_send, halo_recv,
):
    lat_cells, lon_cells, levels, features = fields.shape
    lat_half, lon_half = WIN_LAT // 2, WIN_LON // 2
    lat, lon = lax.axis_index("lat"), lax.axis_index("lon")
    lat_size, lon_size = lax.axis_size("lat"), lax.axis_size("lon")
    west, east = (lon + lon_size - 1) % lon_size, (lon + 1) % lon_size
    barrier = pltpu.get_barrier_semaphore()

    def greet(row, col):
        pl.semaphore_signal(barrier, inc=1, device_id=(row, col), device_id_type=MESH)

    greet(lat, east)

    @pl.when(lat < lat_size - 1)
    def _():
        greet(lat + 1, lon)
        greet(lat + 1, east)

    def transfer(which, source, target, row, col):
        return pltpu.make_async_remote_copy(
            src_ref=source, dst_ref=target,
            send_sem=halo_send.at[which], recv_sem=halo_recv.at[which],
            device_id=(row, col), device_id_type=MESH,
        )

    up = jnp.maximum(lat - 1, 0)
    below, beside = pl.ds(lat_cells, lat_half), pl.ds(lon_cells, lon_half)
    rows, cols = pl.ds(lat_half, lat_cells - lat_half), pl.ds(lon_half, lon_cells - lon_half)
    top, left = pl.ds(0, lat_half), pl.ds(0, lon_half)
    to_north = transfer(0, fields.at[top, cols], ext.at[below, cols], up, lon)
    to_west = transfer(1, fields.at[rows, left], ext.at[rows, beside], lat, west)
    to_corner = transfer(2, fields.at[top, left], ext.at[below, beside], up, west)

    def send_halos():
        @pl.when(lat > 0)
        def _():
            pl.semaphore_wait(barrier, 3)
            to_north.start()
            to_corner.start()

        @pl.when(lat == 0)
        def _():
            pl.semaphore_wait(barrier, 1)

        to_west.start()

    first_col = lon * sizes.cols
    total = jnp.int32(0)
    for place, inside_only in ((0, True), (1, False)):
        following = jnp.int32(sizes.count)
        chains[sizes.count] = following
        chains[sizes.count + 1] = following
        found = jnp.int32(0)
        for window in reversed(range(sizes.count)):
            if sizes.interior(window) == inside_only:
                ocean = mask[window // sizes.cols, first_col + window % sizes.cols]
                following = jnp.where(ocean == 1, window, following)
                found = found + ocean
            chains[window] = following
        plan[place] = found
        spot = following
        for n in range(sizes.count):
            plan[2 + place * sizes.count + n] = jnp.where(spot == sizes.count, 0, spot)
            spot = chains[spot + 1]

    for window in range(sizes.count):
        plan[2 + 2 * sizes.count + window] = mask[
            window // sizes.cols, first_col + window % sizes.cols
        ]
    early_pairs = jnp.where(lon == 0, EARLY_PAIRS + MORE_PAIRS, EARLY_PAIRS)
    plan[2 + 3 * sizes.count] = early_pairs
    gain_one_t[...] = jnp.broadcast_to(gain_one[...], (128, features)).T
    gain_two_t[...] = jnp.broadcast_to(gain_two[...] * ROOT_HALF, (128, features)).T
    for source, target in ((w_qkv, qkv_t), (w_proj, proj_t), (w_up, up_t), (w_down, down_t)):
        target[...] = source[...].T
    weights = dict(
        qkv=qkv_t, proj=proj_t, up=up_t, down=down_t,
        gain_one=gain_one_t, gain_two=gain_two_t, bias=bias,
    )

    def blocks(step):
        return [sizes.fetch(fields, plan[2 + step * PAIR + n]) for n in range(PAIR)]

    def keep(step, windows):
        for n, window in enumerate(windows):
            results[step * PAIR + n] = window.reshape(results.shape[1:])

    tokens = WIN_LAT * WIN_LON * levels
    line = Pipeline(weights, flipped, normed, middle, tokens, keep)
    line.prepare(0, blocks(0))
    line.advance(0, before=False, blocks=blocks(1))

    @pl.when(lon > 0)
    def _():
        send_halos()

    def early_step(step, carry):
        line.advance(step, blocks=blocks(step + 1))

        @pl.when((lon == 0) & (step == jnp.where(lat == 0, min(FIRST_SENDS, EARLY_PAIRS - 2), 1)))
        def _():
            send_halos()

        return carry

    lax.fori_loop(1, early_pairs - 1, early_step, 0)
    line.advance(early_pairs - 1)
    ext[rows, cols] = fields[rows, cols]
    to_west.wait()

    @pl.when(lat > 0)
    def _():
        to_north.wait_send()
        to_corner.wait_send()

    @pl.when(lat < lat_size - 1)
    def _():
        to_north.wait_recv()
        to_corner.wait_recv()


def late_kernel(
    sizes,
    plan, results, before, ext,
    qkv_t, proj_t, up_t, down_t, gain_one_t, gain_two_t, bias,
    output, flipped, normed, middle, late, zero, sems,
):
    inside, edges, lead = plan[0], plan[1], plan[2 + 3 * sizes.count]
    early = jnp.minimum(inside, lead * PAIR)
    rest = inside + edges - early
    pairs = (rest + PAIR - 1) // PAIR
    zero[...] = jnp.zeros_like(zero)

    def send(source, window):
        row, col = window // sizes.cols, window % sizes.cols
        target = output.at[pl.ds(row * WIN_LAT, WIN_LAT), pl.ds(col * WIN_LON, WIN_LON)]
        return pltpu.make_async_copy(source, target, sems.at[window])

    for window in range(sizes.count):

        @pl.when(plan[2 + 2 * sizes.count + window] == 0)
        def _():
            send(zero, window).start()

    def write_early(n, carry):
        send(results.at[n], plan[2 + n]).start()
        return carry

    ready = jnp.minimum(early, (lead - 1) * PAIR)
    lax.fori_loop(0, ready, write_early, 0)

    def window_of(n):
        n = jnp.clip(n, 0, sizes.count - 1)
        other = jnp.clip(early + n - edges, 0, sizes.count - 1)
        return jnp.where(n < edges, plan[2 + sizes.count + n], plan[2 + other])

    def blocks(step):
        first = (step - lead) * PAIR
        return [sizes.fetch(ext, window_of(first + n)) for n in range(PAIR)]

    def keep(step, windows):
        for n, window in enumerate(windows):
            place = (step - lead) * PAIR + n
            slot = (place + PAIR) % late.shape[0]
            late[slot] = window.reshape(zero.shape)

            @pl.when((place >= 0) & (place < rest))
            def _():
                send(late.at[slot], window_of(place)).start()

            older = lead * PAIR + place

            @pl.when((place < 0) & (older < early))
            def _():
                send(late.at[slot], plan[2 + jnp.clip(older, 0, sizes.count - 1)]).start()

    weights = dict(
        qkv=qkv_t, proj=proj_t, up=up_t, down=down_t,
        gain_one=gain_one_t, gain_two=gain_two_t, bias=bias,
    )
    tokens = bias.shape[1]
    line = Pipeline(weights, flipped, normed, middle, tokens, keep)
    last = lead - 1
    middle[last % 2] = before[last % 2]
    line.prepare(lead, blocks(lead))

    def late_step(step, carry):
        line.advance(step, blocks=blocks(step + 1))
        return carry

    lax.fori_loop(lead, lead + pairs, late_step, 0)
    line.finish(last + pairs)

    def wait(window, carry):
        send(zero, window).wait()
        return carry

    lax.fori_loop(0, sizes.count, wait, 0)


def vmem():
    return pl.BlockSpec(memory_space=pltpu.VMEM)


def smem():
    return pl.BlockSpec(memory_space=pltpu.SMEM)


def any_space():
    return pl.BlockSpec(memory_space=pl.ANY)


def cost(flops, moved):
    return pl.CostEstimate(flops=flops, bytes_accessed=moved, transcendentals=0)


def body(fields, ocean_mask, gain_one, w_qkv, rel_bias, w_proj, gain_two, w_up, w_down):
    sizes = Sizes(fields.shape)
    lat_cells, lon_cells, levels, features = fields.shape
    heads, length = rel_bias.shape
    group = WIN_LON * levels
    tokens = WIN_LAT * group
    window = (WIN_LAT, WIN_LON, levels, features)
    bf16, f32 = jnp.bfloat16, jnp.float32
    shape = jax.ShapeDtypeStruct
    gains = [gain_one.reshape(1, -1), gain_two.reshape(1, -1)]
    sources = [w_qkv, w_proj, w_up, w_down]
    flips = [shape(w.shape[::-1], w.dtype) for w in sources]
    dma = pltpu.SemaphoreType.DMA
    token = pl.pallas_call(
        first_kernel,
        out_shape=shape((8, 128), f32),
        out_specs=vmem(),
        cost_estimate=cost(2**36, 2**26),
        compiler_params=pltpu.CompilerParams(vmem_limit_bytes=2**20),
    )()
    bias = pl.pallas_call(
        functools.partial(table_kernel, levels),
        out_shape=shape((heads // 2, tokens, 2 * tokens), f32),
        in_specs=[vmem()] * 2,
        out_specs=vmem(),
        scratch_shapes=[
            pltpu.VMEM((heads, (length + 255) // 128 * 128), f32),
            pltpu.VMEM((heads, group, 2 * tokens), f32),
        ],
        cost_estimate=cost(0, 2**10),
        compiler_params=pltpu.CompilerParams(vmem_limit_bytes=6 * 2**20),
    )(token, rel_bias)
    pair_shape = (2, features, PAIR * tokens)
    tables = [shape((features, 128), f32)] * 2
    outcome = pl.pallas_call(
        functools.partial(early_kernel, sizes),
        out_shape=[
            shape((sizes.early,) + window, bf16),
            shape(pair_shape, bf16),
            shape((3 + 3 * sizes.count,), jnp.int32),
            shape((lat_cells + WIN_LAT // 2, lon_cells + WIN_LON // 2, levels, features), bf16),
        ]
        + flips
        + tables,
        in_specs=[smem()] + [vmem()] * 8,
        out_specs=[vmem(), vmem(), smem()] + [vmem()] * 7,
        scratch_shapes=[
            pltpu.VMEM(pair_shape, bf16),
            pltpu.VMEM(pair_shape, bf16),
            pltpu.SMEM((sizes.count + 2,), jnp.int32),
            dma((3,)),
            dma((3,)),
        ],
        cost_estimate=cost(2**36, 2**26),
        compiler_params=pltpu.CompilerParams(
            collective_id=0, has_side_effects=True, vmem_limit_bytes=24 * 2**20
        ),
    )(ocean_mask, bias, fields, gains[0], w_qkv, w_proj, gains[1], w_up, w_down)
    results, middle, plan, ext = outcome[:4]
    return pl.pallas_call(
        functools.partial(late_kernel, sizes),
        out_shape=shape(fields.shape, fields.dtype),
        in_specs=[smem()] + [vmem()] * 10,
        out_specs=any_space(),
        scratch_shapes=[
            pltpu.VMEM(pair_shape, bf16),
            pltpu.VMEM(pair_shape, bf16),
            pltpu.VMEM(pair_shape, bf16),
            pltpu.VMEM((sizes.count + PAIR,) + window, bf16),
            pltpu.VMEM(window, bf16),
            dma((sizes.count,)),
        ],
        cost_estimate=cost(0, 4 * fields.size),
        compiler_params=pltpu.CompilerParams(vmem_limit_bytes=16 * 2**20),
    )(plan, results, middle, ext, *outcome[4:], bias)


def solution(mesh):
    in_specs = (P("lat", "lon", None, None), P("lat", None), P(), P(), P(), P(), P(), P(), P())
    out_specs = P("lat", "lon", None, None)
    return jax.shard_map(body, mesh=mesh, in_specs=in_specs, out_specs=out_specs, check_vma=False)
```

```python
import functools
import math

import jax
import jax.numpy as jnp
from jax import lax
from jax.experimental import pallas as pl
from jax.experimental.pallas import tpu as pltpu
from jax.sharding import PartitionSpec as P

WIN_LAT = 8
WIN_LON = 8
NORM_FLOOR = 0.25
MESH = pl.DeviceIdType.MESH
LOG2E = math.log2(math.e)
ROOT_HALF = math.sqrt(0.5)
PAIR = 2
EARLY_PAIRS = 5
MORE_PAIRS = 1
FIRST_SENDS = 2


def dot(left, right):
    return jnp.dot(left, right, preferred_element_type=jnp.float32)


def normalise(values, gain):
    share = 1.0 / values.shape[0]
    average = jnp.sum(values, axis=0, keepdims=True) * share
    centred = values - average
    spread = jnp.sum(centred * centred, axis=0, keepdims=True) * share
    return (centred * lax.rsqrt(spread + NORM_FLOOR) * gain).astype(jnp.bfloat16)


def wide(gain, columns):
    return jnp.concatenate([gain] * (columns // gain.shape[1]), axis=1)


def flip_steps(store, blocks, weights):
    flipped = jnp.concatenate([block.T for block in blocks], axis=1)
    gain = wide(weights["gain_one"][...], flipped.shape[1])
    store.extend([flipped, normalise(flipped.astype(jnp.float32), gain)])
    yield


def attention_steps(store, flipped, normed, weights):
    qkv_t, proj_t, bias = weights["qkv"], weights["proj"], weights["bias"]
    features, columns = normed.shape
    half, tokens, _ = bias.shape
    dim = features // (2 * half)
    scale = LOG2E / math.sqrt(dim)
    key_t = dot(qkv_t[features : 2 * features], normed).astype(jnp.bfloat16)
    yield
    query_t = (dot(qkv_t[:features], normed) * scale).astype(jnp.bfloat16)
    yield
    value_t = dot(qkv_t[2 * features :], normed).astype(jnp.bfloat16)
    yield
    lane_head = lax.broadcasted_iota(jnp.int32, (tokens, features), 1) // dim % half
    nothing = jnp.zeros((features // 2, tokens), jnp.bfloat16)
    ones = jnp.ones((16, tokens), jnp.bfloat16)
    spans = [slice(n, n + tokens) for n in range(0, columns, tokens)]
    every = []
    for lanes in spans:
        key = key_t[:, lanes].T
        masked = [jnp.where(lane_head == h, key, jnp.zeros_like(key)) for h in range(half)]
        upper = jnp.concatenate([query_t[: features // 2, lanes], nothing], axis=1)
        lower = jnp.concatenate([nothing, query_t[features // 2 :, lanes]], axis=1)
        every.append(dot(jnp.concatenate(masked, axis=0), jnp.concatenate([upper, lower], axis=0)))
        yield
    mixed = []
    for lanes, products in zip(spans, every):
        first, second = [], []
        for h in range(half):
            scores = products[h * tokens : (h + 1) * tokens] + bias[h]
            power = jnp.exp2(scores - jnp.max(scores, axis=0, keepdims=True)).astype(jnp.bfloat16)
            one, two = h * dim, (h + half) * dim
            rows = [value_t[one : one + dim, lanes], value_t[two : two + dim, lanes], ones]
            piece = dot(jnp.concatenate(rows, axis=0), power)
            share = 1.0 / piece[2 * dim : 2 * dim + 1]
            first.append((piece[:dim, :tokens] * share[:, :tokens]).astype(jnp.bfloat16))
            second.append((piece[dim : 2 * dim, tokens:] * share[:, tokens:]).astype(jnp.bfloat16))
            yield
        mixed.append(jnp.concatenate(first + second, axis=0))
    projected = dot(proj_t[...], jnp.concatenate(mixed, axis=1))
    store.append((flipped.astype(jnp.float32) + projected).astype(jnp.bfloat16))
    yield


def mlp_steps(store, middle, weights, tokens):
    up_t, down_t, gain = weights["up"], weights["down"], weights["gain_two"]
    features, hidden = middle.shape[0], up_t.shape[0]
    residual = middle.astype(jnp.float32)
    normed = normalise(residual, wide(gain[...], middle.shape[1]))
    yield
    total = None
    for part in range(hidden // features):
        rows = slice(part * features, (part + 1) * features)
        grown = dot(up_t[rows], normed)
        yield
        grown = (grown * (1.0 + lax.erf(grown))).astype(jnp.bfloat16)
        piece = dot(down_t[:, rows], grown)
        total = piece if total is None else total + piece
        yield
    result = (residual + total * ROOT_HALF).astype(jnp.bfloat16)
    for n in range(middle.shape[1] // tokens):
        store.append(result[:, n * tokens : (n + 1) * tokens].T)
    yield


def weave(*steps):
    steps = list(steps)
    while steps:
        for chain in list(steps):
            try:
                next(chain)
            except StopIteration:
                steps.remove(chain)


def bias_strips(rel_bias, padded, strips, levels):
    heads, length = rel_bias.shape
    col_step = 2 * levels - 1
    row_step = (2 * WIN_LON - 1) * col_step
    offsets = [c * col_step + lev for c in range(WIN_LON) for lev in range(levels)]
    top = offsets[-1]
    width = padded.shape[1] - 128
    padded[...] = jnp.zeros_like(padded)
    padded[:, :length] = rel_bias[...] * LOG2E
    table = padded[...]
    left = jnp.concatenate([table[:, top - q : top - q + width] for q in offsets], axis=0)
    group = WIN_LON * levels
    lane = lax.broadcasted_iota(jnp.int32, (width, strips.shape[2]), 1)
    inner = lane % group
    target = lane // group * row_step + inner // levels * col_step + inner % levels
    pick = lax.broadcasted_iota(jnp.int32, target.shape, 0) == target
    found = jnp.dot(
        left,
        pick.astype(jnp.float32),
        precision=lax.Precision.HIGHEST,
        preferred_element_type=jnp.float32,
    )
    for place in range(group):
        strips[:, place, :] = found[place * heads : (place + 1) * heads]


def bias_table(strips, bias):
    heads, group, _ = strips.shape
    tokens = WIN_LAT * group
    for row in range(WIN_LAT):
        first = (WIN_LAT - 1 - row) * group
        piece = strips[:, :, first : first + tokens]
        places = slice(row * group, (row + 1) * group)
        bias[:, places, :tokens] = piece[: heads // 2]
        bias[:, places, tokens:] = piece[heads // 2 :]


class Sizes:
    def __init__(self, fields_shape):
        self.rows = fields_shape[0] // WIN_LAT
        self.cols = fields_shape[1] // WIN_LON
        self.count = self.rows * self.cols
        self.early = (EARLY_PAIRS + MORE_PAIRS) * PAIR

    def interior(self, window):
        return window // self.cols < self.rows - 1 and window % self.cols < self.cols - 1

    def fetch(self, source, window):
        row, col = window // self.cols, window % self.cols
        rows = pl.ds(row * WIN_LAT + WIN_LAT // 2, WIN_LAT)
        block = source[rows, pl.ds(col * WIN_LON + WIN_LON // 2, WIN_LON)]
        return block.reshape(block.shape[0] * block.shape[1] * block.shape[2], block.shape[3])


class Pipeline:
    def __init__(self, weights, flipped, normed, middle, tokens, keep):
        self.weights, self.tokens, self.keep = weights, tokens, keep
        self.flipped, self.normed, self.middle = flipped, normed, middle

    def prepare(self, step, blocks):
        flip = []
        weave(flip_steps(flip, blocks, self.weights))
        self.flipped[step % 2], self.normed[step % 2] = flip

    def advance(self, step, before=True, blocks=None):
        new, windows = [], []
        flip = self.flipped[step % 2], self.normed[step % 2]
        chains = [attention_steps(new, *flip, self.weights)]
        if before:
            last = self.middle[(step + 1) % 2]
            chains.insert(0, mlp_steps(windows, last, self.weights, self.tokens))
        weave(*chains)
        if blocks is not None:
            self.prepare(step + 1, blocks)
        if before:
            self.keep(step - 1, windows)
        self.middle[step % 2] = new[0]

    def finish(self, step):
        windows = []
        weave(mlp_steps(windows, self.middle[step % 2], self.weights, self.tokens))
        self.keep(step, windows)


def first_kernel(token):
    token[...] = jnp.zeros_like(token)


def table_kernel(levels, token, rel_bias, bias, padded, strips):
    bias_strips(rel_bias, padded, strips, levels)
    bias_table(strips, bias)


def early_kernel(
    sizes,
    mask, bias, fields, gain_one, w_qkv, w_proj, gain_two, w_up, w_down,
    results, middle, plan, ext, qkv_t, proj_t, up_t, down_t, gain_one_t, gain_two_t,
    flipped, normed, chains, halo_send, halo_recv,
):
    lat_cells, lon_cells, levels, features = fields.shape
    lat_half, lon_half = WIN_LAT // 2, WIN_LON // 2
    lat, lon = lax.axis_index("lat"), lax.axis_index("lon")
    lat_size, lon_size = lax.axis_size("lat"), lax.axis_size("lon")
    west, east = (lon + lon_size - 1) % lon_size, (lon + 1) % lon_size
    barrier = pltpu.get_barrier_semaphore()

    def greet(row, col):
        pl.semaphore_signal(barrier, inc=1, device_id=(row, col), device_id_type=MESH)

    greet(lat, east)

    @pl.when(lat < lat_size - 1)
    def _():
        greet(lat + 1, lon)
        greet(lat + 1, east)

    def transfer(which, source, target, row, col):
        return pltpu.make_async_remote_copy(
            src_ref=source, dst_ref=target,
            send_sem=halo_send.at[which], recv_sem=halo_recv.at[which],
            device_id=(row, col), device_id_type=MESH,
        )

    up = jnp.maximum(lat - 1, 0)
    below, beside = pl.ds(lat_cells, lat_half), pl.ds(lon_cells, lon_half)
    rows, cols = pl.ds(lat_half, lat_cells - lat_half), pl.ds(lon_half, lon_cells - lon_half)
    top, left = pl.ds(0, lat_half), pl.ds(0, lon_half)
    to_north = transfer(0, fields.at[top, cols], ext.at[below, cols], up, lon)
    to_west = transfer(1, fields.at[rows, left], ext.at[rows, beside], lat, west)
    to_corner = transfer(2, fields.at[top, left], ext.at[below, beside], up, west)

    def send_halos():
        @pl.when(lat > 0)
        def _():
            pl.semaphore_wait(barrier, 3)
            to_north.start()
            to_corner.start()

        @pl.when(lat == 0)
        def _():
            pl.semaphore_wait(barrier, 1)

        to_west.start()

    first_col = lon * sizes.cols
    total = jnp.int32(0)
    for place, inside_only in ((0, True), (1, False)):
        following = jnp.int32(sizes.count)
        chains[sizes.count] = following
        chains[sizes.count + 1] = following
        found = jnp.int32(0)
        for window in reversed(range(sizes.count)):
            if sizes.interior(window) == inside_only:
                ocean = mask[window // sizes.cols, first_col + window % sizes.cols]
                following = jnp.where(ocean == 1, window, following)
                found = found + ocean
            chains[window] = following
        plan[place] = found
        spot = following
        for n in range(sizes.count):
            plan[2 + place * sizes.count + n] = jnp.where(spot == sizes.count, 0, spot)
            spot = chains[spot + 1]

    for window in range(sizes.count):
        plan[2 + 2 * sizes.count + window] = mask[
            window // sizes.cols, first_col + window % sizes.cols
        ]
    early_pairs = jnp.where(lon == 0, EARLY_PAIRS + MORE_PAIRS, EARLY_PAIRS)
    plan[2 + 3 * sizes.count] = early_pairs
    gain_one_t[...] = jnp.broadcast_to(gain_one[...], (128, features)).T
    gain_two_t[...] = jnp.broadcast_to(gain_two[...] * ROOT_HALF, (128, features)).T
    for source, target in ((w_qkv, qkv_t), (w_proj, proj_t), (w_up, up_t), (w_down, down_t)):
        target[...] = source[...].T
    weights = dict(
        qkv=qkv_t, proj=proj_t, up=up_t, down=down_t,
        gain_one=gain_one_t, gain_two=gain_two_t, bias=bias,
    )

    def blocks(step):
        return [sizes.fetch(fields, plan[2 + step * PAIR + n]) for n in range(PAIR)]

    def keep(step, windows):
        for n, window in enumerate(windows):
            results[step * PAIR + n] = window.reshape(results.shape[1:])

    tokens = WIN_LAT * WIN_LON * levels
    line = Pipeline(weights, flipped, normed, middle, tokens, keep)
    line.prepare(0, blocks(0))
    line.advance(0, before=False, blocks=blocks(1))

    @pl.when(lon > 0)
    def _():
        send_halos()

    def early_step(step, carry):
        line.advance(step, blocks=blocks(step + 1))

        @pl.when((lon == 0) & (step == jnp.where(lat % 2 == 0, min(FIRST_SENDS, EARLY_PAIRS - 2), 1)))
        def _():
            send_halos()

        return carry

    lax.fori_loop(1, early_pairs - 1, early_step, 0)
    line.advance(early_pairs - 1)
    ext[rows, cols] = fields[rows, cols]
    to_west.wait()

    @pl.when(lat > 0)
    def _():
        to_north.wait_send()
        to_corner.wait_send()

    @pl.when(lat < lat_size - 1)
    def _():
        to_north.wait_recv()
        to_corner.wait_recv()


def late_kernel(
    sizes,
    plan, results, before, ext,
    qkv_t, proj_t, up_t, down_t, gain_one_t, gain_two_t, bias,
    output, flipped, normed, middle, late, zero, sems,
):
    inside, edges, lead = plan[0], plan[1], plan[2 + 3 * sizes.count]
    early = jnp.minimum(inside, lead * PAIR)
    rest = inside + edges - early
    pairs = (rest + PAIR - 1) // PAIR
    zero[...] = jnp.zeros_like(zero)

    def send(source, window):
        row, col = window // sizes.cols, window % sizes.cols
        target = output.at[pl.ds(row * WIN_LAT, WIN_LAT), pl.ds(col * WIN_LON, WIN_LON)]
        return pltpu.make_async_copy(source, target, sems.at[window])

    for window in range(sizes.count):

        @pl.when(plan[2 + 2 * sizes.count + window] == 0)
        def _():
            send(zero, window).start()

    def write_early(n, carry):
        send(results.at[n], plan[2 + n]).start()
        return carry

    ready = jnp.minimum(early, (lead - 1) * PAIR)
    lax.fori_loop(0, ready, write_early, 0)

    def window_of(n):
        n = jnp.clip(n, 0, sizes.count - 1)
        other = jnp.clip(early + n - edges, 0, sizes.count - 1)
        return jnp.where(n < edges, plan[2 + sizes.count + n], plan[2 + other])

    def blocks(step):
        first = (step - lead) * PAIR
        return [sizes.fetch(ext, window_of(first + n)) for n in range(PAIR)]

    def keep(step, windows):
        for n, window in enumerate(windows):
            place = (step - lead) * PAIR + n
            slot = (place + PAIR) % late.shape[0]
            late[slot] = window.reshape(zero.shape)

            @pl.when((place >= 0) & (place < rest))
            def _():
                send(late.at[slot], window_of(place)).start()

            older = lead * PAIR + place

            @pl.when((place < 0) & (older < early))
            def _():
                send(late.at[slot], plan[2 + jnp.clip(older, 0, sizes.count - 1)]).start()

    weights = dict(
        qkv=qkv_t, proj=proj_t, up=up_t, down=down_t,
        gain_one=gain_one_t, gain_two=gain_two_t, bias=bias,
    )
    tokens = bias.shape[1]
    line = Pipeline(weights, flipped, normed, middle, tokens, keep)
    last = lead - 1
    middle[last % 2] = before[last % 2]
    line.prepare(lead, blocks(lead))

    def late_step(step, carry):
        line.advance(step, blocks=blocks(step + 1))
        return carry

    lax.fori_loop(lead, lead + pairs, late_step, 0)
    line.finish(last + pairs)

    def wait(window, carry):
        send(zero, window).wait()
        return carry

    lax.fori_loop(0, sizes.count, wait, 0)


def vmem():
    return pl.BlockSpec(memory_space=pltpu.VMEM)


def smem():
    return pl.BlockSpec(memory_space=pltpu.SMEM)


def any_space():
    return pl.BlockSpec(memory_space=pl.ANY)


def cost(flops, moved):
    return pl.CostEstimate(flops=flops, bytes_accessed=moved, transcendentals=0)


def body(fields, ocean_mask, gain_one, w_qkv, rel_bias, w_proj, gain_two, w_up, w_down):
    sizes = Sizes(fields.shape)
    lat_cells, lon_cells, levels, features = fields.shape
    heads, length = rel_bias.shape
    group = WIN_LON * levels
    tokens = WIN_LAT * group
    window = (WIN_LAT, WIN_LON, levels, features)
    bf16, f32 = jnp.bfloat16, jnp.float32
    shape = jax.ShapeDtypeStruct
    gains = [gain_one.reshape(1, -1), gain_two.reshape(1, -1)]
    sources = [w_qkv, w_proj, w_up, w_down]
    flips = [shape(w.shape[::-1], w.dtype) for w in sources]
    dma = pltpu.SemaphoreType.DMA
    token = pl.pallas_call(
        first_kernel,
        out_shape=shape((8, 128), f32),
        out_specs=vmem(),
        cost_estimate=cost(2**36, 2**26),
        compiler_params=pltpu.CompilerParams(vmem_limit_bytes=2**20),
    )()
    bias = pl.pallas_call(
        functools.partial(table_kernel, levels),
        out_shape=shape((heads // 2, tokens, 2 * tokens), f32),
        in_specs=[vmem()] * 2,
        out_specs=vmem(),
        scratch_shapes=[
            pltpu.VMEM((heads, (length + 255) // 128 * 128), f32),
            pltpu.VMEM((heads, group, 2 * tokens), f32),
        ],
        cost_estimate=cost(0, 2**10),
        compiler_params=pltpu.CompilerParams(vmem_limit_bytes=6 * 2**20),
    )(token, rel_bias)
    pair_shape = (2, features, PAIR * tokens)
    tables = [shape((features, 128), f32)] * 2
    outcome = pl.pallas_call(
        functools.partial(early_kernel, sizes),
        out_shape=[
            shape((sizes.early,) + window, bf16),
            shape(pair_shape, bf16),
            shape((3 + 3 * sizes.count,), jnp.int32),
            shape((lat_cells + WIN_LAT // 2, lon_cells + WIN_LON // 2, levels, features), bf16),
        ]
        + flips
        + tables,
        in_specs=[smem()] + [vmem()] * 8,
        out_specs=[vmem(), vmem(), smem()] + [vmem()] * 7,
        scratch_shapes=[
            pltpu.VMEM(pair_shape, bf16),
            pltpu.VMEM(pair_shape, bf16),
            pltpu.SMEM((sizes.count + 2,), jnp.int32),
            dma((3,)),
            dma((3,)),
        ],
        cost_estimate=cost(2**36, 2**26),
        compiler_params=pltpu.CompilerParams(
            collective_id=0, has_side_effects=True, vmem_limit_bytes=24 * 2**20
        ),
    )(ocean_mask, bias, fields, gains[0], w_qkv, w_proj, gains[1], w_up, w_down)
    results, middle, plan, ext = outcome[:4]
    return pl.pallas_call(
        functools.partial(late_kernel, sizes),
        out_shape=shape(fields.shape, fields.dtype),
        in_specs=[smem()] + [vmem()] * 10,
        out_specs=any_space(),
        scratch_shapes=[
            pltpu.VMEM(pair_shape, bf16),
            pltpu.VMEM(pair_shape, bf16),
            pltpu.VMEM(pair_shape, bf16),
            pltpu.VMEM((sizes.count + PAIR,) + window, bf16),
            pltpu.VMEM(window, bf16),
            dma((sizes.count,)),
        ],
        cost_estimate=cost(0, 4 * fields.size),
        compiler_params=pltpu.CompilerParams(vmem_limit_bytes=16 * 2**20),
    )(plan, results, middle, ext, *outcome[4:], bias)


def solution(mesh):
    in_specs = (P("lat", "lon", None, None), P("lat", None), P(), P(), P(), P(), P(), P(), P())
    out_specs = P("lat", "lon", None, None)
    return jax.shard_map(body, mesh=mesh, in_specs=in_specs, out_specs=out_specs, check_vma=False)
```
